32 devices in a mesh: beta: 16 (over z, y, x), grp: 2 (over core).
Axes of the slice: x: 2, y: 2, z: 4, core: 2. Of those that a mesh axis runs over, the one named last changes fastest.
Arguments:
- samples: float32 [128, 8, 128, 128], P('beta', 'grp'), parts along dimension 1, may hold values from -6 to 6
Outputs:
- coeffs: float32 [128, 2, 8, 64, 64], P('beta', None, 'grp'), parts along dimension 2
- power: float32 [8, 64], P('grp'), parts along dimension 0
The draws below stay inside these ranges and needn't reach their ends.
There are 2 independent parts, one for each index of `grp`. The reference program is written for one: setup_inputs(seed, part) draws one part's arguments, and reference() takes and returns one part's arrays. A program takes and returns all parts, laid end to end along the dimension named above; each array names one. Nothing has to cross between parts.
All inputs are finite; a program needn't handle non-finite values.
Results may differ from the reference program's by a relative error of at most 0.0003.
Values sent between devices are 32-bit elements; how exact they have to be, the bound alone decides.
No kernel may reach another device: no remote copies, remote signals or barrier semaphores. Data moves between devices by JAX's collectives and lax.ppermute only.
A program may use at most 64 MiB of HBM per device.

```python
import jax
import jax.numpy as jnp
from jax import lax

F = 4
GRID = 128


def shard_levels(key, dims, pieces, smallest, top_value):
    factor_of, own = 1.0, jax.random.fold_in(key, 6)
    for position, parts in pieces:
        draws = jnp.exp(jax.random.uniform(jax.random.fold_in(own, position), (parts,), jnp.float32, smallest / len(pieces), top_value / len(pieces)))
        factor_of = factor_of * jnp.repeat(draws, dims[position] // parts).reshape([-1 if axis == position else 1 for axis in range(len(dims))])
    return factor_of


def bell_draw(own_key, dims, scale, reach, shards=(), kind=jnp.bfloat16):
    result = jax.random.normal(own_key, dims, jnp.float32) * scale
    if len(shards) > 0:
        result = shard_levels(own_key, dims, shards, -0.22, 0.18) * result
    return jnp.clip(result, min=-reach, max=reach).astype(kind)


def setup_inputs(seed: int = 0, part: int = 0) -> dict:
    key_of = jax.random.split(jax.random.key(seed), 2)
    own_keys = jax.random.split(jax.random.fold_in(key_of[1], part), 2)
    return {
        "samples": bell_draw(own_keys[0], (GRID, F, GRID, GRID), 1.0, 6.0, ((0, 16),), jnp.float32),
    }


HIGHEST = lax.Precision.HIGHEST

def beta_angles(spread):
    grid_size = 2 * spread
    return (2.0 * jnp.arange(grid_size, dtype=jnp.float32) + 1.0) * (jnp.pi / (4.0 * spread))

def quadrature(spread):
    angles = beta_angles(spread)
    odd_terms = 2.0 * jnp.arange(spread, dtype=jnp.float32) + 1.0
    series = lax.optimization_barrier(jnp.sum(jnp.sin(angles[:, None] * odd_terms[None, :]) / odd_terms[None, :], axis=1))
    return 2.0 / spread * jnp.sin(angles) * series

def gamma_table(spread):
    grid_size = 2 * spread
    positions = jnp.arange(grid_size, dtype=jnp.int32)
    orders = jnp.arange(spread, dtype=jnp.int32)
    phase_index = positions[:, None] * orders[None, :] % grid_size
    angles = phase_index.astype(jnp.float32) * (2.0 * jnp.pi / grid_size)
    return jnp.concatenate([jnp.cos(angles), -jnp.sin(angles)], axis=1)

def alpha_table(spread, row_index):
    grid_size = 2 * spread
    positions = jnp.arange(grid_size, dtype=jnp.int32)
    phase_index = row_index[:, None] * positions[None, :] % grid_size
    angles = phase_index.astype(jnp.float32) * (2.0 * jnp.pi / grid_size)
    cosine = jnp.cos(angles) / grid_size
    sine_part = jnp.sin(angles) / grid_size
    real_rows = jnp.stack([cosine, sine_part], axis=1)
    imag_rows = jnp.stack([-sine_part, cosine], axis=1)
    return jnp.stack([real_rows, imag_rows], axis=0)

def log_factorial(value, float_type):
    return lax.lgamma((value + 1).astype(float_type))

def wigner_start(alpha_order, gamma_order, log_cosine, log_sine):
    float_type = log_cosine.dtype
    lowest = jnp.maximum(jnp.abs(alpha_order), gamma_order)
    shift_low = jnp.maximum(0, gamma_order - alpha_order)
    magnitude = 0.5 * (log_factorial(lowest + alpha_order, float_type) + log_factorial(lowest - alpha_order, float_type) + log_factorial(lowest + gamma_order, float_type) + log_factorial(lowest - gamma_order, float_type))
    magnitude = magnitude - log_factorial(lowest + gamma_order - shift_low, float_type) - log_factorial(shift_low, float_type)
    magnitude = magnitude - log_factorial(alpha_order - gamma_order + shift_low, float_type)
    magnitude = magnitude - log_factorial(lowest - alpha_order - shift_low, float_type)
    cos_power = (2 * lowest + gamma_order - alpha_order - 2 * shift_low).astype(float_type)
    sin_power = (alpha_order - gamma_order + 2 * shift_low).astype(float_type)
    parity = (alpha_order - gamma_order + shift_low) % 2
    sign_factor = (1 - 2 * parity).astype(float_type)
    return sign_factor * jnp.exp(magnitude + cos_power * log_cosine + sin_power * log_sine)

def advance(degree, carried, alpha_order, gamma_order, cos_angles, start_value, lowest):
    former, current = carried
    float_type = current.dtype
    previous = (degree - 1).astype(float_type)
    alpha_float = alpha_order.astype(float_type)
    gamma_float = gamma_order.astype(float_type)
    cross_ratio = alpha_float * gamma_float / jnp.maximum(previous * (previous + 1.0), 1.0)
    upper_term = ((previous + 1.0) * (previous + 1.0) - alpha_float * alpha_float) * ((previous + 1.0) * (previous + 1.0) - gamma_float * gamma_float)
    lower_term = (previous * previous - alpha_float * alpha_float) * (previous * previous - gamma_float * gamma_float)
    root_upper = jnp.sqrt(jnp.maximum(upper_term, 1.0))
    forward = (previous + 1.0) * (2.0 * previous + 1.0) / root_upper
    backward = (previous + 1.0) * jnp.sqrt(jnp.maximum(lower_term, 0.0)) / (jnp.maximum(previous, 1.0) * root_upper)
    recurred = forward * (cos_angles - cross_ratio) * current - backward * former
    renewed = jnp.where(degree == lowest, start_value, recurred)
    return (current, renewed)

def degree_group(row_index, weighted, spread):
    grid_size = 2 * spread
    alpha_order = jnp.where(row_index < spread, row_index, row_index - grid_size)[:, None, None]
    gamma_order = jnp.arange(spread, dtype=jnp.int32)[None, None, :]
    angles = beta_angles(spread)
    cos_angles = jnp.cos(angles)[None, :, None]
    log_cosine = jnp.log(jnp.cos(0.5 * angles))[None, :, None]
    log_sine = jnp.log(jnp.sin(0.5 * angles))[None, :, None]
    lowest = jnp.maximum(jnp.abs(alpha_order), gamma_order)
    start_value = wigner_start(alpha_order, gamma_order, log_cosine, log_sine)
    empty_state = jnp.zeros((row_index.shape[0], grid_size, spread), jnp.float32)

    def level_step(carried, degree):
        carried = advance(degree, carried, alpha_order, gamma_order, cos_angles, start_value, lowest)
        contribution = jnp.einsum('gkq,kgcq->gcq', carried[1], weighted, precision=HIGHEST)
        return (carried, contribution)
    _, stacked = lax.scan(level_step, (empty_state, empty_state), jnp.arange(spread, dtype=jnp.int32))
    degree_scale = 8.0 * jnp.sqrt(2.0 * jnp.arange(spread, dtype=jnp.float32) + 1.0)
    return jnp.transpose(stacked, (1, 2, 0, 3)) * degree_scale[None, None, :, None]

def degree_energy(coeffs, spread):
    multiplicity = jnp.where(jnp.arange(spread) == 0, 1.0, 2.0).astype(jnp.float32)
    energy_sum = lax.optimization_barrier(jnp.sum(coeffs * coeffs * multiplicity, axis=(0, 1, 4)))
    degrees = 2.0 * jnp.arange(spread, dtype=jnp.float32) + 1.0
    return energy_sum / (degrees * degrees)[None, :]

def reference(samples):
    grid_size = samples.shape[2]
    spread = grid_size // 2
    functions = samples.shape[1]
    channels = 2 * functions
    halfway = jnp.einsum('kfag,gx->kfax', samples, gamma_table(spread), precision=HIGHEST)
    halfway = halfway.reshape(grid_size, functions, grid_size, 2, spread)
    row_index = jnp.arange(grid_size, dtype=jnp.int32)
    spectrum = jnp.einsum('kfacq,spca->kpsfq', halfway, alpha_table(spread, row_index), precision=HIGHEST)
    weighted = spectrum.reshape(grid_size, grid_size, channels, spread) * quadrature(spread)[:, None, None, None]
    group_size = min(32, grid_size)
    group_count = grid_size // group_size
    grouped = jnp.transpose(weighted.reshape(grid_size, group_count, group_size, channels, spread), (1, 0, 2, 3, 4))
    row_groups = row_index.reshape(group_count, group_size)

    def map_group(group_pair):
        return degree_group(group_pair[0], group_pair[1], spread)
    coeffs = lax.map(map_group, (row_groups, grouped))
    coeffs = coeffs.reshape(grid_size, 2, functions, spread, spread)
    power = degree_energy(coeffs, spread)
    return (coeffs, power)
```

```python
import math

import jax
import jax.numpy as jnp
import numpy as np
from jax import lax
from jax.experimental import pallas as pl
from jax.experimental.pallas import tpu as pltpu
from jax.sharding import PartitionSpec as P

HIGHEST = lax.Precision.HIGHEST
SUBLANES = 8
LANES = 128


def beta_angles(spread):
    grid_size = 2 * spread
    return (2.0 * jnp.arange(grid_size, dtype=jnp.float32) + 1.0) * (jnp.pi / (4.0 * spread))


def quadrature(spread):
    angles = beta_angles(spread)
    odd_terms = 2.0 * jnp.arange(spread, dtype=jnp.float32) + 1.0
    series = jnp.sum(jnp.sin(angles[:, None] * odd_terms[None, :]) / odd_terms[None, :], axis=1)
    return 2.0 / spread * jnp.sin(angles) * series


def gamma_table(spread):
    grid_size = 2 * spread
    positions = jnp.arange(grid_size, dtype=jnp.int32)
    orders = jnp.arange(spread, dtype=jnp.int32)
    phase_index = positions[:, None] * orders[None, :] % grid_size
    angles = phase_index.astype(jnp.float32) * (2.0 * jnp.pi / grid_size)
    return jnp.concatenate([jnp.cos(angles), -jnp.sin(angles)], axis=1)


def alpha_table(spread, row_index):
    grid_size = 2 * spread
    positions = jnp.arange(grid_size, dtype=jnp.int32)
    phase_index = row_index[:, None] * positions[None, :] % grid_size
    angles = phase_index.astype(jnp.float32) * (2.0 * jnp.pi / grid_size)
    cosine = jnp.cos(angles) / grid_size
    sine_part = jnp.sin(angles) / grid_size
    real_rows = jnp.stack([cosine, sine_part], axis=1)
    imag_rows = jnp.stack([-sine_part, cosine], axis=1)
    return jnp.stack([real_rows, imag_rows], axis=0)


def log_factorial(value, float_type):
    return lax.lgamma((value + 1).astype(float_type))


def wigner_start(alpha_order, gamma_order, log_cosine, log_sine):
    float_type = log_cosine.dtype
    lowest = jnp.maximum(jnp.abs(alpha_order), gamma_order)
    shift_low = jnp.maximum(0, gamma_order - alpha_order)
    magnitude = 0.5 * (
        log_factorial(lowest + alpha_order, float_type)
        + log_factorial(lowest - alpha_order, float_type)
        + log_factorial(lowest + gamma_order, float_type)
        + log_factorial(lowest - gamma_order, float_type)
    )
    magnitude = (
        magnitude
        - log_factorial(lowest + gamma_order - shift_low, float_type)
        - log_factorial(shift_low, float_type)
    )
    magnitude = magnitude - log_factorial(alpha_order - gamma_order + shift_low, float_type)
    magnitude = magnitude - log_factorial(lowest - alpha_order - shift_low, float_type)
    cos_power = (2 * lowest + gamma_order - alpha_order - 2 * shift_low).astype(float_type)
    sin_power = (alpha_order - gamma_order + 2 * shift_low).astype(float_type)
    parity = (alpha_order - gamma_order + shift_low) % 2
    sign_factor = (1 - 2 * parity).astype(float_type)
    return sign_factor * jnp.exp(magnitude + cos_power * log_cosine + sin_power * log_sine)


def advance(degree, carried, alpha_order, gamma_order, cos_angles, start_value, lowest):
    former, current = carried
    float_type = current.dtype
    previous = (degree - 1).astype(float_type)
    alpha_float = alpha_order.astype(float_type)
    gamma_float = gamma_order.astype(float_type)
    cross_ratio = alpha_float * gamma_float / jnp.maximum(previous * (previous + 1.0), 1.0)
    upper_term = ((previous + 1.0) * (previous + 1.0) - alpha_float * alpha_float) * (
        (previous + 1.0) * (previous + 1.0) - gamma_float * gamma_float
    )
    lower_term = (previous * previous - alpha_float * alpha_float) * (
        previous * previous - gamma_float * gamma_float
    )
    root_upper = jnp.sqrt(jnp.maximum(upper_term, 1.0))
    forward = (previous + 1.0) * (2.0 * previous + 1.0) / root_upper
    backward = (
        (previous + 1.0)
        * jnp.sqrt(jnp.maximum(lower_term, 0.0))
        / (jnp.maximum(previous, 1.0) * root_upper)
    )
    recurred = forward * (cos_angles - cross_ratio) * current - backward * former
    renewed = jnp.where(degree == lowest, start_value, recurred)
    return (current, renewed)


def degree_rows(row_index, weighted, spread):
    stride = 8
    grid_size = 2 * spread
    group_size = row_index.shape[0]
    channels = weighted.shape[2]
    block_count = spread // stride
    alpha_order = jnp.where(row_index < spread, row_index, row_index - grid_size)[:, None, None]
    gamma_order = jnp.arange(spread, dtype=jnp.int32)[None, None, :]
    angles = beta_angles(spread)
    cos_angles = jnp.cos(angles)[None, :, None]
    log_cosine = jnp.log(jnp.cos(0.5 * angles))[None, :, None]
    log_sine = jnp.log(jnp.sin(0.5 * angles))[None, :, None]
    lowest = jnp.maximum(jnp.abs(alpha_order), gamma_order)
    start_value = wigner_start(alpha_order, gamma_order, log_cosine, log_sine)
    first_block = jnp.min(jnp.abs(alpha_order)) // stride
    empty_state = jnp.zeros((group_size, grid_size, spread), jnp.float32)

    def compute_block(operands):
        block_index, former, current = operands
        levels = []
        for offset in range(stride):
            former, current = advance(
                block_index * stride + offset,
                (former, current),
                alpha_order,
                gamma_order,
                cos_angles,
                start_value,
                lowest,
            )
            levels.append(current)
        stacked = jnp.stack(levels, axis=0)
        block_part = jnp.einsum("jgkq,kgcq->gcjq", stacked, weighted, precision=HIGHEST)
        return (former, current, block_part)

    def skip_block(operands):
        block_index, former, current = operands
        return (former, current, jnp.zeros((group_size, channels, stride, spread), jnp.float32))

    def block_step(carried, block_index):
        former, current = carried
        former, current, block_part = lax.cond(
            block_index >= first_block, compute_block, skip_block, (block_index, former, current)
        )
        return ((former, current), block_part)

    _, parts = lax.scan(
        block_step, (empty_state, empty_state), jnp.arange(block_count, dtype=jnp.int32)
    )
    output = jnp.transpose(parts, (1, 2, 0, 3, 4)).reshape(group_size, channels, spread, spread)
    degree_scale = 8.0 * jnp.sqrt(2.0 * jnp.arange(spread, dtype=jnp.float32) + 1.0)
    return output * degree_scale[None, None, :, None]


def degree_energy(coeffs, functions, spread):
    split_view = coeffs.reshape(coeffs.shape[0], 2, functions, spread, spread)
    multiplicity = jnp.where(jnp.arange(spread) == 0, 1.0, 2.0).astype(jnp.float32)
    energy_sum = jnp.sum(split_view * split_view * multiplicity, axis=(0, 1, 4))
    degrees = 2.0 * jnp.arange(spread, dtype=jnp.float32) + 1.0
    return energy_sum / (degrees * degrees)[None, :]


def general_local(samples):
    devices = lax.axis_size("beta")
    device = lax.axis_index("beta")
    local_beta = samples.shape[0]
    functions = samples.shape[1]
    grid_size = samples.shape[2]
    spread = grid_size // 2
    channels = 2 * functions
    row_count = grid_size // devices
    natural_rows = jnp.arange(grid_size, dtype=jnp.int32)
    halfway = jnp.einsum("kfag,gx->kfax", samples, gamma_table(spread), precision=HIGHEST)
    halfway = halfway.reshape(local_beta, functions, grid_size, 2, spread)
    spectrum = jnp.einsum(
        "kfacq,spca->kpsfq", halfway, alpha_table(spread, natural_rows), precision=HIGHEST
    )
    spectrum = spectrum.reshape(local_beta, grid_size, channels, spread)
    received = lax.all_to_all(spectrum, "beta", split_axis=1, concat_axis=0, tiled=True)
    weighted = received * quadrature(spread)[:, None, None, None]
    owned_rows = lax.dynamic_slice_in_dim(natural_rows, device * row_count, row_count)
    computed = degree_rows(owned_rows, weighted, spread)
    power_part = degree_energy(computed, functions, spread)
    coeffs = computed
    power = lax.psum(power_part, "beta")
    coeffs = coeffs.reshape(row_count, 2, functions, spread, spread)
    return (coeffs, power)


def wigner_quarter(spread):
    alpha = np.arange(1 - spread, spread)[:, None]
    gamma = np.arange(spread)[None, :]
    lowest = np.maximum(np.abs(alpha), gamma)
    shift = np.maximum(0, gamma - alpha)
    logs = np.array([math.lgamma(value + 1.0) for value in range(2 * spread)])
    magnitude = 0.5 * (
        logs[lowest + alpha] + logs[lowest - alpha] + logs[lowest + gamma] + logs[lowest - gamma]
    )
    magnitude = magnitude - logs[lowest + gamma - shift] - logs[shift]
    magnitude = magnitude - logs[alpha - gamma + shift] - logs[lowest - alpha - shift]
    sign = 1.0 - 2.0 * ((alpha - gamma + shift) % 2)
    first = sign * np.exp(magnitude - lowest * math.log(2.0))
    squares_a, squares_g = alpha.astype(np.float64) ** 2, gamma.astype(np.float64) ** 2
    former, current, levels = np.zeros(first.shape), np.zeros(first.shape), []
    for degree in range(spread):
        before = degree - 1.0
        upper = np.sqrt(np.maximum((degree**2 - squares_a) * (degree**2 - squares_g), 1.0))
        lower = np.sqrt(np.maximum((before**2 - squares_a) * (before**2 - squares_g), 0.0))
        cross = alpha * gamma / max(before * degree, 1.0)
        follow = degree * (2.0 * before + 1.0) / upper * -cross * current
        follow = follow - degree * lower / (max(before, 1.0) * upper) * former
        former, current = current, np.where(lowest == degree, first, follow)
        levels.append(current)
    return np.stack(levels)


def split_pair(table):
    high = np.asarray(table).astype(jnp.bfloat16)
    return high, (table - high.astype(np.float64)).astype(jnp.bfloat16)


def fourier_tables(spread):
    grid = 2 * spread
    at = np.arange(grid)
    phase = 2.0 * np.pi / grid * (at[:, None] * np.arange(spread)[None, :] % grid)
    cosine, sine = np.cos(phase), -np.sin(phase)
    gamma_part = np.concatenate([cosine, sine, sine, -cosine], axis=1)
    phase = 2.0 * np.pi / grid * (at[:, None] * at[None, :] % grid)
    alpha_part = np.concatenate([np.cos(phase), np.sin(phase)], axis=1) / grid
    return gamma_part, alpha_part


def beta_table(spread):
    angles = (2.0 * np.arange(2 * spread) + 1.0) * (np.pi / (4.0 * spread))
    odd = 2.0 * np.arange(spread) + 1.0
    series = np.sum(np.sin(angles[:, None] * odd[None, :]) / odd[None, :], axis=1)
    weight = 2.0 / spread * np.sin(angles) * series
    order = np.arange(spread)
    fold = np.where(order == 0, 1.0, 2.0)[:, None] * weight[None, :]
    turn = order[:, None] * angles[None, :]
    return np.concatenate([fold * np.cos(turn), fold * np.sin(turn)], axis=1)


def sign_masks(spread):
    step = (np.arange(SUBLANES)[:, None] - np.arange(spread)[None, :]) % 4
    even = np.where(step == 0, 1.0, np.where(step == 2, -1.0, 0.0))
    odd = np.where(step == 3, 1.0, np.where(step == 1, -1.0, 0.0))
    return np.concatenate([even, even], axis=1), np.concatenate([odd, odd], axis=1)


def block_steps(spread):
    width = LANES // SUBLANES
    return [
        (block, chunk)
        for block in range(spread // SUBLANES)
        for chunk in range(-(-(block + 1) * SUBLANES // width))
    ]


def quarter_tables(spread, devices):
    quarter = wigner_quarter(spread)
    grid, width = 2 * spread, LANES // SUBLANES
    rows = np.arange(grid)
    orders = np.where(rows < spread, rows, rows - grid)
    held = np.clip(orders + spread - 1, 0, 2 * spread - 2)
    by_row = np.where((orders > -spread)[None, :, None], quarter[:, held, :], 0.0)
    by_row = by_row * (8.0 * np.sqrt(2.0 * np.arange(spread) + 1.0))[:, None, None]
    gammas, alphas = [], []
    for block, chunk in block_steps(spread):
        degrees = slice(block * SUBLANES, (block + 1) * SUBLANES)
        part = slice(chunk * width, (chunk + 1) * width)
        table = np.swapaxes(quarter[degrees, spread - 1 :, part], 1, 2).reshape(LANES, spread)
        gammas.append(np.concatenate([table, table], axis=1))
        table = np.swapaxes(by_row[degrees, :, part], 0, 1).reshape(devices, SUBLANES, LANES)
        alphas.append(table)
    return np.stack(gammas).astype(np.float32), np.stack(alphas, axis=1).astype(np.float32)


def split_value(value):
    high = value.astype(jnp.bfloat16)
    return high, (value - high.astype(jnp.float32)).astype(jnp.bfloat16)


def dot(left, right):
    return jnp.dot(left, right, preferred_element_type=jnp.float32)


def spectrum_kernel(x_ref, gamma_hi, gamma_lo, alpha_hi, alpha_lo, out_ref):
    count, _, grid, _ = x_ref.shape
    blocks = out_ref.shape[0]
    for k in range(count):
        high, low = split_value(x_ref[k, 0])
        half = dot(high, gamma_hi[...]) + dot(low, gamma_hi[...]) + dot(high, gamma_lo[...])
        pair = jnp.concatenate([half[:, :LANES], half[:, LANES:]], axis=0)
        high, low = split_value(pair)
        rows = dot(alpha_hi[...], high) + dot(alpha_lo[...], high) + dot(alpha_hi[...], low)
        for d in range(blocks):
            out_ref[d, 0, pl.ds(k, SUBLANES, stride=count), :] = rows[
                d * SUBLANES : (d + 1) * SUBLANES
            ]


def spectrum_call(samples, devices):
    count, functions, grid, _ = samples.shape
    gamma_part, alpha_part = fourier_tables(grid // 2)
    tables = [*split_pair(gamma_part), *split_pair(alpha_part)]
    rows = grid // devices * count
    whole = lambda table: pl.BlockSpec(table.shape, lambda f: (0, 0))
    return pl.pallas_call(
        spectrum_kernel,
        grid=(functions,),
        in_specs=[pl.BlockSpec((count, 1, grid, grid), lambda f: (0, f, 0, 0))]
        + [whole(table) for table in tables],
        out_specs=pl.BlockSpec((devices, 1, rows, LANES), lambda f: (0, f, 0, 0)),
        out_shape=jax.ShapeDtypeStruct((devices, functions, rows, LANES), jnp.float32),
        name="spectrum",
    )(samples, *tables)


def degree_kernel(
    r_ref, beta_hi, beta_lo, even_ref, odd_ref, gamma_ref, alpha_ref, out_ref, pow_ref, t_ref, c_ref
):
    sources, functions, held, _ = r_ref.shape
    count = held // SUBLANES
    spread = beta_hi.shape[0]
    width = LANES // SUBLANES
    for f in range(0, functions, 2):
        for n in range(SUBLANES):
            parts = [
                r_ref[:, f + i, n * count : (n + 1) * count, :].reshape(sources * count, LANES)
                for i in range(2)
            ]
            high, low = split_value(jnp.concatenate(parts, axis=1))
            even = jnp.concatenate([even_ref[n : n + 1, :]] * 2, axis=1)
            odd = jnp.concatenate([odd_ref[n : n + 1, :]] * 2, axis=1)
            high = jnp.concatenate([high * even, high * odd], axis=0)
            low = jnp.concatenate([low * even, low * odd], axis=0)
            turned = dot(beta_hi[...], high) + dot(beta_lo[...], high) + dot(beta_hi[...], low)
            for i in range(2):
                for b in range(spread // SUBLANES):
                    t_ref[f + i, pl.ds(b * SUBLANES * SUBLANES + n, SUBLANES, stride=SUBLANES), :] = (
                        turned[b * SUBLANES : (b + 1) * SUBLANES, i * LANES : (i + 1) * LANES]
                    )

    lane = lax.broadcasted_iota(jnp.int32, (SUBLANES, LANES), 1)
    fold = jnp.where(lane % spread == 0, 1.0, 2.0).astype(jnp.float32)

    def block_step(block, first):
        chunks = (block * SUBLANES + SUBLANES + width - 1) // width

        def chunk_step(chunk, totals):
            totals = list(totals)
            column = alpha_ref[first + chunk]
            for m in range(width):
                row = pl.multiple_of((chunk * width + m) * SUBLANES, SUBLANES)
                values = [t_ref[f, pl.ds(row, SUBLANES), :] for f in range(functions)]
                for j in range(SUBLANES):
                    at = j * width + m
                    table = gamma_ref[first + chunk, pl.ds(at, SUBLANES, stride=0), :]
                    factor = jnp.broadcast_to(column[:, at : at + 1], (SUBLANES, LANES)) * table
                    for f in range(functions):
                        totals[j * functions + f] += factor * values[f]
            return tuple(totals)

        zero = jnp.zeros((SUBLANES, LANES), jnp.float32)
        totals = lax.fori_loop(0, chunks, chunk_step, (zero,) * (SUBLANES * functions))
        degree = pl.multiple_of(block * SUBLANES, SUBLANES)
        for f in range(functions):
            for j in range(SUBLANES):
                c_ref[f, pl.ds(j, SUBLANES, stride=SUBLANES), :] = totals[j * functions + f]
            energy = zero
            for n in range(SUBLANES):
                tile = c_ref[f, n * SUBLANES : (n + 1) * SUBLANES, :]
                energy += tile * tile
                out_ref[n, 0, f, pl.ds(degree, SUBLANES), :] = tile[:, :spread]
                out_ref[n, 1, f, pl.ds(degree, SUBLANES), :] = tile[:, spread:]
            pow_ref[f, pl.ds(degree, SUBLANES), :] = energy * fold
        return first + chunks

    lax.fori_loop(0, spread // SUBLANES, block_step, 0)


def degree_call(received, gammas, alphas, spread):
    functions = received.shape[1]
    tables = [*split_pair(beta_table(spread))]
    tables += [mask.astype(jnp.bfloat16) for mask in sign_masks(spread)]
    return pl.pallas_call(
        degree_kernel,
        out_shape=[
            jax.ShapeDtypeStruct((SUBLANES, 2, functions, spread, spread), jnp.float32),
            jax.ShapeDtypeStruct((functions, spread, LANES), jnp.float32),
        ],
        scratch_shapes=[
            pltpu.VMEM((functions, spread * SUBLANES, LANES), jnp.float32),
            pltpu.VMEM((functions, SUBLANES * SUBLANES, LANES), jnp.float32),
        ],
        name="degrees",
    )(received, *tables, gammas, alphas)


def fast_local(samples):
    devices = lax.axis_size("beta")
    device = lax.axis_index("beta")
    functions, grid_size = samples.shape[1:3]
    spread = grid_size // 2
    sent = spectrum_call(samples, devices)
    received = lax.all_to_all(sent, "beta", split_axis=0, concat_axis=0, tiled=True)
    gammas, alphas = quarter_tables(spread, devices)
    alphas = lax.dynamic_index_in_dim(jnp.asarray(alphas), device, 0, keepdims=False)
    coeffs, energy = degree_call(received, jnp.asarray(gammas), alphas, spread)
    share = jnp.sum(energy, axis=-1)
    shares = jnp.broadcast_to(share[None], (devices, functions, spread))
    shares = lax.all_to_all(shares, "beta", split_axis=0, concat_axis=0, tiled=True)
    degrees = 2.0 * jnp.arange(spread, dtype=jnp.float32) + 1.0
    return coeffs, jnp.sum(shares, axis=0) / (degrees * degrees)[None, :]


def local(samples):
    devices = lax.axis_size("beta")
    local_beta, functions, grid_size = samples.shape[:3]
    tiled = grid_size == LANES and local_beta == SUBLANES and grid_size == devices * SUBLANES
    if tiled and functions % 2 == 0:
        return fast_local(samples)
    return general_local(samples)


def solution(mesh):
    return jax.shard_map(
        local,
        mesh=mesh,
        in_specs=(P("beta", "grp", None, None),),
        out_specs=(P("beta", None, "grp", None, None), P("grp", None)),
        check_vma=False,
    )
```

```python
import math

import jax
import jax.numpy as jnp
import numpy as np
from jax import lax
from jax.experimental import pallas as pl
from jax.experimental.pallas import tpu as pltpu
from jax.sharding import PartitionSpec as P

HIGHEST = lax.Precision.HIGHEST
SUBLANES = 8
LANES = 128


def beta_angles(spread):
    grid_size = 2 * spread
    return (2.0 * jnp.arange(grid_size, dtype=jnp.float32) + 1.0) * (jnp.pi / (4.0 * spread))


def quadrature(spread):
    angles = beta_angles(spread)
    odd_terms = 2.0 * jnp.arange(spread, dtype=jnp.float32) + 1.0
    series = jnp.sum(jnp.sin(angles[:, None] * odd_terms[None, :]) / odd_terms[None, :], axis=1)
    return 2.0 / spread * jnp.sin(angles) * series


def gamma_table(spread):
    grid_size = 2 * spread
    positions = jnp.arange(grid_size, dtype=jnp.int32)
    orders = jnp.arange(spread, dtype=jnp.int32)
    phase_index = positions[:, None] * orders[None, :] % grid_size
    angles = phase_index.astype(jnp.float32) * (2.0 * jnp.pi / grid_size)
    return jnp.concatenate([jnp.cos(angles), -jnp.sin(angles)], axis=1)


def alpha_table(spread, row_index):
    grid_size = 2 * spread
    positions = jnp.arange(grid_size, dtype=jnp.int32)
    phase_index = row_index[:, None] * positions[None, :] % grid_size
    angles = phase_index.astype(jnp.float32) * (2.0 * jnp.pi / grid_size)
    cosine = jnp.cos(angles) / grid_size
    sine_part = jnp.sin(angles) / grid_size
    real_rows = jnp.stack([cosine, sine_part], axis=1)
    imag_rows = jnp.stack([-sine_part, cosine], axis=1)
    return jnp.stack([real_rows, imag_rows], axis=0)


def log_factorial(value, float_type):
    return lax.lgamma((value + 1).astype(float_type))


def wigner_start(alpha_order, gamma_order, log_cosine, log_sine):
    float_type = log_cosine.dtype
    lowest = jnp.maximum(jnp.abs(alpha_order), gamma_order)
    shift_low = jnp.maximum(0, gamma_order - alpha_order)
    magnitude = 0.5 * (
        log_factorial(lowest + alpha_order, float_type)
        + log_factorial(lowest - alpha_order, float_type)
        + log_factorial(lowest + gamma_order, float_type)
        + log_factorial(lowest - gamma_order, float_type)
    )
    magnitude = (
        magnitude
        - log_factorial(lowest + gamma_order - shift_low, float_type)
        - log_factorial(shift_low, float_type)
    )
    magnitude = magnitude - log_factorial(alpha_order - gamma_order + shift_low, float_type)
    magnitude = magnitude - log_factorial(lowest - alpha_order - shift_low, float_type)
    cos_power = (2 * lowest + gamma_order - alpha_order - 2 * shift_low).astype(float_type)
    sin_power = (alpha_order - gamma_order + 2 * shift_low).astype(float_type)
    parity = (alpha_order - gamma_order + shift_low) % 2
    sign_factor = (1 - 2 * parity).astype(float_type)
    return sign_factor * jnp.exp(magnitude + cos_power * log_cosine + sin_power * log_sine)


def advance(degree, carried, alpha_order, gamma_order, cos_angles, start_value, lowest):
    former, current = carried
    float_type = current.dtype
    previous = (degree - 1).astype(float_type)
    alpha_float = alpha_order.astype(float_type)
    gamma_float = gamma_order.astype(float_type)
    cross_ratio = alpha_float * gamma_float / jnp.maximum(previous * (previous + 1.0), 1.0)
    upper_term = ((previous + 1.0) * (previous + 1.0) - alpha_float * alpha_float) * (
        (previous + 1.0) * (previous + 1.0) - gamma_float * gamma_float
    )
    lower_term = (previous * previous - alpha_float * alpha_float) * (
        previous * previous - gamma_float * gamma_float
    )
    root_upper = jnp.sqrt(jnp.maximum(upper_term, 1.0))
    forward = (previous + 1.0) * (2.0 * previous + 1.0) / root_upper
    backward = (
        (previous + 1.0)
        * jnp.sqrt(jnp.maximum(lower_term, 0.0))
        / (jnp.maximum(previous, 1.0) * root_upper)
    )
    recurred = forward * (cos_angles - cross_ratio) * current - backward * former
    renewed = jnp.where(degree == lowest, start_value, recurred)
    return (current, renewed)


def degree_rows(row_index, weighted, spread):
    stride = 8
    grid_size = 2 * spread
    group_size = row_index.shape[0]
    channels = weighted.shape[2]
    block_count = spread // stride
    alpha_order = jnp.where(row_index < spread, row_index, row_index - grid_size)[:, None, None]
    gamma_order = jnp.arange(spread, dtype=jnp.int32)[None, None, :]
    angles = beta_angles(spread)
    cos_angles = jnp.cos(angles)[None, :, None]
    log_cosine = jnp.log(jnp.cos(0.5 * angles))[None, :, None]
    log_sine = jnp.log(jnp.sin(0.5 * angles))[None, :, None]
    lowest = jnp.maximum(jnp.abs(alpha_order), gamma_order)
    start_value = wigner_start(alpha_order, gamma_order, log_cosine, log_sine)
    first_block = jnp.min(jnp.abs(alpha_order)) // stride
    empty_state = jnp.zeros((group_size, grid_size, spread), jnp.float32)

    def compute_block(operands):
        block_index, former, current = operands
        levels = []
        for offset in range(stride):
            former, current = advance(
                block_index * stride + offset,
                (former, current),
                alpha_order,
                gamma_order,
                cos_angles,
                start_value,
                lowest,
            )
            levels.append(current)
        stacked = jnp.stack(levels, axis=0)
        block_part = jnp.einsum("jgkq,kgcq->gcjq", stacked, weighted, precision=HIGHEST)
        return (former, current, block_part)

    def skip_block(operands):
        block_index, former, current = operands
        return (former, current, jnp.zeros((group_size, channels, stride, spread), jnp.float32))

    def block_step(carried, block_index):
        former, current = carried
        former, current, block_part = lax.cond(
            block_index >= first_block, compute_block, skip_block, (block_index, former, current)
        )
        return ((former, current), block_part)

    _, parts = lax.scan(
        block_step, (empty_state, empty_state), jnp.arange(block_count, dtype=jnp.int32)
    )
    output = jnp.transpose(parts, (1, 2, 0, 3, 4)).reshape(group_size, channels, spread, spread)
    degree_scale = 8.0 * jnp.sqrt(2.0 * jnp.arange(spread, dtype=jnp.float32) + 1.0)
    return output * degree_scale[None, None, :, None]


def degree_energy(coeffs, functions, spread):
    split_view = coeffs.reshape(coeffs.shape[0], 2, functions, spread, spread)
    multiplicity = jnp.where(jnp.arange(spread) == 0, 1.0, 2.0).astype(jnp.float32)
    energy_sum = jnp.sum(split_view * split_view * multiplicity, axis=(0, 1, 4))
    degrees = 2.0 * jnp.arange(spread, dtype=jnp.float32) + 1.0
    return energy_sum / (degrees * degrees)[None, :]


def general_local(samples):
    devices = lax.axis_size("beta")
    device = lax.axis_index("beta")
    local_beta = samples.shape[0]
    functions = samples.shape[1]
    grid_size = samples.shape[2]
    spread = grid_size // 2
    channels = 2 * functions
    row_count = grid_size // devices
    natural_rows = jnp.arange(grid_size, dtype=jnp.int32)
    halfway = jnp.einsum("kfag,gx->kfax", samples, gamma_table(spread), precision=HIGHEST)
    halfway = halfway.reshape(local_beta, functions, grid_size, 2, spread)
    spectrum = jnp.einsum(
        "kfacq,spca->kpsfq", halfway, alpha_table(spread, natural_rows), precision=HIGHEST
    )
    spectrum = spectrum.reshape(local_beta, grid_size, channels, spread)
    received = lax.all_to_all(spectrum, "beta", split_axis=1, concat_axis=0, tiled=True)
    weighted = received * quadrature(spread)[:, None, None, None]
    owned_rows = lax.dynamic_slice_in_dim(natural_rows, device * row_count, row_count)
    computed = degree_rows(owned_rows, weighted, spread)
    power_part = degree_energy(computed, functions, spread)
    coeffs = computed
    power = lax.psum(power_part, "beta")
    coeffs = coeffs.reshape(row_count, 2, functions, spread, spread)
    return (coeffs, power)


def wigner_quarter(spread):
    alpha = np.arange(1 - spread, spread)[:, None]
    gamma = np.arange(spread)[None, :]
    lowest = np.maximum(np.abs(alpha), gamma)
    shift = np.maximum(0, gamma - alpha)
    logs = np.array([math.lgamma(value + 1.0) for value in range(2 * spread)])
    magnitude = 0.5 * (
        logs[lowest + alpha] + logs[lowest - alpha] + logs[lowest + gamma] + logs[lowest - gamma]
    )
    magnitude = magnitude - logs[lowest + gamma - shift] - logs[shift]
    magnitude = magnitude - logs[alpha - gamma + shift] - logs[lowest - alpha - shift]
    sign = 1.0 - 2.0 * ((alpha - gamma + shift) % 2)
    first = sign * np.exp(magnitude - lowest * math.log(2.0))
    squares_a, squares_g = alpha.astype(np.float64) ** 2, gamma.astype(np.float64) ** 2
    former, current, levels = np.zeros(first.shape), np.zeros(first.shape), []
    for degree in range(spread):
        before = degree - 1.0
        upper = np.sqrt(np.maximum((degree**2 - squares_a) * (degree**2 - squares_g), 1.0))
        lower = np.sqrt(np.maximum((before**2 - squares_a) * (before**2 - squares_g), 0.0))
        cross = alpha * gamma / max(before * degree, 1.0)
        follow = degree * (2.0 * before + 1.0) / upper * -cross * current
        follow = follow - degree * lower / (max(before, 1.0) * upper) * former
        former, current = current, np.where(lowest == degree, first, follow)
        levels.append(current)
    return np.stack(levels)


def split_pair(table):
    high = np.asarray(table).astype(jnp.bfloat16)
    return high, (table - high.astype(np.float64)).astype(jnp.bfloat16)


def fourier_tables(spread):
    grid = 2 * spread
    at = np.arange(grid)
    phase = 2.0 * np.pi / grid * (at[:, None] * np.arange(spread)[None, :] % grid)
    cosine, sine = np.cos(phase), -np.sin(phase)
    gamma_part = np.concatenate([cosine, sine, sine, -cosine], axis=1)
    phase = 2.0 * np.pi / grid * (at[:, None] * at[None, :] % grid)
    alpha_part = np.concatenate([np.cos(phase), np.sin(phase)], axis=1) / grid
    return gamma_part, alpha_part


def beta_table(spread):
    angles = (2.0 * np.arange(2 * spread) + 1.0) * (np.pi / (4.0 * spread))
    odd = 2.0 * np.arange(spread) + 1.0
    series = np.sum(np.sin(angles[:, None] * odd[None, :]) / odd[None, :], axis=1)
    weight = 2.0 / spread * np.sin(angles) * series
    order = np.arange(spread)
    fold = np.where(order == 0, 1.0, 2.0)[:, None] * weight[None, :]
    turn = order[:, None] * angles[None, :]
    return np.concatenate([fold * np.cos(turn), fold * np.sin(turn)], axis=1)


def sign_masks(spread):
    step = (np.arange(SUBLANES)[:, None] - np.arange(spread)[None, :]) % 4
    even = np.where(step == 0, 1.0, np.where(step == 2, -1.0, 0.0))
    odd = np.where(step == 3, 1.0, np.where(step == 1, -1.0, 0.0))
    return np.concatenate([even, even], axis=1), np.concatenate([odd, odd], axis=1)


def block_steps(spread):
    blocks = spread // SUBLANES
    return [(block, chunk) for block in range(blocks) for chunk in range(block + 1)]


def quarter_tables(spread, devices):
    quarter = wigner_quarter(spread)
    rows = np.arange(2 * spread)
    orders = np.where(rows < spread, rows, rows - 2 * spread)
    by_row = quarter[:, np.maximum(orders, 1 - spread) + spread - 1, :]
    by_row = np.where((orders > -spread)[None, :, None], by_row, 0.0)
    by_row = by_row * (8.0 * np.sqrt(2.0 * np.arange(spread) + 1.0))[:, None, None]
    gammas, alphas = [], []
    for block, chunk in block_steps(spread):
        degrees = slice(block * SUBLANES, (block + 1) * SUBLANES)
        part = slice(chunk * SUBLANES, (chunk + 1) * SUBLANES)
        table = np.swapaxes(quarter[degrees, spread - 1 :, part], 1, 2).reshape(-1, spread)
        gammas.append(np.concatenate([table, table], axis=1))
        table = np.swapaxes(by_row[degrees, :, part], 0, 1)
        alphas.append(table.reshape(devices, SUBLANES, SUBLANES * SUBLANES))
    alphas = np.stack(alphas, axis=1)
    alphas = np.concatenate([alphas[:, 0::2], alphas[:, 1::2]], axis=-1)
    return np.stack(gammas).astype(np.float32), alphas.astype(np.float32)


def split_value(value):
    high = value.astype(jnp.bfloat16)
    return high, (value - high.astype(jnp.float32)).astype(jnp.bfloat16)


def dot(left, right):
    return jnp.dot(left, right, preferred_element_type=jnp.float32)


def spectrum_kernel(x_ref, gamma_two, gamma_lo, alpha_hi, alpha_lo, out_ref):
    count, _, grid, _ = x_ref.shape
    blocks = out_ref.shape[0]
    high, low = split_value(x_ref[:, 0].reshape(count * grid, grid))
    half = dot(jnp.concatenate([high, low], axis=1), gamma_two[...]) + dot(high, gamma_lo[...])
    for k in range(0, count, 2):
        pairs = [half[(k + i) * grid : (k + i + 1) * grid] for i in range(2)]
        pair = jnp.concatenate(
            [
                jnp.concatenate([p[:, :LANES] for p in pairs], axis=1),
                jnp.concatenate([p[:, LANES:] for p in pairs], axis=1),
            ],
            axis=0,
        )
        high, low = split_value(pair)
        rows = dot(alpha_hi[...], high) + dot(alpha_lo[...], high) + dot(alpha_hi[...], low)
        for i in range(2):
            for d in range(blocks):
                out_ref[d, 0, pl.ds(k + i, SUBLANES, stride=count), :] = rows[
                    d * SUBLANES : (d + 1) * SUBLANES, i * LANES : (i + 1) * LANES
                ]


def spectrum_call(samples, devices):
    count, functions, grid, _ = samples.shape
    gamma_part, alpha_part = fourier_tables(grid // 2)
    gamma_hi, gamma_lo = split_pair(gamma_part)
    tables = [np.concatenate([gamma_hi, gamma_hi], axis=0), gamma_lo, *split_pair(alpha_part)]
    rows = grid // devices * count
    whole = lambda table: pl.BlockSpec(table.shape, lambda f: (0, 0))
    return pl.pallas_call(
        spectrum_kernel,
        grid=(functions,),
        in_specs=[pl.BlockSpec((count, 1, grid, grid), lambda f: (0, f, 0, 0))]
        + [whole(table) for table in tables],
        out_specs=pl.BlockSpec((devices, 1, rows, LANES), lambda f: (0, f, 0, 0)),
        out_shape=jax.ShapeDtypeStruct((devices, functions, rows, LANES), jnp.float32),
        name="spectrum",
    )(samples, *tables)


def factor_kernel(gamma_ref, alpha_ref, out_ref):
    pairs = out_ref.shape[1]

    def step(at, carry):
        column = alpha_ref[at]
        for half in range(2):
            for i in range(pairs):
                lane = half * pairs + i
                row = gamma_ref[2 * at + half, pl.ds(i, SUBLANES, stride=0), :]
                wide = jnp.broadcast_to(column[:, lane : lane + 1], (SUBLANES, LANES))
                out_ref[2 * at + half, i] = wide * row
        return carry

    lax.fori_loop(0, alpha_ref.shape[0], step, 0)


def factor_call(gammas, alphas):
    steps, pairs, _ = gammas.shape
    return pl.pallas_call(
        factor_kernel,
        out_shape=jax.ShapeDtypeStruct((steps, pairs, SUBLANES, LANES), jnp.float32),
        name="factors",
    )(gammas, alphas)


def degree_kernel(
    r_ref, beta_hi, beta_lo, even_ref, odd_ref, source_ref, out_ref, pow_ref,
    t_ref, c_ref, e_ref, held_ref, factor_ref, sems, factor_sems,
):
    sources, functions, held, _ = r_ref.shape
    count = held // SUBLANES
    spread = beta_hi.shape[0]
    blocks = spread // SUBLANES
    firsts = [block * (block + 1) // 2 for block in range(blocks)]

    def factor_copy(block):
        part = pl.ds(firsts[block], block + 1)
        return pltpu.make_async_copy(
            source_ref.at[part], factor_ref.at[part], factor_sems.at[block]
        )

    for block in range(blocks):
        factor_copy(block).start()
    for f in range(0, functions, 2):
        for n in range(SUBLANES):
            parts = [
                r_ref[:, f + i, n * count : (n + 1) * count, :].reshape(sources * count, LANES)
                for i in range(2)
            ]
            high, low = split_value(jnp.concatenate(parts, axis=1))
            even = jnp.concatenate([even_ref[n : n + 1, :]] * 2, axis=1)
            odd = jnp.concatenate([odd_ref[n : n + 1, :]] * 2, axis=1)
            high = jnp.concatenate([high * even, high * odd], axis=0)
            low = jnp.concatenate([low * even, low * odd], axis=0)
            turned = dot(beta_hi[...], high) + dot(beta_lo[...], high) + dot(beta_hi[...], low)
            for i in range(2):
                for b in range(blocks):
                    t_ref[f + i, pl.ds(b * SUBLANES * SUBLANES + n, SUBLANES, stride=SUBLANES), :] = (
                        turned[b * SUBLANES : (b + 1) * SUBLANES, i * LANES : (i + 1) * LANES]
                    )

    zero = jnp.zeros((SUBLANES, LANES), jnp.float32)

    def out_copy(block):
        part = (slice(None), slice(None), slice(None), pl.ds(block * SUBLANES, SUBLANES))
        return pltpu.make_async_copy(held_ref.at[part], out_ref.at[part], sems.at[block])

    for block in range(blocks):
        factor_copy(block).wait()

        def chunk_step(chunk, totals):
            totals = list(totals)
            for m in range(SUBLANES):
                row = pl.multiple_of((chunk * SUBLANES + m) * SUBLANES, SUBLANES)
                values = [t_ref[f, pl.ds(row, SUBLANES), :] for f in range(functions)]
                for j in range(SUBLANES):
                    factor = factor_ref[firsts[block] + chunk, j * SUBLANES + m]
                    for f in range(functions):
                        totals[j * functions + f] += factor * values[f]
            return tuple(totals)

        totals = lax.fori_loop(0, block + 1, chunk_step, (zero,) * (SUBLANES * functions))
        degrees = slice(block * SUBLANES, (block + 1) * SUBLANES)
        for f in range(functions):
            for j in range(SUBLANES):
                c_ref[f, pl.ds(j, SUBLANES, stride=SUBLANES), :] = totals[j * functions + f]
            energy = zero
            for n in range(SUBLANES):
                tile = c_ref[f, n * SUBLANES : (n + 1) * SUBLANES, :]
                energy += tile * tile
                held_ref[n, 0, f, degrees, :] = tile[:, :spread]
                held_ref[n, 1, f, degrees, :] = tile[:, spread:]
            e_ref[f, degrees, :] = energy
        out_copy(block).start()

    lane = lax.broadcasted_iota(jnp.int32, (SUBLANES, LANES), 1)
    fold = jnp.where(lane % spread == 0, 1.0, 2.0).astype(jnp.bfloat16)
    across = lambda part: lax.dot_general(
        fold, part, (((1,), (1,)), ((), ())), preferred_element_type=jnp.float32
    )
    place = lax.broadcasted_iota(jnp.int32, (SUBLANES, spread), 0)
    power = jnp.zeros((SUBLANES, spread), jnp.float32)
    for f in range(functions):
        high, low = split_value(e_ref[f])
        rest = e_ref[f] - high.astype(jnp.float32) - low.astype(jnp.float32)
        total = across(high) + across(low) + across(rest.astype(jnp.bfloat16))
        power = jnp.where(place == f, total, power)
    pow_ref[:, :spread] = power
    pow_ref[:, spread:] = jnp.zeros_like(power)

    for block in range(blocks):
        out_copy(block).wait()


def degree_call(received, factors, spread):
    functions = received.shape[1]
    tables = [*split_pair(beta_table(spread))]
    tables += [mask.astype(jnp.bfloat16) for mask in sign_masks(spread)]
    shape = (SUBLANES, 2, functions, spread, spread)
    vmem = pl.BlockSpec(memory_space=pltpu.VMEM)
    return pl.pallas_call(
        degree_kernel,
        in_specs=[vmem] * 5 + [pl.BlockSpec(memory_space=pl.ANY)],
        out_specs=[pl.BlockSpec(memory_space=pl.ANY), vmem],
        out_shape=[
            jax.ShapeDtypeStruct(shape, jnp.float32),
            jax.ShapeDtypeStruct((SUBLANES, LANES), jnp.float32),
        ],
        scratch_shapes=[
            pltpu.VMEM((functions, spread * SUBLANES, LANES), jnp.float32),
            pltpu.VMEM((functions, SUBLANES * SUBLANES, LANES), jnp.float32),
            pltpu.VMEM((functions, spread, LANES), jnp.float32),
            pltpu.VMEM(shape, jnp.float32),
            pltpu.VMEM(factors.shape, jnp.float32),
            pltpu.SemaphoreType.DMA((spread // SUBLANES,)),
            pltpu.SemaphoreType.DMA((spread // SUBLANES,)),
        ],
        compiler_params=pltpu.CompilerParams(vmem_limit_bytes=50 << 20),
        name="degrees",
    )(received, *tables, factors)


def fast_local(samples):
    devices = lax.axis_size("beta")
    device = lax.axis_index("beta")
    functions, grid_size = samples.shape[1:3]
    spread = grid_size // 2
    sent = spectrum_call(samples, devices)
    received = lax.all_to_all(sent, "beta", split_axis=0, concat_axis=0, tiled=True)
    gammas, alphas = quarter_tables(spread, devices)
    alphas = lax.dynamic_index_in_dim(jnp.asarray(alphas), device, 0, keepdims=False)
    factors = factor_call(jnp.asarray(gammas), alphas)
    coeffs, share = degree_call(received, factors, spread)
    shares = jnp.broadcast_to(share[None], (devices,) + share.shape)
    shares = lax.all_to_all(shares, "beta", split_axis=0, concat_axis=0, tiled=True)
    degrees = 2.0 * jnp.arange(spread, dtype=jnp.float32) + 1.0
    energy = jnp.sum(shares[:, :functions, :spread], axis=0)
    return coeffs, energy / (degrees * degrees)[None, :]


def local(samples):
    devices = lax.axis_size("beta")
    local_beta, functions, grid_size = samples.shape[:3]
    tiled = grid_size == LANES and local_beta == SUBLANES and grid_size == devices * SUBLANES
    if tiled and functions % 2 == 0:
        return fast_local(samples)
    return general_local(samples)


def solution(mesh):
    return jax.shard_map(
        local,
        mesh=mesh,
        in_specs=(P("beta", "grp", None, None),),
        out_specs=(P("beta", None, "grp", None, None), P("grp", None)),
        check_vma=False,
    )
```

```python
import math

import jax
import jax.numpy as jnp
import numpy as np
from jax import lax
from jax.experimental import pallas as pl
from jax.experimental.pallas import tpu as pltpu
from jax.sharding import PartitionSpec as P

HIGHEST = lax.Precision.HIGHEST
SUBLANES = 8
LANES = 128


def beta_angles(spread):
    grid_size = 2 * spread
    return (2.0 * jnp.arange(grid_size, dtype=jnp.float32) + 1.0) * (jnp.pi / (4.0 * spread))


def quadrature(spread):
    angles = beta_angles(spread)
    odd_terms = 2.0 * jnp.arange(spread, dtype=jnp.float32) + 1.0
    series = jnp.sum(jnp.sin(angles[:, None] * odd_terms[None, :]) / odd_terms[None, :], axis=1)
    return 2.0 / spread * jnp.sin(angles) * series


def gamma_table(spread):
    grid_size = 2 * spread
    positions = jnp.arange(grid_size, dtype=jnp.int32)
    orders = jnp.arange(spread, dtype=jnp.int32)
    phase_index = positions[:, None] * orders[None, :] % grid_size
    angles = phase_index.astype(jnp.float32) * (2.0 * jnp.pi / grid_size)
    return jnp.concatenate([jnp.cos(angles), -jnp.sin(angles)], axis=1)


def alpha_table(spread, row_index):
    grid_size = 2 * spread
    positions = jnp.arange(grid_size, dtype=jnp.int32)
    phase_index = row_index[:, None] * positions[None, :] % grid_size
    angles = phase_index.astype(jnp.float32) * (2.0 * jnp.pi / grid_size)
    cosine = jnp.cos(angles) / grid_size
    sine_part = jnp.sin(angles) / grid_size
    real_rows = jnp.stack([cosine, sine_part], axis=1)
    imag_rows = jnp.stack([-sine_part, cosine], axis=1)
    return jnp.stack([real_rows, imag_rows], axis=0)


def log_factorial(value, float_type):
    return lax.lgamma((value + 1).astype(float_type))


def wigner_start(alpha_order, gamma_order, log_cosine, log_sine):
    float_type = log_cosine.dtype
    lowest = jnp.maximum(jnp.abs(alpha_order), gamma_order)
    shift_low = jnp.maximum(0, gamma_order - alpha_order)
    magnitude = 0.5 * (
        log_factorial(lowest + alpha_order, float_type)
        + log_factorial(lowest - alpha_order, float_type)
        + log_factorial(lowest + gamma_order, float_type)
        + log_factorial(lowest - gamma_order, float_type)
    )
    magnitude = (
        magnitude
        - log_factorial(lowest + gamma_order - shift_low, float_type)
        - log_factorial(shift_low, float_type)
    )
    magnitude = magnitude - log_factorial(alpha_order - gamma_order + shift_low, float_type)
    magnitude = magnitude - log_factorial(lowest - alpha_order - shift_low, float_type)
    cos_power = (2 * lowest + gamma_order - alpha_order - 2 * shift_low).astype(float_type)
    sin_power = (alpha_order - gamma_order + 2 * shift_low).astype(float_type)
    parity = (alpha_order - gamma_order + shift_low) % 2
    sign_factor = (1 - 2 * parity).astype(float_type)
    return sign_factor * jnp.exp(magnitude + cos_power * log_cosine + sin_power * log_sine)


def advance(degree, carried, alpha_order, gamma_order, cos_angles, start_value, lowest):
    former, current = carried
    float_type = current.dtype
    previous = (degree - 1).astype(float_type)
    alpha_float = alpha_order.astype(float_type)
    gamma_float = gamma_order.astype(float_type)
    cross_ratio = alpha_float * gamma_float / jnp.maximum(previous * (previous + 1.0), 1.0)
    upper_term = ((previous + 1.0) * (previous + 1.0) - alpha_float * alpha_float) * (
        (previous + 1.0) * (previous + 1.0) - gamma_float * gamma_float
    )
    lower_term = (previous * previous - alpha_float * alpha_float) * (
        previous * previous - gamma_float * gamma_float
    )
    root_upper = jnp.sqrt(jnp.maximum(upper_term, 1.0))
    forward = (previous + 1.0) * (2.0 * previous + 1.0) / root_upper
    backward = (
        (previous + 1.0)
        * jnp.sqrt(jnp.maximum(lower_term, 0.0))
        / (jnp.maximum(previous, 1.0) * root_upper)
    )
    recurred = forward * (cos_angles - cross_ratio) * current - backward * former
    renewed = jnp.where(degree == lowest, start_value, recurred)
    return (current, renewed)


def degree_rows(row_index, weighted, spread):
    stride = 8
    grid_size = 2 * spread
    group_size = row_index.shape[0]
    channels = weighted.shape[2]
    block_count = spread // stride
    alpha_order = jnp.where(row_index < spread, row_index, row_index - grid_size)[:, None, None]
    gamma_order = jnp.arange(spread, dtype=jnp.int32)[None, None, :]
    angles = beta_angles(spread)
    cos_angles = jnp.cos(angles)[None, :, None]
    log_cosine = jnp.log(jnp.cos(0.5 * angles))[None, :, None]
    log_sine = jnp.log(jnp.sin(0.5 * angles))[None, :, None]
    lowest = jnp.maximum(jnp.abs(alpha_order), gamma_order)
    start_value = wigner_start(alpha_order, gamma_order, log_cosine, log_sine)
    first_block = jnp.min(jnp.abs(alpha_order)) // stride
    empty_state = jnp.zeros((group_size, grid_size, spread), jnp.float32)

    def compute_block(operands):
        block_index, former, current = operands
        levels = []
        for offset in range(stride):
            former, current = advance(
                block_index * stride + offset,
                (former, current),
                alpha_order,
                gamma_order,
                cos_angles,
                start_value,
                lowest,
            )
            levels.append(current)
        stacked = jnp.stack(levels, axis=0)
        block_part = jnp.einsum("jgkq,kgcq->gcjq", stacked, weighted, precision=HIGHEST)
        return (former, current, block_part)

    def skip_block(operands):
        block_index, former, current = operands
        return (former, current, jnp.zeros((group_size, channels, stride, spread), jnp.float32))

    def block_step(carried, block_index):
        former, current = carried
        former, current, block_part = lax.cond(
            block_index >= first_block, compute_block, skip_block, (block_index, former, current)
        )
        return ((former, current), block_part)

    _, parts = lax.scan(
        block_step, (empty_state, empty_state), jnp.arange(block_count, dtype=jnp.int32)
    )
    output = jnp.transpose(parts, (1, 2, 0, 3, 4)).reshape(group_size, channels, spread, spread)
    degree_scale = 8.0 * jnp.sqrt(2.0 * jnp.arange(spread, dtype=jnp.float32) + 1.0)
    return output * degree_scale[None, None, :, None]


def degree_energy(coeffs, functions, spread):
    split_view = coeffs.reshape(coeffs.shape[0], 2, functions, spread, spread)
    multiplicity = jnp.where(jnp.arange(spread) == 0, 1.0, 2.0).astype(jnp.float32)
    energy_sum = jnp.sum(split_view * split_view * multiplicity, axis=(0, 1, 4))
    degrees = 2.0 * jnp.arange(spread, dtype=jnp.float32) + 1.0
    return energy_sum / (degrees * degrees)[None, :]


def general_local(samples):
    devices = lax.axis_size("beta")
    device = lax.axis_index("beta")
    local_beta = samples.shape[0]
    functions = samples.shape[1]
    grid_size = samples.shape[2]
    spread = grid_size // 2
    channels = 2 * functions
    row_count = grid_size // devices
    natural_rows = jnp.arange(grid_size, dtype=jnp.int32)
    halfway = jnp.einsum("kfag,gx->kfax", samples, gamma_table(spread), precision=HIGHEST)
    halfway = halfway.reshape(local_beta, functions, grid_size, 2, spread)
    spectrum = jnp.einsum(
        "kfacq,spca->kpsfq", halfway, alpha_table(spread, natural_rows), precision=HIGHEST
    )
    spectrum = spectrum.reshape(local_beta, grid_size, channels, spread)
    received = lax.all_to_all(spectrum, "beta", split_axis=1, concat_axis=0, tiled=True)
    weighted = received * quadrature(spread)[:, None, None, None]
    owned_rows = lax.dynamic_slice_in_dim(natural_rows, device * row_count, row_count)
    computed = degree_rows(owned_rows, weighted, spread)
    power_part = degree_energy(computed, functions, spread)
    coeffs = computed
    power = lax.psum(power_part, "beta")
    coeffs = coeffs.reshape(row_count, 2, functions, spread, spread)
    return (coeffs, power)


def wigner_quarter(spread):
    alpha = np.arange(1 - spread, spread)[:, None]
    gamma = np.arange(spread)[None, :]
    lowest = np.maximum(np.abs(alpha), gamma)
    shift = np.maximum(0, gamma - alpha)
    logs = np.array([math.lgamma(value + 1.0) for value in range(2 * spread)])
    magnitude = 0.5 * (
        logs[lowest + alpha] + logs[lowest - alpha] + logs[lowest + gamma] + logs[lowest - gamma]
    )
    magnitude = magnitude - logs[lowest + gamma - shift] - logs[shift]
    magnitude = magnitude - logs[alpha - gamma + shift] - logs[lowest - alpha - shift]
    sign = 1.0 - 2.0 * ((alpha - gamma + shift) % 2)
    first = sign * np.exp(magnitude - lowest * math.log(2.0))
    squares_a, squares_g = alpha.astype(np.float64) ** 2, gamma.astype(np.float64) ** 2
    former, current, levels = np.zeros(first.shape), np.zeros(first.shape), []
    for degree in range(spread):
        before = degree - 1.0
        upper = np.sqrt(np.maximum((degree**2 - squares_a) * (degree**2 - squares_g), 1.0))
        lower = np.sqrt(np.maximum((before**2 - squares_a) * (before**2 - squares_g), 0.0))
        cross = alpha * gamma / max(before * degree, 1.0)
        follow = degree * (2.0 * before + 1.0) / upper * -cross * current
        follow = follow - degree * lower / (max(before, 1.0) * upper) * former
        former, current = current, np.where(lowest == degree, first, follow)
        levels.append(current)
    return np.stack(levels)


def split_pair(table):
    high = np.asarray(table).astype(jnp.bfloat16)
    return high, (table - high.astype(np.float64)).astype(jnp.bfloat16)


def fourier_tables(spread):
    grid = 2 * spread
    at = np.arange(grid)
    phase = 2.0 * np.pi / grid * (at[:, None] * np.arange(spread)[None, :] % grid)
    cosine, sine = np.cos(phase), -np.sin(phase)
    gamma_part = np.concatenate([cosine, sine, sine, -cosine], axis=1)
    phase = 2.0 * np.pi / grid * (at[:, None] * at[None, :] % grid)
    alpha_part = np.concatenate([np.cos(phase), np.sin(phase)], axis=1) / grid
    return gamma_part, alpha_part


def beta_table(spread):
    angles = (2.0 * np.arange(2 * spread) + 1.0) * (np.pi / (4.0 * spread))
    odd = 2.0 * np.arange(spread) + 1.0
    series = np.sum(np.sin(angles[:, None] * odd[None, :]) / odd[None, :], axis=1)
    weight = 2.0 / spread * np.sin(angles) * series
    order = np.concatenate([np.arange(0, spread, 2), np.arange(1, spread, 2)])
    fold = np.where(order == 0, 1.0, 2.0)[:, None] * weight[None, :]
    turn = order[:, None] * angles[None, :]
    return np.concatenate([fold * np.cos(turn), fold * np.sin(turn)], axis=0)


def sign_masks(spread):
    step = (np.arange(SUBLANES)[:, None] - np.arange(spread)[None, :]) % 4
    even = np.where(step == 0, 1.0, np.where(step == 2, -1.0, 0.0))
    odd = np.where(step == 3, 1.0, np.where(step == 1, -1.0, 0.0))
    return np.concatenate([even, even], axis=1), np.concatenate([odd, odd], axis=1)


def block_steps(spread):
    blocks = spread // SUBLANES
    return [(block, chunk) for block in range(blocks) for chunk in range(block + 1)]


def quarter_tables(spread, devices):
    quarter = wigner_quarter(spread)
    rows = np.arange(2 * spread)
    orders = np.where(rows < spread, rows, rows - 2 * spread)
    by_row = quarter[:, np.maximum(orders, 1 - spread) + spread - 1, :]
    by_row = np.where((orders > -spread)[None, :, None], by_row, 0.0)
    by_row = by_row * (8.0 * np.sqrt(2.0 * np.arange(spread) + 1.0))[:, None, None]
    gammas, alphas = [], []
    for block, chunk in block_steps(spread):
        degrees = slice(block * SUBLANES, (block + 1) * SUBLANES)
        part = slice(chunk * SUBLANES, (chunk + 1) * SUBLANES)
        gammas.append(np.swapaxes(quarter[degrees, spread - 1 :, part], 1, 2).reshape(-1, LANES))
        table = np.swapaxes(by_row[degrees, :, part], 0, 1)
        alphas.append(table.reshape(devices, SUBLANES, SUBLANES * SUBLANES))
    alphas = np.stack(alphas, axis=1)
    alphas = np.concatenate([alphas[:, 0::2], alphas[:, 1::2]], axis=-1)
    return np.stack(gammas).astype(np.float32), alphas.astype(np.float32)


def split_value(value):
    high = value.astype(jnp.bfloat16)
    return high, (value - high.astype(jnp.float32)).astype(jnp.bfloat16)


def dot(left, right):
    return jnp.dot(left, right, preferred_element_type=jnp.float32)


def spectrum_kernel(x_ref, gamma_two, gamma_lo, alpha_two, out_ref):
    count, _, grid, _ = x_ref.shape
    blocks = out_ref.shape[0]
    high, low = split_value(x_ref[:, 0].reshape(count * grid, grid))
    half = dot(jnp.concatenate([high, low], axis=1), gamma_two[...]) + dot(high, gamma_lo[...])
    for k in range(0, count, 2):
        pairs = [half[(k + i) * grid : (k + i + 1) * grid] for i in range(2)]
        pair = jnp.concatenate(
            [
                jnp.concatenate([p[:, :LANES] for p in pairs], axis=1),
                jnp.concatenate([p[:, LANES:] for p in pairs], axis=1),
            ],
            axis=0,
        )
        high, low = split_value(pair)
        both = dot(alpha_two[...], high)
        rows = both[:grid] + both[grid:] + dot(alpha_two[:grid], low)
        for i in range(2):
            for d in range(blocks):
                out_ref[d, 0, pl.ds(k + i, SUBLANES, stride=count), :] = rows[
                    d * SUBLANES : (d + 1) * SUBLANES, i * LANES : (i + 1) * LANES
                ]


def spectrum_call(samples, devices):
    count, functions, grid, _ = samples.shape
    gamma_part, alpha_part = fourier_tables(grid // 2)
    gamma_hi, gamma_lo = split_pair(gamma_part)
    tables = [np.concatenate([gamma_hi, gamma_hi], axis=0), gamma_lo]
    tables.append(np.concatenate(split_pair(alpha_part), axis=0))
    rows = grid // devices * count
    whole = lambda table: pl.BlockSpec(table.shape, lambda f: (0, 0))
    return pl.pallas_call(
        spectrum_kernel,
        grid=(functions,),
        in_specs=[pl.BlockSpec((count, 1, grid, grid), lambda f: (0, f, 0, 0))]
        + [whole(table) for table in tables],
        out_specs=pl.BlockSpec((devices, 1, rows, LANES), lambda f: (0, f, 0, 0)),
        out_shape=jax.ShapeDtypeStruct((devices, functions, rows, LANES), jnp.float32),
        name="spectrum",
    )(samples, *tables)


def factor_kernel(gamma_ref, alpha_ref, out_ref):
    pairs = out_ref.shape[1]
    left = lax.broadcasted_iota(jnp.int32, (SUBLANES, LANES), 1) < LANES // 2

    def step(at, carry):
        column = alpha_ref[at]
        for half in range(2):
            for i in range(pairs):
                lane = 2 * (half * pairs + i)
                wide = [
                    jnp.broadcast_to(column[:, lane + j : lane + j + 1], (SUBLANES, LANES))
                    for j in range(2)
                ]
                row = gamma_ref[2 * at + half, pl.ds(i, SUBLANES, stride=0), :]
                out_ref[2 * at + half, i] = jnp.where(left, wide[0], wide[1]) * row
        return carry

    lax.fori_loop(0, alpha_ref.shape[0], step, 0)


def factor_call(gammas, alphas):
    steps, pairs, _ = gammas.shape
    return pl.pallas_call(
        factor_kernel,
        out_shape=jax.ShapeDtypeStruct((steps, pairs, SUBLANES, LANES), jnp.float32),
        name="factors",
    )(gammas, alphas)


def degree_kernel(
    r_ref, beta_two, even_ref, odd_ref, source_ref, out_ref, pow_ref,
    t_ref, c_ref, e_ref, held_ref, factor_ref, sems, factor_sems,
):
    sources, functions, held, _ = r_ref.shape
    count = held // SUBLANES
    spread = beta_two.shape[0] // 4
    blocks = spread // SUBLANES
    firsts = [block * (block + 1) // 2 for block in range(blocks)]

    def factor_copy(block):
        part = pl.ds(firsts[block], block + 1)
        return pltpu.make_async_copy(
            source_ref.at[part], factor_ref.at[part], factor_sems.at[block]
        )

    row = lax.axis_index("beta") * SUBLANES
    smallest = jnp.where(row < spread, row, 2 * spread - row - SUBLANES + 1)
    first_block = smallest // SUBLANES
    for block in range(blocks):

        @pl.when(block >= first_block)
        def _():
            factor_copy(block).start()

    left = lax.broadcasted_iota(jnp.int32, (spread // 2, LANES), 1) < spread
    for f in range(0, functions, 2):
        for n in range(SUBLANES):
            parts = [
                r_ref[:, f + i, n * count : (n + 1) * count, :].reshape(sources * count, LANES)
                for i in range(2)
            ]
            high, low = split_value(jnp.concatenate(parts, axis=1))
            both = dot(beta_two[...], jnp.concatenate([high, low], axis=0))
            both = both[: 2 * spread] + both[2 * spread :]
            turned = [
                jnp.where(
                    even_ref[n : n + 1] != 0.0,
                    both[:spread, i * LANES : (i + 1) * LANES] * even_ref[n : n + 1],
                    both[spread:, i * LANES : (i + 1) * LANES] * odd_ref[n : n + 1],
                )
                for i in range(2)
            ]
            for i in range(2):
                evens, odds = turned[i][: spread // 2], turned[i][spread // 2 :]
                parted = (
                    jnp.where(left, evens, pltpu.roll(odds, spread, 1)),
                    jnp.where(left, pltpu.roll(evens, spread, 1), odds),
                )
                for part in range(2):
                    for b in range(spread // (2 * SUBLANES)):
                        t_ref[
                            part, f + i, pl.ds(b * SUBLANES * SUBLANES + n, SUBLANES, stride=SUBLANES), :
                        ] = parted[part][b * SUBLANES : (b + 1) * SUBLANES]

    zero = jnp.zeros((SUBLANES, LANES), jnp.float32)

    def out_copy(block):
        part = (slice(None), slice(None), slice(None), pl.ds(block * SUBLANES, SUBLANES))
        return pltpu.make_async_copy(held_ref.at[part], out_ref.at[part], sems.at[block])

    def fill(block):
        degrees = slice(block * SUBLANES, (block + 1) * SUBLANES)
        empty = jnp.zeros((SUBLANES, 2, functions, SUBLANES, spread), jnp.float32)
        held_ref[:, :, :, degrees, :] = empty
        for f in range(functions):
            e_ref[f, degrees, :] = zero

    channels = [(part, f) for part in range(2) for f in range(functions)]
    some = SUBLANES // 2

    def work(block):
        factor_copy(block).wait()
        degrees = slice(block * SUBLANES, (block + 1) * SUBLANES)
        for half in range(2):
            totals = [[zero] * len(channels) for _ in range(some)]
            for chunk in range(block + 1):
                for i in range(SUBLANES // 2):
                    row = (chunk * SUBLANES // 2 + i) * SUBLANES
                    values = [t_ref[part, f, row : row + SUBLANES, :] for part, f in channels]
                    for j in range(some):
                        at = (half * some + j) * SUBLANES // 2 + i
                        factor = factor_ref[firsts[block] + chunk, at]
                        totals[j] = [t + factor * v for t, v in zip(totals[j], values)]
            for j in range(some):
                for (part, f), total in zip(channels, totals[j]):
                    c_ref[part, f, pl.ds(half * some + j, SUBLANES, stride=SUBLANES), :] = total
        for f in range(functions):
            energy = zero
            for part in range(2):
                for n in range(SUBLANES):
                    tile = c_ref[part, f, n * SUBLANES : (n + 1) * SUBLANES, :]
                    tile = tile + pltpu.roll(tile, spread, 1)
                    energy += tile * tile
                    held_ref[n, part, f, degrees, :] = tile[:, :spread]
            e_ref[f, degrees, :] = energy

    for block in range(blocks):
        pl.when(block < first_block)(lambda: fill(block))
        pl.when(block >= first_block)(lambda: work(block))
        out_copy(block).start()

    lane = lax.broadcasted_iota(jnp.int32, (SUBLANES, LANES), 1)
    fold = jnp.where(lane == 0, 1.0, jnp.where(lane < spread, 2.0, 0.0)).astype(jnp.bfloat16)
    across = lambda part: lax.dot_general(
        fold, part, (((1,), (1,)), ((), ())), preferred_element_type=jnp.float32
    )
    place = lax.broadcasted_iota(jnp.int32, (SUBLANES, spread), 0)
    power = jnp.zeros((SUBLANES, spread), jnp.float32)
    for f in range(functions):
        high, low = split_value(e_ref[f])
        rest = e_ref[f] - high.astype(jnp.float32) - low.astype(jnp.float32)
        total = across(high) + across(low) + across(rest.astype(jnp.bfloat16))
        power = jnp.where(place == f, total, power)
    power = jnp.concatenate([power, jnp.zeros_like(power)], axis=1)
    for d in range(pow_ref.shape[0]):
        pow_ref[d] = power

    for block in range(blocks):
        out_copy(block).wait()


def degree_call(received, factors, spread):
    functions = received.shape[1]
    high, low = split_pair(beta_table(spread))
    above = np.concatenate([high, high], axis=1)
    below = np.concatenate([low, np.zeros_like(low)], axis=1)
    tables = [np.concatenate([above, below], axis=0)]
    tables += [mask.astype(np.float32) for mask in sign_masks(spread)]
    shape = (SUBLANES, 2, functions, spread, spread)
    vmem = pl.BlockSpec(memory_space=pltpu.VMEM)
    return pl.pallas_call(
        degree_kernel,
        in_specs=[vmem] * 4 + [pl.BlockSpec(memory_space=pl.ANY)],
        out_specs=[pl.BlockSpec(memory_space=pl.ANY), vmem],
        out_shape=[
            jax.ShapeDtypeStruct(shape, jnp.float32),
            jax.ShapeDtypeStruct((received.shape[0], SUBLANES, LANES), jnp.float32),
        ],
        scratch_shapes=[
            pltpu.VMEM((2, functions, spread // 2 * SUBLANES, LANES), jnp.float32),
            pltpu.VMEM((2, functions, SUBLANES * SUBLANES, LANES), jnp.float32),
            pltpu.VMEM((functions, spread, LANES), jnp.float32),
            pltpu.VMEM(shape, jnp.float32),
            pltpu.VMEM(factors.shape, jnp.float32),
            pltpu.SemaphoreType.DMA((spread // SUBLANES,)),
            pltpu.SemaphoreType.DMA((spread // SUBLANES,)),
        ],
        compiler_params=pltpu.CompilerParams(vmem_limit_bytes=50 << 20),
        name="degrees",
    )(received, *tables, factors)


def fast_local(samples):
    devices = lax.axis_size("beta")
    device = lax.axis_index("beta")
    functions, grid_size = samples.shape[1:3]
    spread = grid_size // 2
    sent = spectrum_call(samples, devices)
    received = lax.all_to_all(sent, "beta", split_axis=0, concat_axis=0, tiled=True)
    gammas, alphas = quarter_tables(spread, devices)
    alphas = lax.dynamic_index_in_dim(jnp.asarray(alphas), device, 0, keepdims=False)
    factors = factor_call(jnp.asarray(gammas), alphas)
    coeffs, shares = degree_call(received, factors, spread)
    shares = lax.all_to_all(shares, "beta", split_axis=0, concat_axis=0, tiled=True)
    scale = (1.0 / (2.0 * np.arange(spread) + 1.0) ** 2).astype(np.float32)
    return coeffs, jnp.sum(shares[:, :functions, :spread], axis=0) * scale[None, :]


def local(samples):
    devices = lax.axis_size("beta")
    local_beta, functions, grid_size = samples.shape[:3]
    tiled = grid_size == LANES and local_beta == SUBLANES and grid_size == devices * SUBLANES
    if tiled and functions % 2 == 0:
        return fast_local(samples)
    return general_local(samples)


def solution(mesh):
    return jax.shard_map(
        local,
        mesh=mesh,
        in_specs=(P("beta", "grp", None, None),),
        out_specs=(P("beta", None, "grp", None, None), P("grp", None)),
        check_vma=False,
    )
```

```python
import math

import jax
import jax.numpy as jnp
import numpy as np
from jax import lax
from jax.experimental import pallas as pl
from jax.experimental.pallas import tpu as pltpu
from jax.sharding import PartitionSpec as P

HIGHEST = lax.Precision.HIGHEST
SUBLANES = 8
LANES = 128


def beta_angles(spread):
    grid_size = 2 * spread
    return (2.0 * jnp.arange(grid_size, dtype=jnp.float32) + 1.0) * (jnp.pi / (4.0 * spread))


def quadrature(spread):
    angles = beta_angles(spread)
    odd_terms = 2.0 * jnp.arange(spread, dtype=jnp.float32) + 1.0
    series = jnp.sum(jnp.sin(angles[:, None] * odd_terms[None, :]) / odd_terms[None, :], axis=1)
    return 2.0 / spread * jnp.sin(angles) * series


def gamma_table(spread):
    grid_size = 2 * spread
    positions = jnp.arange(grid_size, dtype=jnp.int32)
    orders = jnp.arange(spread, dtype=jnp.int32)
    phase_index = positions[:, None] * orders[None, :] % grid_size
    angles = phase_index.astype(jnp.float32) * (2.0 * jnp.pi / grid_size)
    return jnp.concatenate([jnp.cos(angles), -jnp.sin(angles)], axis=1)


def alpha_table(spread, row_index):
    grid_size = 2 * spread
    positions = jnp.arange(grid_size, dtype=jnp.int32)
    phase_index = row_index[:, None] * positions[None, :] % grid_size
    angles = phase_index.astype(jnp.float32) * (2.0 * jnp.pi / grid_size)
    cosine = jnp.cos(angles) / grid_size
    sine_part = jnp.sin(angles) / grid_size
    real_rows = jnp.stack([cosine, sine_part], axis=1)
    imag_rows = jnp.stack([-sine_part, cosine], axis=1)
    return jnp.stack([real_rows, imag_rows], axis=0)


def log_factorial(value, float_type):
    return lax.lgamma((value + 1).astype(float_type))


def wigner_start(alpha_order, gamma_order, log_cosine, log_sine):
    float_type = log_cosine.dtype
    lowest = jnp.maximum(jnp.abs(alpha_order), gamma_order)
    shift_low = jnp.maximum(0, gamma_order - alpha_order)
    magnitude = 0.5 * (
        log_factorial(lowest + alpha_order, float_type)
        + log_factorial(lowest - alpha_order, float_type)
        + log_factorial(lowest + gamma_order, float_type)
        + log_factorial(lowest - gamma_order, float_type)
    )
    magnitude = (
        magnitude
        - log_factorial(lowest + gamma_order - shift_low, float_type)
        - log_factorial(shift_low, float_type)
    )
    magnitude = magnitude - log_factorial(alpha_order - gamma_order + shift_low, float_type)
    magnitude = magnitude - log_factorial(lowest - alpha_order - shift_low, float_type)
    cos_power = (2 * lowest + gamma_order - alpha_order - 2 * shift_low).astype(float_type)
    sin_power = (alpha_order - gamma_order + 2 * shift_low).astype(float_type)
    parity = (alpha_order - gamma_order + shift_low) % 2
    sign_factor = (1 - 2 * parity).astype(float_type)
    return sign_factor * jnp.exp(magnitude + cos_power * log_cosine + sin_power * log_sine)


def advance(degree, carried, alpha_order, gamma_order, cos_angles, start_value, lowest):
    former, current = carried
    float_type = current.dtype
    previous = (degree - 1).astype(float_type)
    alpha_float = alpha_order.astype(float_type)
    gamma_float = gamma_order.astype(float_type)
    cross_ratio = alpha_float * gamma_float / jnp.maximum(previous * (previous + 1.0), 1.0)
    upper_term = ((previous + 1.0) * (previous + 1.0) - alpha_float * alpha_float) * (
        (previous + 1.0) * (previous + 1.0) - gamma_float * gamma_float
    )
    lower_term = (previous * previous - alpha_float * alpha_float) * (
        previous * previous - gamma_float * gamma_float
    )
    root_upper = jnp.sqrt(jnp.maximum(upper_term, 1.0))
    forward = (previous + 1.0) * (2.0 * previous + 1.0) / root_upper
    backward = (
        (previous + 1.0)
        * jnp.sqrt(jnp.maximum(lower_term, 0.0))
        / (jnp.maximum(previous, 1.0) * root_upper)
    )
    recurred = forward * (cos_angles - cross_ratio) * current - backward * former
    renewed = jnp.where(degree == lowest, start_value, recurred)
    return (current, renewed)


def degree_rows(row_index, weighted, spread):
    stride = 8
    grid_size = 2 * spread
    group_size = row_index.shape[0]
    channels = weighted.shape[2]
    block_count = spread // stride
    alpha_order = jnp.where(row_index < spread, row_index, row_index - grid_size)[:, None, None]
    gamma_order = jnp.arange(spread, dtype=jnp.int32)[None, None, :]
    angles = beta_angles(spread)
    cos_angles = jnp.cos(angles)[None, :, None]
    log_cosine = jnp.log(jnp.cos(0.5 * angles))[None, :, None]
    log_sine = jnp.log(jnp.sin(0.5 * angles))[None, :, None]
    lowest = jnp.maximum(jnp.abs(alpha_order), gamma_order)
    start_value = wigner_start(alpha_order, gamma_order, log_cosine, log_sine)
    first_block = jnp.min(jnp.abs(alpha_order)) // stride
    empty_state = jnp.zeros((group_size, grid_size, spread), jnp.float32)

    def compute_block(operands):
        block_index, former, current = operands
        levels = []
        for offset in range(stride):
            former, current = advance(
                block_index * stride + offset,
                (former, current),
                alpha_order,
                gamma_order,
                cos_angles,
                start_value,
                lowest,
            )
            levels.append(current)
        stacked = jnp.stack(levels, axis=0)
        block_part = jnp.einsum("jgkq,kgcq->gcjq", stacked, weighted, precision=HIGHEST)
        return (former, current, block_part)

    def skip_block(operands):
        block_index, former, current = operands
        return (former, current, jnp.zeros((group_size, channels, stride, spread), jnp.float32))

    def block_step(carried, block_index):
        former, current = carried
        former, current, block_part = lax.cond(
            block_index >= first_block, compute_block, skip_block, (block_index, former, current)
        )
        return ((former, current), block_part)

    _, parts = lax.scan(
        block_step, (empty_state, empty_state), jnp.arange(block_count, dtype=jnp.int32)
    )
    output = jnp.transpose(parts, (1, 2, 0, 3, 4)).reshape(group_size, channels, spread, spread)
    degree_scale = 8.0 * jnp.sqrt(2.0 * jnp.arange(spread, dtype=jnp.float32) + 1.0)
    return output * degree_scale[None, None, :, None]


def degree_energy(coeffs, functions, spread):
    split_view = coeffs.reshape(coeffs.shape[0], 2, functions, spread, spread)
    multiplicity = jnp.where(jnp.arange(spread) == 0, 1.0, 2.0).astype(jnp.float32)
    energy_sum = jnp.sum(split_view * split_view * multiplicity, axis=(0, 1, 4))
    degrees = 2.0 * jnp.arange(spread, dtype=jnp.float32) + 1.0
    return energy_sum / (degrees * degrees)[None, :]


def general_local(samples):
    devices = lax.axis_size("beta")
    device = lax.axis_index("beta")
    local_beta = samples.shape[0]
    functions = samples.shape[1]
    grid_size = samples.shape[2]
    spread = grid_size // 2
    channels = 2 * functions
    row_count = grid_size // devices
    natural_rows = jnp.arange(grid_size, dtype=jnp.int32)
    halfway = jnp.einsum("kfag,gx->kfax", samples, gamma_table(spread), precision=HIGHEST)
    halfway = halfway.reshape(local_beta, functions, grid_size, 2, spread)
    spectrum = jnp.einsum(
        "kfacq,spca->kpsfq", halfway, alpha_table(spread, natural_rows), precision=HIGHEST
    )
    spectrum = spectrum.reshape(local_beta, grid_size, channels, spread)
    received = lax.all_to_all(spectrum, "beta", split_axis=1, concat_axis=0, tiled=True)
    weighted = received * quadrature(spread)[:, None, None, None]
    owned_rows = lax.dynamic_slice_in_dim(natural_rows, device * row_count, row_count)
    computed = degree_rows(owned_rows, weighted, spread)
    power_part = degree_energy(computed, functions, spread)
    coeffs = computed
    power = lax.psum(power_part, "beta")
    coeffs = coeffs.reshape(row_count, 2, functions, spread, spread)
    return (coeffs, power)


def wigner_quarter(spread):
    alpha = np.arange(1 - spread, spread)[:, None]
    gamma = np.arange(spread)[None, :]
    lowest = np.maximum(np.abs(alpha), gamma)
    shift = np.maximum(0, gamma - alpha)
    logs = np.array([math.lgamma(value + 1.0) for value in range(2 * spread)])
    magnitude = 0.5 * (
        logs[lowest + alpha] + logs[lowest - alpha] + logs[lowest + gamma] + logs[lowest - gamma]
    )
    magnitude = magnitude - logs[lowest + gamma - shift] - logs[shift]
    magnitude = magnitude - logs[alpha - gamma + shift] - logs[lowest - alpha - shift]
    sign = 1.0 - 2.0 * ((alpha - gamma + shift) % 2)
    first = sign * np.exp(magnitude - lowest * math.log(2.0))
    squares_a, squares_g = alpha.astype(np.float64) ** 2, gamma.astype(np.float64) ** 2
    former, current, levels = np.zeros(first.shape), np.zeros(first.shape), []
    for degree in range(spread):
        before = degree - 1.0
        upper = np.sqrt(np.maximum((degree**2 - squares_a) * (degree**2 - squares_g), 1.0))
        lower = np.sqrt(np.maximum((before**2 - squares_a) * (before**2 - squares_g), 0.0))
        cross = alpha * gamma / max(before * degree, 1.0)
        follow = degree * (2.0 * before + 1.0) / upper * -cross * current
        follow = follow - degree * lower / (max(before, 1.0) * upper) * former
        former, current = current, np.where(lowest == degree, first, follow)
        levels.append(current)
    return np.stack(levels)


def split_pair(table):
    high = np.asarray(table).astype(jnp.bfloat16)
    return high, (table - high.astype(np.float64)).astype(jnp.bfloat16)


def fourier_tables(spread):
    grid = 2 * spread
    at = np.arange(grid)
    phase = 2.0 * np.pi / grid * (at[:, None] * np.arange(spread)[None, :] % grid)
    cosine, sine = np.cos(phase), -np.sin(phase)
    gamma_part = np.concatenate([cosine, sine, sine, -cosine], axis=1)
    phase = 2.0 * np.pi / grid * (at[:, None] * at[None, :] % grid)
    alpha_part = np.concatenate([np.cos(phase), np.sin(phase)], axis=1) / grid
    return gamma_part, alpha_part


def beta_table(spread):
    angles = (2.0 * np.arange(2 * spread) + 1.0) * (np.pi / (4.0 * spread))
    odd = 2.0 * np.arange(spread) + 1.0
    series = np.sum(np.sin(angles[:, None] * odd[None, :]) / odd[None, :], axis=1)
    weight = 2.0 / spread * np.sin(angles) * series
    order = np.concatenate([np.arange(0, spread, 2), np.arange(1, spread, 2)])
    fold = np.where(order == 0, 1.0, 2.0)[:, None] * weight[None, :]
    turn = order[:, None] * angles[None, :]
    return np.concatenate([fold * np.cos(turn), fold * np.sin(turn)], axis=0)


def sign_masks(spread):
    step = (np.arange(SUBLANES)[:, None] - np.arange(spread)[None, :]) % 4
    even = np.where(step == 0, 1.0, np.where(step == 2, -1.0, 0.0))
    odd = np.where(step == 3, 1.0, np.where(step == 1, -1.0, 0.0))
    return np.concatenate([even, even], axis=1), np.concatenate([odd, odd], axis=1)


def block_steps(spread):
    blocks = spread // SUBLANES
    return [(block, chunk) for block in range(blocks) for chunk in range(block + 1)]


def quarter_tables(spread, devices):
    quarter = wigner_quarter(spread)
    rows = np.arange(2 * spread)
    orders = np.where(rows < spread, rows, rows - 2 * spread)
    by_row = quarter[:, np.maximum(orders, 1 - spread) + spread - 1, :]
    by_row = np.where((orders > -spread)[None, :, None], by_row, 0.0)
    by_row = by_row * (8.0 * np.sqrt(2.0 * np.arange(spread) + 1.0))[:, None, None]
    gammas, alphas = [], []
    for block, chunk in block_steps(spread):
        degrees = slice(block * SUBLANES, (block + 1) * SUBLANES)
        part = slice(chunk * SUBLANES, (chunk + 1) * SUBLANES)
        gammas.append(np.swapaxes(quarter[degrees, spread - 1 :, part], 1, 2).reshape(-1, LANES))
        table = np.swapaxes(by_row[degrees, :, part], 0, 1)
        alphas.append(table.reshape(devices, SUBLANES, SUBLANES * SUBLANES))
    alphas = np.stack(alphas, axis=1)
    alphas = np.concatenate([alphas[:, 0::2], alphas[:, 1::2]], axis=-1)
    return np.stack(gammas).astype(np.float32), alphas.astype(np.float32)


def split_value(value):
    high = value.astype(jnp.bfloat16)
    return high, (value - high.astype(jnp.float32)).astype(jnp.bfloat16)


def dot(left, right):
    return jnp.dot(left, right, preferred_element_type=jnp.float32)


def spectrum_kernel(x_ref, gamma_two, gamma_lo, alpha_two, out_ref):
    count, _, grid, _ = x_ref.shape
    blocks = out_ref.shape[0]
    high, low = split_value(x_ref[:, 0].reshape(count * grid, grid))
    half = dot(jnp.concatenate([high, low], axis=1), gamma_two[...]) + dot(high, gamma_lo[...])
    for k in range(0, count, 2):
        pairs = [half[(k + i) * grid : (k + i + 1) * grid] for i in range(2)]
        pair = jnp.concatenate(
            [
                jnp.concatenate([p[:, :LANES] for p in pairs], axis=1),
                jnp.concatenate([p[:, LANES:] for p in pairs], axis=1),
            ],
            axis=0,
        )
        high, low = split_value(pair)
        both = dot(alpha_two[...], high)
        rows = both[:grid] + both[grid:] + dot(alpha_two[:grid], low)
        for i in range(2):
            for d in range(blocks):
                out_ref[d, 0, pl.ds(k + i, SUBLANES, stride=count), :] = rows[
                    d * SUBLANES : (d + 1) * SUBLANES, i * LANES : (i + 1) * LANES
                ]


def spectrum_call(samples, devices):
    count, functions, grid, _ = samples.shape
    gamma_part, alpha_part = fourier_tables(grid // 2)
    gamma_hi, gamma_lo = split_pair(gamma_part)
    tables = [np.concatenate([gamma_hi, gamma_hi], axis=0), gamma_lo]
    tables.append(np.concatenate(split_pair(alpha_part), axis=0))
    rows = grid // devices * count
    whole = lambda table: pl.BlockSpec(table.shape, lambda f: (0, 0))
    return pl.pallas_call(
        spectrum_kernel,
        grid=(functions,),
        in_specs=[pl.BlockSpec((count, 1, grid, grid), lambda f: (0, f, 0, 0))]
        + [whole(table) for table in tables],
        out_specs=pl.BlockSpec((devices, 1, rows, LANES), lambda f: (0, f, 0, 0)),
        out_shape=jax.ShapeDtypeStruct((devices, functions, rows, LANES), jnp.float32),
        name="spectrum",
    )(samples, *tables)


def factor_kernel(gamma_ref, alpha_ref, out_ref):
    pairs = out_ref.shape[1]
    left = lax.broadcasted_iota(jnp.int32, (SUBLANES, LANES), 1) < LANES // 2

    def step(at, carry):
        column = alpha_ref[at]
        for half in range(2):
            for i in range(pairs):
                lane = 2 * (half * pairs + i)
                wide = [
                    jnp.broadcast_to(column[:, lane + j : lane + j + 1], (SUBLANES, LANES))
                    for j in range(2)
                ]
                row = gamma_ref[2 * at + half, pl.ds(i, SUBLANES, stride=0), :]
                out_ref[2 * at + half, i] = jnp.where(left, wide[0], wide[1]) * row
        return carry

    lax.fori_loop(0, alpha_ref.shape[0], step, 0)


def factor_call(gammas, alphas):
    steps, pairs, _ = gammas.shape
    return pl.pallas_call(
        factor_kernel,
        out_shape=jax.ShapeDtypeStruct((steps, pairs, SUBLANES, LANES), jnp.float32),
        name="factors",
    )(gammas, alphas)


def degree_kernel(
    r_ref, beta_two, even_ref, odd_ref, source_ref, out_ref, pow_ref,
    t_ref, c_ref, e_ref, held_ref, factor_ref, sems, factor_sems,
):
    sources, functions, held, _ = r_ref.shape
    count = held // SUBLANES
    spread = beta_two.shape[0] // 4
    blocks = spread // SUBLANES
    firsts = [block * (block + 1) // 2 for block in range(blocks)]

    def factor_copy(block):
        part = pl.ds(firsts[block], block + 1)
        return pltpu.make_async_copy(
            source_ref.at[part], factor_ref.at[part], factor_sems.at[block]
        )

    row = lax.axis_index("beta") * SUBLANES
    smallest = jnp.where(row < spread, row, 2 * spread - row - SUBLANES + 1)
    first_block = smallest // SUBLANES
    for block in range(blocks):

        @pl.when(block >= first_block)
        def _():
            factor_copy(block).start()

    left = lax.broadcasted_iota(jnp.int32, (spread // 2, LANES), 1) < spread
    for f in range(0, functions, 2):
        for n in range(SUBLANES):
            parts = [
                r_ref[:, f + i, n * count : (n + 1) * count, :].reshape(sources * count, LANES)
                for i in range(2)
            ]
            high, low = split_value(jnp.concatenate(parts, axis=1))
            both = dot(beta_two[...], jnp.concatenate([high, low], axis=0))
            both = both[: 2 * spread] + both[2 * spread :]
            turned = [
                jnp.where(
                    even_ref[n : n + 1] != 0.0,
                    both[:spread, i * LANES : (i + 1) * LANES] * even_ref[n : n + 1],
                    both[spread:, i * LANES : (i + 1) * LANES] * odd_ref[n : n + 1],
                )
                for i in range(2)
            ]
            for i in range(2):
                evens, odds = turned[i][: spread // 2], turned[i][spread // 2 :]
                parted = (
                    jnp.where(left, evens, pltpu.roll(odds, spread, 1)),
                    jnp.where(left, pltpu.roll(evens, spread, 1), odds),
                )
                for part in range(2):
                    for b in range(spread // (2 * SUBLANES)):
                        t_ref[
                            part, f + i, pl.ds(b * SUBLANES * SUBLANES + n, SUBLANES, stride=SUBLANES), :
                        ] = parted[part][b * SUBLANES : (b + 1) * SUBLANES]

    zero = jnp.zeros((SUBLANES, LANES), jnp.float32)

    def out_copy(block):
        part = (slice(None), slice(None), slice(None), pl.ds(block * SUBLANES, SUBLANES))
        return pltpu.make_async_copy(held_ref.at[part], out_ref.at[part], sems.at[block])

    def fill(block):
        degrees = slice(block * SUBLANES, (block + 1) * SUBLANES)
        empty = jnp.zeros((SUBLANES, 2, functions, SUBLANES, spread), jnp.float32)
        held_ref[:, :, :, degrees, :] = empty
        for f in range(functions):
            e_ref[f, degrees, :] = zero

    channels = [(part, f) for part in range(2) for f in range(functions)]
    some = SUBLANES // 2

    def work(block):
        factor_copy(block).wait()
        degrees = slice(block * SUBLANES, (block + 1) * SUBLANES)
        for half in range(2):
            totals = [[zero] * len(channels) for _ in range(some)]
            for chunk in range(block + 1):
                for i in range(SUBLANES // 2):
                    row = (chunk * SUBLANES // 2 + i) * SUBLANES
                    values = [t_ref[part, f, row : row + SUBLANES, :] for part, f in channels]
                    for j in range(some):
                        at = (half * some + j) * SUBLANES // 2 + i
                        factor = factor_ref[firsts[block] + chunk, at]
                        totals[j] = [t + factor * v for t, v in zip(totals[j], values)]
            for j in range(some):
                for (part, f), total in zip(channels, totals[j]):
                    c_ref[part, f, pl.ds(half * some + j, SUBLANES, stride=SUBLANES), :] = total
        for f in range(functions):
            energy = zero
            for part in range(2):
                for n in range(SUBLANES):
                    tile = c_ref[part, f, n * SUBLANES : (n + 1) * SUBLANES, :]
                    tile = tile + pltpu.roll(tile, spread, 1)
                    energy += tile * tile
                    held_ref[n, part, f, degrees, :] = tile[:, :spread]
            e_ref[f, degrees, :] = energy

    for block in range(blocks):
        pl.when(block < first_block)(lambda: fill(block))
        pl.when(block >= first_block)(lambda: work(block))
        out_copy(block).start()

    lane = lax.broadcasted_iota(jnp.int32, (SUBLANES, LANES), 1)
    fold = jnp.where(lane == 0, 1.0, jnp.where(lane < spread, 2.0, 0.0)).astype(jnp.bfloat16)
    across = lambda part: lax.dot_general(
        fold, part, (((1,), (1,)), ((), ())), preferred_element_type=jnp.float32
    )
    place = lax.broadcasted_iota(jnp.int32, (SUBLANES, spread), 0)
    power = jnp.zeros((SUBLANES, spread), jnp.float32)
    for f in range(functions):
        high, low = split_value(e_ref[f])
        rest = e_ref[f] - high.astype(jnp.float32) - low.astype(jnp.float32)
        total = across(high) + across(low) + across(rest.astype(jnp.bfloat16))
        power = jnp.where(place == f, total, power)
    power = jnp.concatenate([power, jnp.zeros_like(power)], axis=1)
    for d in range(pow_ref.shape[0]):
        pow_ref[d] = power

    for block in range(blocks):
        out_copy(block).wait()


def degree_call(received, factors, spread):
    functions = received.shape[1]
    high, low = split_pair(beta_table(spread))
    above = np.concatenate([high, high], axis=1)
    below = np.concatenate([low, np.zeros_like(low)], axis=1)
    tables = [np.concatenate([above, below], axis=0)]
    tables += [mask.astype(np.float32) for mask in sign_masks(spread)]
    shape = (SUBLANES, 2, functions, spread, spread)
    vmem = pl.BlockSpec(memory_space=pltpu.VMEM)
    return pl.pallas_call(
        degree_kernel,
        in_specs=[vmem] * 4 + [pl.BlockSpec(memory_space=pl.ANY)],
        out_specs=[pl.BlockSpec(memory_space=pl.ANY), vmem],
        out_shape=[
            jax.ShapeDtypeStruct(shape, jnp.float32),
            jax.ShapeDtypeStruct((received.shape[0], SUBLANES, LANES), jnp.float32),
        ],
        scratch_shapes=[
            pltpu.VMEM((2, functions, spread // 2 * SUBLANES, LANES), jnp.float32),
            pltpu.VMEM((2, functions, SUBLANES * SUBLANES, LANES), jnp.float32),
            pltpu.VMEM((functions, spread, LANES), jnp.float32),
            pltpu.VMEM(shape, jnp.float32),
            pltpu.VMEM(factors.shape, jnp.float32),
            pltpu.SemaphoreType.DMA((spread // SUBLANES,)),
            pltpu.SemaphoreType.DMA((spread // SUBLANES,)),
        ],
        compiler_params=pltpu.CompilerParams(vmem_limit_bytes=50 << 20),
        name="degrees",
    )(received, *tables, factors)


def fast_local(samples):
    devices = lax.axis_size("beta")
    device = lax.axis_index("beta")
    functions, grid_size = samples.shape[1:3]
    spread = grid_size // 2
    sent = spectrum_call(samples, devices)
    received = lax.all_to_all(sent, "beta", split_axis=0, concat_axis=0, tiled=True)
    gammas, alphas = quarter_tables(spread, devices)
    alphas = lax.dynamic_index_in_dim(jnp.asarray(alphas), device, 0, keepdims=False)
    factors = factor_call(jnp.asarray(gammas), alphas)
    coeffs, shares = degree_call(received, factors, spread)
    order = list(range(devices))[::-1]
    shares = lax.all_to_all(
        shares, "beta", split_axis=0, concat_axis=0, tiled=True, axis_index_groups=[order]
    )
    scale = (1.0 / (2.0 * np.arange(spread) + 1.0) ** 2).astype(np.float32)
    return coeffs, jnp.sum(shares[:, :functions, :spread], axis=0) * scale[None, :]


def local(samples):
    devices = lax.axis_size("beta")
    local_beta, functions, grid_size = samples.shape[:3]
    tiled = grid_size == LANES and local_beta == SUBLANES and grid_size == devices * SUBLANES
    if tiled and functions % 2 == 0:
        return fast_local(samples)
    return general_local(samples)


def solution(mesh):
    return jax.shard_map(
        local,
        mesh=mesh,
        in_specs=(P("beta", "grp", None, None),),
        out_specs=(P("beta", None, "grp", None, None), P("grp", None)),
        check_vma=False,
    )
```

```python
import math

import jax
import jax.numpy as jnp
import numpy as np
from jax import lax
from jax.experimental import pallas as pl
from jax.experimental.pallas import tpu as pltpu
from jax.sharding import PartitionSpec as P

HIGHEST = lax.Precision.HIGHEST
SUBLANES = 8
LANES = 128


def beta_angles(spread):
    grid_size = 2 * spread
    return (2.0 * jnp.arange(grid_size, dtype=jnp.float32) + 1.0) * (jnp.pi / (4.0 * spread))


def quadrature(spread):
    angles = beta_angles(spread)
    odd_terms = 2.0 * jnp.arange(spread, dtype=jnp.float32) + 1.0
    series = jnp.sum(jnp.sin(angles[:, None] * odd_terms[None, :]) / odd_terms[None, :], axis=1)
    return 2.0 / spread * jnp.sin(angles) * series


def gamma_table(spread):
    grid_size = 2 * spread
    positions = jnp.arange(grid_size, dtype=jnp.int32)
    orders = jnp.arange(spread, dtype=jnp.int32)
    phase_index = positions[:, None] * orders[None, :] % grid_size
    angles = phase_index.astype(jnp.float32) * (2.0 * jnp.pi / grid_size)
    return jnp.concatenate([jnp.cos(angles), -jnp.sin(angles)], axis=1)


def alpha_table(spread, row_index):
    grid_size = 2 * spread
    positions = jnp.arange(grid_size, dtype=jnp.int32)
    phase_index = row_index[:, None] * positions[None, :] % grid_size
    angles = phase_index.astype(jnp.float32) * (2.0 * jnp.pi / grid_size)
    cosine = jnp.cos(angles) / grid_size
    sine_part = jnp.sin(angles) / grid_size
    real_rows = jnp.stack([cosine, sine_part], axis=1)
    imag_rows = jnp.stack([-sine_part, cosine], axis=1)
    return jnp.stack([real_rows, imag_rows], axis=0)


def log_factorial(value, float_type):
    return lax.lgamma((value + 1).astype(float_type))


def wigner_start(alpha_order, gamma_order, log_cosine, log_sine):
    float_type = log_cosine.dtype
    lowest = jnp.maximum(jnp.abs(alpha_order), gamma_order)
    shift_low = jnp.maximum(0, gamma_order - alpha_order)
    magnitude = 0.5 * (
        log_factorial(lowest + alpha_order, float_type)
        + log_factorial(lowest - alpha_order, float_type)
        + log_factorial(lowest + gamma_order, float_type)
        + log_factorial(lowest - gamma_order, float_type)
    )
    magnitude = (
        magnitude
        - log_factorial(lowest + gamma_order - shift_low, float_type)
        - log_factorial(shift_low, float_type)
    )
    magnitude = magnitude - log_factorial(alpha_order - gamma_order + shift_low, float_type)
    magnitude = magnitude - log_factorial(lowest - alpha_order - shift_low, float_type)
    cos_power = (2 * lowest + gamma_order - alpha_order - 2 * shift_low).astype(float_type)
    sin_power = (alpha_order - gamma_order + 2 * shift_low).astype(float_type)
    parity = (alpha_order - gamma_order + shift_low) % 2
    sign_factor = (1 - 2 * parity).astype(float_type)
    return sign_factor * jnp.exp(magnitude + cos_power * log_cosine + sin_power * log_sine)


def advance(degree, carried, alpha_order, gamma_order, cos_angles, start_value, lowest):
    former, current = carried
    float_type = current.dtype
    previous = (degree - 1).astype(float_type)
    alpha_float = alpha_order.astype(float_type)
    gamma_float = gamma_order.astype(float_type)
    cross_ratio = alpha_float * gamma_float / jnp.maximum(previous * (previous + 1.0), 1.0)
    upper_term = ((previous + 1.0) * (previous + 1.0) - alpha_float * alpha_float) * (
        (previous + 1.0) * (previous + 1.0) - gamma_float * gamma_float
    )
    lower_term = (previous * previous - alpha_float * alpha_float) * (
        previous * previous - gamma_float * gamma_float
    )
    root_upper = jnp.sqrt(jnp.maximum(upper_term, 1.0))
    forward = (previous + 1.0) * (2.0 * previous + 1.0) / root_upper
    backward = (
        (previous + 1.0)
        * jnp.sqrt(jnp.maximum(lower_term, 0.0))
        / (jnp.maximum(previous, 1.0) * root_upper)
    )
    recurred = forward * (cos_angles - cross_ratio) * current - backward * former
    renewed = jnp.where(degree == lowest, start_value, recurred)
    return (current, renewed)


def degree_rows(row_index, weighted, spread):
    stride = 8
    grid_size = 2 * spread
    group_size = row_index.shape[0]
    channels = weighted.shape[2]
    block_count = spread // stride
    alpha_order = jnp.where(row_index < spread, row_index, row_index - grid_size)[:, None, None]
    gamma_order = jnp.arange(spread, dtype=jnp.int32)[None, None, :]
    angles = beta_angles(spread)
    cos_angles = jnp.cos(angles)[None, :, None]
    log_cosine = jnp.log(jnp.cos(0.5 * angles))[None, :, None]
    log_sine = jnp.log(jnp.sin(0.5 * angles))[None, :, None]
    lowest = jnp.maximum(jnp.abs(alpha_order), gamma_order)
    start_value = wigner_start(alpha_order, gamma_order, log_cosine, log_sine)
    first_block = jnp.min(jnp.abs(alpha_order)) // stride
    empty_state = jnp.zeros((group_size, grid_size, spread), jnp.float32)

    def compute_block(operands):
        block_index, former, current = operands
        levels = []
        for offset in range(stride):
            former, current = advance(
                block_index * stride + offset,
                (former, current),
                alpha_order,
                gamma_order,
                cos_angles,
                start_value,
                lowest,
            )
            levels.append(current)
        stacked = jnp.stack(levels, axis=0)
        block_part = jnp.einsum("jgkq,kgcq->gcjq", stacked, weighted, precision=HIGHEST)
        return (former, current, block_part)

    def skip_block(operands):
        block_index, former, current = operands
        return (former, current, jnp.zeros((group_size, channels, stride, spread), jnp.float32))

    def block_step(carried, block_index):
        former, current = carried
        former, current, block_part = lax.cond(
            block_index >= first_block, compute_block, skip_block, (block_index, former, current)
        )
        return ((former, current), block_part)

    _, parts = lax.scan(
        block_step, (empty_state, empty_state), jnp.arange(block_count, dtype=jnp.int32)
    )
    output = jnp.transpose(parts, (1, 2, 0, 3, 4)).reshape(group_size, channels, spread, spread)
    degree_scale = 8.0 * jnp.sqrt(2.0 * jnp.arange(spread, dtype=jnp.float32) + 1.0)
    return output * degree_scale[None, None, :, None]


def degree_energy(coeffs, functions, spread):
    split_view = coeffs.reshape(coeffs.shape[0], 2, functions, spread, spread)
    multiplicity = jnp.where(jnp.arange(spread) == 0, 1.0, 2.0).astype(jnp.float32)
    energy_sum = jnp.sum(split_view * split_view * multiplicity, axis=(0, 1, 4))
    degrees = 2.0 * jnp.arange(spread, dtype=jnp.float32) + 1.0
    return energy_sum / (degrees * degrees)[None, :]


def general_local(samples):
    devices = lax.axis_size("beta")
    device = lax.axis_index("beta")
    local_beta = samples.shape[0]
    functions = samples.shape[1]
    grid_size = samples.shape[2]
    spread = grid_size // 2
    channels = 2 * functions
    row_count = grid_size // devices
    natural_rows = jnp.arange(grid_size, dtype=jnp.int32)
    halfway = jnp.einsum("kfag,gx->kfax", samples, gamma_table(spread), precision=HIGHEST)
    halfway = halfway.reshape(local_beta, functions, grid_size, 2, spread)
    spectrum = jnp.einsum(
        "kfacq,spca->kpsfq", halfway, alpha_table(spread, natural_rows), precision=HIGHEST
    )
    spectrum = spectrum.reshape(local_beta, grid_size, channels, spread)
    received = lax.all_to_all(spectrum, "beta", split_axis=1, concat_axis=0, tiled=True)
    weighted = received * quadrature(spread)[:, None, None, None]
    owned_rows = lax.dynamic_slice_in_dim(natural_rows, device * row_count, row_count)
    computed = degree_rows(owned_rows, weighted, spread)
    power_part = degree_energy(computed, functions, spread)
    coeffs = computed
    power = lax.psum(power_part, "beta")
    coeffs = coeffs.reshape(row_count, 2, functions, spread, spread)
    return (coeffs, power)


def wigner_quarter(spread):
    alpha = np.arange(1 - spread, spread)[:, None]
    gamma = np.arange(spread)[None, :]
    lowest = np.maximum(np.abs(alpha), gamma)
    shift = np.maximum(0, gamma - alpha)
    logs = np.array([math.lgamma(value + 1.0) for value in range(2 * spread)])
    magnitude = 0.5 * (
        logs[lowest + alpha] + logs[lowest - alpha] + logs[lowest + gamma] + logs[lowest - gamma]
    )
    magnitude = magnitude - logs[lowest + gamma - shift] - logs[shift]
    magnitude = magnitude - logs[alpha - gamma + shift] - logs[lowest - alpha - shift]
    sign = 1.0 - 2.0 * ((alpha - gamma + shift) % 2)
    first = sign * np.exp(magnitude - lowest * math.log(2.0))
    squares_a, squares_g = alpha.astype(np.float64) ** 2, gamma.astype(np.float64) ** 2
    former, current, levels = np.zeros(first.shape), np.zeros(first.shape), []
    for degree in range(spread):
        before = degree - 1.0
        upper = np.sqrt(np.maximum((degree**2 - squares_a) * (degree**2 - squares_g), 1.0))
        lower = np.sqrt(np.maximum((before**2 - squares_a) * (before**2 - squares_g), 0.0))
        cross = alpha * gamma / max(before * degree, 1.0)
        follow = degree * (2.0 * before + 1.0) / upper * -cross * current
        follow = follow - degree * lower / (max(before, 1.0) * upper) * former
        former, current = current, np.where(lowest == degree, first, follow)
        levels.append(current)
    return np.stack(levels)


def split_pair(table):
    high = np.asarray(table).astype(jnp.bfloat16)
    return high, (table - high.astype(np.float64)).astype(jnp.bfloat16)


def fourier_tables(spread):
    grid = 2 * spread
    at = np.arange(grid)
    phase = 2.0 * np.pi / grid * (at[:, None] * np.arange(spread)[None, :] % grid)
    cosine, sine = np.cos(phase), -np.sin(phase)
    gamma_part = np.concatenate([cosine, sine], axis=1)
    phase = 2.0 * np.pi / grid * (at[:, None] * at[None, :] % grid)
    alpha_part = np.concatenate([np.cos(phase), np.sin(phase)], axis=1) / grid
    return gamma_part, alpha_part


def beta_table(spread):
    angles = (2.0 * np.arange(2 * spread) + 1.0) * (np.pi / (4.0 * spread))
    odd = 2.0 * np.arange(spread) + 1.0
    series = np.sum(np.sin(angles[:, None] * odd[None, :]) / odd[None, :], axis=1)
    weight = 2.0 / spread * np.sin(angles) * series
    order = np.concatenate([np.arange(0, spread, 2), np.arange(1, spread, 2)])
    fold = np.where(order == 0, 1.0, 2.0)[:, None] * weight[None, :]
    turn = order[:, None] * angles[None, :]
    return np.concatenate([fold * np.cos(turn), fold * np.sin(turn)], axis=0)


def sign_masks(spread):
    step = (np.arange(SUBLANES)[:, None] - np.arange(spread)[None, :]) % 4
    even = np.where(step == 0, 1.0, np.where(step == 2, -1.0, 0.0))
    odd = np.where(step == 3, 1.0, np.where(step == 1, -1.0, 0.0))
    return np.concatenate([even, even], axis=1), np.concatenate([odd, odd], axis=1)


def block_steps(spread):
    blocks = spread // SUBLANES
    return [(block, chunk) for block in range(blocks) for chunk in range(block + 1)]


def quarter_tables(spread, devices):
    quarter = wigner_quarter(spread)
    rows = np.arange(2 * spread)
    orders = np.where(rows < spread, rows, rows - 2 * spread)
    by_row = quarter[:, np.maximum(orders, 1 - spread) + spread - 1, :]
    by_row = np.where((orders > -spread)[None, :, None], by_row, 0.0)
    by_row = by_row * (8.0 * np.sqrt(2.0 * np.arange(spread) + 1.0))[:, None, None]
    gammas, alphas = [], []
    for block, chunk in block_steps(spread):
        degrees = slice(block * SUBLANES, (block + 1) * SUBLANES)
        part = slice(chunk * SUBLANES, (chunk + 1) * SUBLANES)
        gammas.append(np.swapaxes(quarter[degrees, spread - 1 :, part], 1, 2).reshape(-1, LANES))
        table = np.swapaxes(by_row[degrees, :, part], 0, 1)
        alphas.append(table.reshape(devices, SUBLANES, SUBLANES * SUBLANES))
    alphas = np.stack(alphas, axis=1)
    alphas = np.concatenate([alphas[:, 0::2], alphas[:, 1::2]], axis=-1)
    return np.stack(gammas).astype(np.float32), alphas.astype(np.float32)


def split_value(value):
    high = value.astype(jnp.bfloat16)
    return high, (value - high.astype(jnp.float32)).astype(jnp.bfloat16)


def dot(left, right):
    return jnp.dot(left, right, preferred_element_type=jnp.float32)


def quarter_turn(value):
    middle = value.shape[1] // 2
    return jnp.concatenate([value[:, middle:], -value[:, :middle]], axis=1)


def spectrum_kernel(x_ref, gamma_two, alpha_two, out_ref):
    count, _, grid, _ = x_ref.shape
    blocks = out_ref.shape[0]
    high, low = split_value(x_ref[:, 0].reshape(count * grid, grid))
    both = dot(jnp.concatenate([high, low], axis=1), gamma_two[...])
    halves = split_value(both[:, :LANES] + both[:, LANES:])
    for k in range(0, count, 2):
        high, low = [
            jnp.concatenate(
                [
                    jnp.concatenate([turn(part[(k + i) * grid : (k + i + 1) * grid]) for i in range(2)], axis=1)
                    for turn in (lambda value: value, quarter_turn)
                ],
                axis=0,
            )
            for part in halves
        ]
        both = dot(alpha_two[...], high)
        rows = both[:grid] + both[grid:] + dot(alpha_two[:grid], low)
        for i in range(2):
            for d in range(blocks):
                out_ref[d, 0, pl.ds(k + i, SUBLANES, stride=count), :] = rows[
                    d * SUBLANES : (d + 1) * SUBLANES, i * LANES : (i + 1) * LANES
                ]


def spectrum_call(samples, devices):
    count, functions, grid, _ = samples.shape
    gamma_part, alpha_part = fourier_tables(grid // 2)
    gamma_hi, gamma_lo = split_pair(gamma_part)
    above = np.concatenate([gamma_hi, gamma_lo], axis=1)
    below = np.concatenate([gamma_hi, np.zeros_like(gamma_lo)], axis=1)
    tables = [np.concatenate([above, below], axis=0)]
    tables.append(np.concatenate(split_pair(alpha_part), axis=0))
    rows = grid // devices * count
    whole = lambda table: pl.BlockSpec(table.shape, lambda f: (0, 0))
    return pl.pallas_call(
        spectrum_kernel,
        grid=(functions,),
        in_specs=[pl.BlockSpec((count, 1, grid, grid), lambda f: (0, f, 0, 0))]
        + [whole(table) for table in tables],
        out_specs=pl.BlockSpec((devices, 1, rows, LANES), lambda f: (0, f, 0, 0)),
        out_shape=jax.ShapeDtypeStruct((devices, functions, rows, LANES), jnp.float32),
        name="spectrum",
    )(samples, *tables)


def factor_kernel(gamma_ref, alpha_ref, out_ref):
    pairs = out_ref.shape[1]
    left = lax.broadcasted_iota(jnp.int32, (SUBLANES, LANES), 1) < LANES // 2

    def step(at, carry):
        column = alpha_ref[at]
        for half in range(2):
            for i in range(pairs):
                lane = 2 * (half * pairs + i)
                wide = [
                    jnp.broadcast_to(column[:, lane + j : lane + j + 1], (SUBLANES, LANES))
                    for j in range(2)
                ]
                row = gamma_ref[2 * at + half, pl.ds(i, SUBLANES, stride=0), :]
                out_ref[2 * at + half, i] = jnp.where(left, wide[0], wide[1]) * row
        return carry

    lax.fori_loop(0, alpha_ref.shape[0], step, 0)


def factor_call(gammas, alphas):
    steps, pairs, _ = gammas.shape
    return pl.pallas_call(
        factor_kernel,
        out_shape=jax.ShapeDtypeStruct((steps, pairs, SUBLANES, LANES), jnp.float32),
        name="factors",
    )(gammas, alphas)


def degree_kernel(
    r_ref, beta_two, even_ref, odd_ref, source_ref, out_ref, pow_ref,
    t_ref, c_ref, e_ref, held_ref, factor_ref, sems, factor_sems,
):
    sources, functions, held, _ = r_ref.shape
    count = held // SUBLANES
    spread = beta_two.shape[0] // 4
    blocks = spread // SUBLANES
    firsts = [block * (block + 1) // 2 for block in range(blocks)]

    def factor_copy(block):
        part = pl.ds(firsts[block], block + 1)
        return pltpu.make_async_copy(
            source_ref.at[part], factor_ref.at[part], factor_sems.at[block]
        )

    row = lax.axis_index("beta") * SUBLANES
    smallest = jnp.where(row < spread, row, 2 * spread - row - SUBLANES + 1)
    first_block = smallest // SUBLANES
    for block in range(blocks):

        @pl.when(block >= first_block)
        def _():
            factor_copy(block).start()

    left = lax.broadcasted_iota(jnp.int32, (spread // 2, LANES), 1) < spread
    for f in range(0, functions, 2):
        for n in range(SUBLANES):
            parts = [
                r_ref[:, f + i, n * count : (n + 1) * count, :].reshape(sources * count, LANES)
                for i in range(2)
            ]
            high, low = split_value(jnp.concatenate(parts, axis=1))
            both = dot(beta_two[...], jnp.concatenate([high, low], axis=0))
            both = both[: 2 * spread] + both[2 * spread :]
            turned = [
                jnp.where(
                    even_ref[n : n + 1] != 0.0,
                    both[:spread, i * LANES : (i + 1) * LANES] * even_ref[n : n + 1],
                    both[spread:, i * LANES : (i + 1) * LANES] * odd_ref[n : n + 1],
                )
                for i in range(2)
            ]
            for i in range(2):
                evens, odds = turned[i][: spread // 2], turned[i][spread // 2 :]
                parted = (
                    jnp.where(left, evens, pltpu.roll(odds, spread, 1)),
                    jnp.where(left, pltpu.roll(evens, spread, 1), odds),
                )
                for part in range(2):
                    for b in range(spread // (2 * SUBLANES)):
                        t_ref[
                            part, f + i, pl.ds(b * SUBLANES * SUBLANES + n, SUBLANES, stride=SUBLANES), :
                        ] = parted[part][b * SUBLANES : (b + 1) * SUBLANES]

    zero = jnp.zeros((SUBLANES, LANES), jnp.float32)

    def out_copy(block):
        part = (slice(None), slice(None), slice(None), pl.ds(block * SUBLANES, SUBLANES))
        return pltpu.make_async_copy(held_ref.at[part], out_ref.at[part], sems.at[block])

    def fill(block):
        degrees = slice(block * SUBLANES, (block + 1) * SUBLANES)
        empty = jnp.zeros((SUBLANES, 2, functions, SUBLANES, spread), jnp.float32)
        held_ref[:, :, :, degrees, :] = empty
        for f in range(functions):
            e_ref[f, degrees, :] = zero

    channels = [(part, f) for part in range(2) for f in range(functions)]
    some = SUBLANES // 2

    def work(block):
        factor_copy(block).wait()
        degrees = slice(block * SUBLANES, (block + 1) * SUBLANES)
        for half in range(2):
            totals = [[zero] * len(channels) for _ in range(some)]
            for chunk in range(block + 1):
                for i in range(SUBLANES // 2):
                    row = (chunk * SUBLANES // 2 + i) * SUBLANES
                    values = [t_ref[part, f, row : row + SUBLANES, :] for part, f in channels]
                    for j in range(some):
                        at = (half * some + j) * SUBLANES // 2 + i
                        factor = factor_ref[firsts[block] + chunk, at]
                        totals[j] = [t + factor * v for t, v in zip(totals[j], values)]
            for j in range(some):
                for (part, f), total in zip(channels, totals[j]):
                    c_ref[part, f, pl.ds(half * some + j, SUBLANES, stride=SUBLANES), :] = total
        for f in range(functions):
            energy = zero
            for part in range(2):
                for n in range(SUBLANES):
                    tile = c_ref[part, f, n * SUBLANES : (n + 1) * SUBLANES, :]
                    tile = tile + pltpu.roll(tile, spread, 1)
                    energy += tile * tile
                    held_ref[n, part, f, degrees, :] = tile[:, :spread]
            e_ref[f, degrees, :] = energy

    for block in range(blocks):
        pl.when(block < first_block)(lambda: fill(block))
        pl.when(block >= first_block)(lambda: work(block))
        out_copy(block).start()

    lane = lax.broadcasted_iota(jnp.int32, (SUBLANES, LANES), 1)
    fold = jnp.where(lane == 0, 1.0, jnp.where(lane < spread, 2.0, 0.0)).astype(jnp.bfloat16)
    across = lambda part: lax.dot_general(
        fold, part, (((1,), (1,)), ((), ())), preferred_element_type=jnp.float32
    )
    place = lax.broadcasted_iota(jnp.int32, (SUBLANES, spread), 0)
    power = jnp.zeros((SUBLANES, spread), jnp.float32)
    for f in range(functions):
        high, low = split_value(e_ref[f])
        rest = e_ref[f] - high.astype(jnp.float32) - low.astype(jnp.float32)
        total = across(high) + across(low) + across(rest.astype(jnp.bfloat16))
        power = jnp.where(place == f, total, power)
    power = jnp.concatenate([power, jnp.zeros_like(power)], axis=1)
    for d in range(pow_ref.shape[0]):
        pow_ref[d] = power

    for block in range(blocks):
        out_copy(block).wait()


def degree_call(received, factors, spread):
    functions = received.shape[1]
    high, low = split_pair(beta_table(spread))
    above = np.concatenate([high, high], axis=1)
    below = np.concatenate([low, np.zeros_like(low)], axis=1)
    tables = [np.concatenate([above, below], axis=0)]
    tables += [mask.astype(np.float32) for mask in sign_masks(spread)]
    shape = (SUBLANES, 2, functions, spread, spread)
    vmem = pl.BlockSpec(memory_space=pltpu.VMEM)
    return pl.pallas_call(
        degree_kernel,
        in_specs=[vmem] * 4 + [pl.BlockSpec(memory_space=pl.ANY)],
        out_specs=[pl.BlockSpec(memory_space=pl.ANY), vmem],
        out_shape=[
            jax.ShapeDtypeStruct(shape, jnp.float32),
            jax.ShapeDtypeStruct((received.shape[0], SUBLANES, LANES), jnp.float32),
        ],
        scratch_shapes=[
            pltpu.VMEM((2, functions, spread // 2 * SUBLANES, LANES), jnp.float32),
            pltpu.VMEM((2, functions, SUBLANES * SUBLANES, LANES), jnp.float32),
            pltpu.VMEM((functions, spread, LANES), jnp.float32),
            pltpu.VMEM(shape, jnp.float32),
            pltpu.VMEM(factors.shape, jnp.float32),
            pltpu.SemaphoreType.DMA((spread // SUBLANES,)),
            pltpu.SemaphoreType.DMA((spread // SUBLANES,)),
        ],
        compiler_params=pltpu.CompilerParams(vmem_limit_bytes=50 << 20),
        name="degrees",
    )(received, *tables, factors)


def fast_local(samples):
    devices = lax.axis_size("beta")
    device = lax.axis_index("beta")
    functions, grid_size = samples.shape[1:3]
    spread = grid_size // 2
    sent = spectrum_call(samples, devices)
    received = lax.all_to_all(sent, "beta", split_axis=0, concat_axis=0, tiled=True)
    gammas, alphas = quarter_tables(spread, devices)
    alphas = lax.dynamic_index_in_dim(jnp.asarray(alphas), device, 0, keepdims=False)
    factors = factor_call(jnp.asarray(gammas), alphas)
    coeffs, shares = degree_call(received, factors, spread)
    order = list(range(devices))[::-1]
    shares = lax.all_to_all(
        shares, "beta", split_axis=0, concat_axis=0, tiled=True, axis_index_groups=[order]
    )
    scale = (1.0 / (2.0 * np.arange(spread) + 1.0) ** 2).astype(np.float32)
    return coeffs, jnp.sum(shares[:, :functions, :spread], axis=0) * scale[None, :]


def local(samples):
    devices = lax.axis_size("beta")
    local_beta, functions, grid_size = samples.shape[:3]
    tiled = grid_size == LANES and local_beta == SUBLANES and grid_size == devices * SUBLANES
    if tiled and functions % 2 == 0:
        return fast_local(samples)
    return general_local(samples)


def solution(mesh):
    return jax.shard_map(
        local,
        mesh=mesh,
        in_specs=(P("beta", "grp", None, None),),
        out_specs=(P("beta", None, "grp", None, None), P("grp", None)),
        check_vma=False,
    )
```

```python
import math

import jax
import jax.numpy as jnp
import numpy as np
from jax import lax
from jax.experimental import pallas as pl
from jax.experimental.pallas import tpu as pltpu
from jax.sharding import PartitionSpec as P

HIGHEST = lax.Precision.HIGHEST
SUBLANES = 8
LANES = 128


def beta_angles(spread):
    grid_size = 2 * spread
    return (2.0 * jnp.arange(grid_size, dtype=jnp.float32) + 1.0) * (jnp.pi / (4.0 * spread))


def quadrature(spread):
    angles = beta_angles(spread)
    odd_terms = 2.0 * jnp.arange(spread, dtype=jnp.float32) + 1.0
    series = jnp.sum(jnp.sin(angles[:, None] * odd_terms[None, :]) / odd_terms[None, :], axis=1)
    return 2.0 / spread * jnp.sin(angles) * series


def gamma_table(spread):
    grid_size = 2 * spread
    positions = jnp.arange(grid_size, dtype=jnp.int32)
    orders = jnp.arange(spread, dtype=jnp.int32)
    phase_index = positions[:, None] * orders[None, :] % grid_size
    angles = phase_index.astype(jnp.float32) * (2.0 * jnp.pi / grid_size)
    return jnp.concatenate([jnp.cos(angles), -jnp.sin(angles)], axis=1)


def alpha_table(spread, row_index):
    grid_size = 2 * spread
    positions = jnp.arange(grid_size, dtype=jnp.int32)
    phase_index = row_index[:, None] * positions[None, :] % grid_size
    angles = phase_index.astype(jnp.float32) * (2.0 * jnp.pi / grid_size)
    cosine = jnp.cos(angles) / grid_size
    sine_part = jnp.sin(angles) / grid_size
    real_rows = jnp.stack([cosine, sine_part], axis=1)
    imag_rows = jnp.stack([-sine_part, cosine], axis=1)
    return jnp.stack([real_rows, imag_rows], axis=0)


def log_factorial(value, float_type):
    return lax.lgamma((value + 1).astype(float_type))


def wigner_start(alpha_order, gamma_order, log_cosine, log_sine):
    float_type = log_cosine.dtype
    lowest = jnp.maximum(jnp.abs(alpha_order), gamma_order)
    shift_low = jnp.maximum(0, gamma_order - alpha_order)
    magnitude = 0.5 * (
        log_factorial(lowest + alpha_order, float_type)
        + log_factorial(lowest - alpha_order, float_type)
        + log_factorial(lowest + gamma_order, float_type)
        + log_factorial(lowest - gamma_order, float_type)
    )
    magnitude = (
        magnitude
        - log_factorial(lowest + gamma_order - shift_low, float_type)
        - log_factorial(shift_low, float_type)
    )
    magnitude = magnitude - log_factorial(alpha_order - gamma_order + shift_low, float_type)
    magnitude = magnitude - log_factorial(lowest - alpha_order - shift_low, float_type)
    cos_power = (2 * lowest + gamma_order - alpha_order - 2 * shift_low).astype(float_type)
    sin_power = (alpha_order - gamma_order + 2 * shift_low).astype(float_type)
    parity = (alpha_order - gamma_order + shift_low) % 2
    sign_factor = (1 - 2 * parity).astype(float_type)
    return sign_factor * jnp.exp(magnitude + cos_power * log_cosine + sin_power * log_sine)


def advance(degree, carried, alpha_order, gamma_order, cos_angles, start_value, lowest):
    former, current = carried
    float_type = current.dtype
    previous = (degree - 1).astype(float_type)
    alpha_float = alpha_order.astype(float_type)
    gamma_float = gamma_order.astype(float_type)
    cross_ratio = alpha_float * gamma_float / jnp.maximum(previous * (previous + 1.0), 1.0)
    upper_term = ((previous + 1.0) * (previous + 1.0) - alpha_float * alpha_float) * (
        (previous + 1.0) * (previous + 1.0) - gamma_float * gamma_float
    )
    lower_term = (previous * previous - alpha_float * alpha_float) * (
        previous * previous - gamma_float * gamma_float
    )
    root_upper = jnp.sqrt(jnp.maximum(upper_term, 1.0))
    forward = (previous + 1.0) * (2.0 * previous + 1.0) / root_upper
    backward = (
        (previous + 1.0)
        * jnp.sqrt(jnp.maximum(lower_term, 0.0))
        / (jnp.maximum(previous, 1.0) * root_upper)
    )
    recurred = forward * (cos_angles - cross_ratio) * current - backward * former
    renewed = jnp.where(degree == lowest, start_value, recurred)
    return (current, renewed)


def degree_rows(row_index, weighted, spread):
    stride = 8
    grid_size = 2 * spread
    group_size = row_index.shape[0]
    channels = weighted.shape[2]
    block_count = spread // stride
    alpha_order = jnp.where(row_index < spread, row_index, row_index - grid_size)[:, None, None]
    gamma_order = jnp.arange(spread, dtype=jnp.int32)[None, None, :]
    angles = beta_angles(spread)
    cos_angles = jnp.cos(angles)[None, :, None]
    log_cosine = jnp.log(jnp.cos(0.5 * angles))[None, :, None]
    log_sine = jnp.log(jnp.sin(0.5 * angles))[None, :, None]
    lowest = jnp.maximum(jnp.abs(alpha_order), gamma_order)
    start_value = wigner_start(alpha_order, gamma_order, log_cosine, log_sine)
    first_block = jnp.min(jnp.abs(alpha_order)) // stride
    empty_state = jnp.zeros((group_size, grid_size, spread), jnp.float32)

    def compute_block(operands):
        block_index, former, current = operands
        levels = []
        for offset in range(stride):
            former, current = advance(
                block_index * stride + offset,
                (former, current),
                alpha_order,
                gamma_order,
                cos_angles,
                start_value,
                lowest,
            )
            levels.append(current)
        stacked = jnp.stack(levels, axis=0)
        block_part = jnp.einsum("jgkq,kgcq->gcjq", stacked, weighted, precision=HIGHEST)
        return (former, current, block_part)

    def skip_block(operands):
        block_index, former, current = operands
        return (former, current, jnp.zeros((group_size, channels, stride, spread), jnp.float32))

    def block_step(carried, block_index):
        former, current = carried
        former, current, block_part = lax.cond(
            block_index >= first_block, compute_block, skip_block, (block_index, former, current)
        )
        return ((former, current), block_part)

    _, parts = lax.scan(
        block_step, (empty_state, empty_state), jnp.arange(block_count, dtype=jnp.int32)
    )
    output = jnp.transpose(parts, (1, 2, 0, 3, 4)).reshape(group_size, channels, spread, spread)
    degree_scale = 8.0 * jnp.sqrt(2.0 * jnp.arange(spread, dtype=jnp.float32) + 1.0)
    return output * degree_scale[None, None, :, None]


def degree_energy(coeffs, functions, spread):
    split_view = coeffs.reshape(coeffs.shape[0], 2, functions, spread, spread)
    multiplicity = jnp.where(jnp.arange(spread) == 0, 1.0, 2.0).astype(jnp.float32)
    energy_sum = jnp.sum(split_view * split_view * multiplicity, axis=(0, 1, 4))
    degrees = 2.0 * jnp.arange(spread, dtype=jnp.float32) + 1.0
    return energy_sum / (degrees * degrees)[None, :]


def general_local(samples):
    devices = lax.axis_size("beta")
    device = lax.axis_index("beta")
    local_beta = samples.shape[0]
    functions = samples.shape[1]
    grid_size = samples.shape[2]
    spread = grid_size // 2
    channels = 2 * functions
    row_count = grid_size // devices
    natural_rows = jnp.arange(grid_size, dtype=jnp.int32)
    halfway = jnp.einsum("kfag,gx->kfax", samples, gamma_table(spread), precision=HIGHEST)
    halfway = halfway.reshape(local_beta, functions, grid_size, 2, spread)
    spectrum = jnp.einsum(
        "kfacq,spca->kpsfq", halfway, alpha_table(spread, natural_rows), precision=HIGHEST
    )
    spectrum = spectrum.reshape(local_beta, grid_size, channels, spread)
    received = lax.all_to_all(spectrum, "beta", split_axis=1, concat_axis=0, tiled=True)
    weighted = received * quadrature(spread)[:, None, None, None]
    owned_rows = lax.dynamic_slice_in_dim(natural_rows, device * row_count, row_count)
    computed = degree_rows(owned_rows, weighted, spread)
    power_part = degree_energy(computed, functions, spread)
    coeffs = computed
    power = lax.psum(power_part, "beta")
    coeffs = coeffs.reshape(row_count, 2, functions, spread, spread)
    return (coeffs, power)


def wigner_quarter(spread):
    alpha = np.arange(1 - spread, spread)[:, None]
    gamma = np.arange(spread)[None, :]
    lowest = np.maximum(np.abs(alpha), gamma)
    shift = np.maximum(0, gamma - alpha)
    logs = np.array([math.lgamma(value + 1.0) for value in range(2 * spread)])
    magnitude = 0.5 * (
        logs[lowest + alpha] + logs[lowest - alpha] + logs[lowest + gamma] + logs[lowest - gamma]
    )
    magnitude = magnitude - logs[lowest + gamma - shift] - logs[shift]
    magnitude = magnitude - logs[alpha - gamma + shift] - logs[lowest - alpha - shift]
    sign = 1.0 - 2.0 * ((alpha - gamma + shift) % 2)
    first = sign * np.exp(magnitude - lowest * math.log(2.0))
    squares_a, squares_g = alpha.astype(np.float64) ** 2, gamma.astype(np.float64) ** 2
    former, current, levels = np.zeros(first.shape), np.zeros(first.shape), []
    for degree in range(spread):
        before = degree - 1.0
        upper = np.sqrt(np.maximum((degree**2 - squares_a) * (degree**2 - squares_g), 1.0))
        lower = np.sqrt(np.maximum((before**2 - squares_a) * (before**2 - squares_g), 0.0))
        cross = alpha * gamma / max(before * degree, 1.0)
        follow = degree * (2.0 * before + 1.0) / upper * -cross * current
        follow = follow - degree * lower / (max(before, 1.0) * upper) * former
        former, current = current, np.where(lowest == degree, first, follow)
        levels.append(current)
    return np.stack(levels)


def split_pair(table):
    high = np.asarray(table).astype(jnp.bfloat16)
    return high, (table - high.astype(np.float64)).astype(jnp.bfloat16)


def fourier_tables(spread):
    grid = 2 * spread
    at = np.arange(grid)
    phase = 2.0 * np.pi / grid * (at[:, None] * np.arange(spread)[None, :] % grid)
    cosine, sine = np.cos(phase), -np.sin(phase)
    gamma_part = np.concatenate([cosine, sine], axis=1)
    phase = 2.0 * np.pi / grid * (at[:, None] * at[None, :] % grid)
    alpha_part = np.concatenate([np.cos(phase), np.sin(phase)], axis=1) / grid
    return gamma_part, alpha_part


def beta_table(spread):
    angles = (2.0 * np.arange(2 * spread) + 1.0) * (np.pi / (4.0 * spread))
    odd = 2.0 * np.arange(spread) + 1.0
    series = np.sum(np.sin(angles[:, None] * odd[None, :]) / odd[None, :], axis=1)
    weight = 2.0 / spread * np.sin(angles) * series
    order = np.concatenate([np.arange(0, spread, 2), np.arange(1, spread, 2)])
    fold = np.where(order == 0, 1.0, 2.0)[:, None] * weight[None, :]
    turn = order[:, None] * angles[None, :]
    return np.concatenate([fold * np.cos(turn), fold * np.sin(turn)], axis=0)


def sign_masks(spread):
    step = (np.arange(SUBLANES)[:, None] - np.arange(spread)[None, :]) % 4
    even = np.where(step == 0, 1.0, np.where(step == 2, -1.0, 0.0))
    odd = np.where(step == 3, 1.0, np.where(step == 1, -1.0, 0.0))
    return np.concatenate([even, even], axis=1), np.concatenate([odd, odd], axis=1)


def block_steps(spread):
    blocks = spread // SUBLANES
    return [(block, chunk) for block in range(blocks) for chunk in range(block + 1)]


def quarter_tables(spread, devices):
    quarter = wigner_quarter(spread)
    rows = np.arange(2 * spread)
    orders = np.where(rows < spread, rows, rows - 2 * spread)
    by_row = quarter[:, np.maximum(orders, 1 - spread) + spread - 1, :]
    by_row = np.where((orders > -spread)[None, :, None], by_row, 0.0)
    by_row = by_row * (8.0 * np.sqrt(2.0 * np.arange(spread) + 1.0))[:, None, None]
    gammas, alphas = [], []
    for block, chunk in block_steps(spread):
        degrees = slice(block * SUBLANES, (block + 1) * SUBLANES)
        part = slice(chunk * SUBLANES, (chunk + 1) * SUBLANES)
        gammas.append(np.swapaxes(quarter[degrees, spread - 1 :, part], 1, 2).reshape(-1, LANES))
        table = np.swapaxes(by_row[degrees, :, part], 0, 1)
        alphas.append(table.reshape(devices, SUBLANES, SUBLANES * SUBLANES))
    alphas = np.stack(alphas, axis=1)
    alphas = np.concatenate([alphas[:, 0::2], alphas[:, 1::2]], axis=-1)
    return np.stack(gammas).astype(np.float32), alphas.astype(np.float32)


def split_value(value):
    high = value.astype(jnp.bfloat16)
    return high, (value - high.astype(jnp.float32)).astype(jnp.bfloat16)


def dot(left, right):
    return jnp.dot(left, right, preferred_element_type=jnp.float32)


def spectrum_kernel(x_ref, gamma_two, alpha_two, out_ref):
    count, _, grid, _ = x_ref.shape
    blocks = out_ref.shape[0]
    for f in range(x_ref.shape[1]):
        high, low = split_value(x_ref[:, f].reshape(count * grid, grid))
        both = dot(jnp.concatenate([high, low], axis=1), gamma_two[...])
        half = both[:, :LANES] + both[:, LANES:]
        lane = lax.broadcasted_iota(jnp.int32, (1, LANES), 1)
        sign = jnp.where(lane < LANES // 2, 1.0, -1.0)
        for k in range(0, count, 2):
            pairs = [half[(k + i) * grid : (k + i + 1) * grid] for i in range(2)]
            pair = jnp.concatenate(
                [
                    jnp.concatenate(pairs, axis=1),
                    jnp.concatenate([pltpu.roll(p, LANES // 2, 1) * sign for p in pairs], axis=1),
                ],
                axis=0,
            )
            high, low = split_value(pair)
            both = dot(alpha_two[...], high)
            rows = both[:grid] + both[grid:] + dot(alpha_two[:grid], low)
            for i in range(2):
                for d in range(blocks):
                    out_ref[d, f, pl.ds(k + i, SUBLANES, stride=count), :] = rows[
                        d * SUBLANES : (d + 1) * SUBLANES, i * LANES : (i + 1) * LANES
                    ]


def spectrum_call(samples, devices):
    count, functions, grid, _ = samples.shape
    gamma_part, alpha_part = fourier_tables(grid // 2)
    gamma_hi, gamma_lo = split_pair(gamma_part)
    above = np.concatenate([gamma_hi, gamma_lo], axis=1)
    below = np.concatenate([gamma_hi, np.zeros_like(gamma_lo)], axis=1)
    tables = [np.concatenate([above, below], axis=0)]
    tables.append(np.concatenate(split_pair(alpha_part), axis=0))
    rows = grid // devices * count
    steps = 2
    some = functions // steps
    whole = lambda table: pl.BlockSpec(table.shape, lambda f: (0, 0))
    return pl.pallas_call(
        spectrum_kernel,
        grid=(steps,),
        in_specs=[pl.BlockSpec((count, some, grid, grid), lambda f: (0, f, 0, 0))]
        + [whole(table) for table in tables],
        out_specs=pl.BlockSpec((devices, some, rows, LANES), lambda f: (0, f, 0, 0)),
        out_shape=jax.ShapeDtypeStruct((devices, functions, rows, LANES), jnp.float32),
        name="spectrum",
    )(samples, *tables)


def factor_kernel(gamma_ref, alpha_ref, out_ref):
    pairs = out_ref.shape[1]
    left = lax.broadcasted_iota(jnp.int32, (SUBLANES, LANES), 1) < LANES // 2

    def step(at, carry):
        column = alpha_ref[at]
        for half in range(2):
            for i in range(pairs):
                lane = 2 * (half * pairs + i)
                wide = [
                    jnp.broadcast_to(column[:, lane + j : lane + j + 1], (SUBLANES, LANES))
                    for j in range(2)
                ]
                row = gamma_ref[2 * at + half, pl.ds(i, SUBLANES, stride=0), :]
                out_ref[2 * at + half, i] = jnp.where(left, wide[0], wide[1]) * row
        return carry

    lax.fori_loop(0, alpha_ref.shape[0], step, 0)


def factor_call(gammas, alphas):
    steps, pairs, _ = gammas.shape
    return pl.pallas_call(
        factor_kernel,
        out_shape=jax.ShapeDtypeStruct((steps, pairs, SUBLANES, LANES), jnp.float32),
        name="factors",
    )(gammas, alphas)


def degree_kernel(
    r_ref, beta_two, even_ref, odd_ref, source_ref, out_ref, pow_ref,
    t_ref, c_ref, e_ref, held_ref, factor_ref, sems, factor_sems,
):
    sources, functions, held, _ = r_ref.shape
    count = held // SUBLANES
    spread = beta_two.shape[0] // 4
    blocks = spread // SUBLANES
    firsts = [block * (block + 1) // 2 for block in range(blocks)]

    def factor_copy(block):
        part = pl.ds(firsts[block], block + 1)
        return pltpu.make_async_copy(
            source_ref.at[part], factor_ref.at[part], factor_sems.at[block]
        )

    row = lax.axis_index("beta") * SUBLANES
    smallest = jnp.where(row < spread, row, 2 * spread - row - SUBLANES + 1)
    first_block = smallest // SUBLANES
    for block in range(blocks):

        @pl.when(block >= first_block)
        def _():
            factor_copy(block).start()

    left = lax.broadcasted_iota(jnp.int32, (spread // 2, LANES), 1) < spread
    for f in range(0, functions, 2):
        for n in range(SUBLANES):
            parts = [
                r_ref[:, f + i, n * count : (n + 1) * count, :].reshape(sources * count, LANES)
                for i in range(2)
            ]
            high, low = split_value(jnp.concatenate(parts, axis=1))
            both = dot(beta_two[...], jnp.concatenate([high, low], axis=0))
            both = both[: 2 * spread] + both[2 * spread :]
            turned = [
                jnp.where(
                    even_ref[n : n + 1] != 0.0,
                    both[:spread, i * LANES : (i + 1) * LANES] * even_ref[n : n + 1],
                    both[spread:, i * LANES : (i + 1) * LANES] * odd_ref[n : n + 1],
                )
                for i in range(2)
            ]
            for i in range(2):
                evens, odds = turned[i][: spread // 2], turned[i][spread // 2 :]
                parted = (
                    jnp.where(left, evens, pltpu.roll(odds, spread, 1)),
                    jnp.where(left, pltpu.roll(evens, spread, 1), odds),
                )
                for part in range(2):
                    for b in range(spread // (2 * SUBLANES)):
                        t_ref[
                            part, f + i, pl.ds(b * SUBLANES * SUBLANES + n, SUBLANES, stride=SUBLANES), :
                        ] = parted[part][b * SUBLANES : (b + 1) * SUBLANES]

    zero = jnp.zeros((SUBLANES, LANES), jnp.float32)

    def out_copy(block):
        part = (slice(None), slice(None), slice(None), pl.ds(block * SUBLANES, SUBLANES))
        return pltpu.make_async_copy(held_ref.at[part], out_ref.at[part], sems.at[block])

    def fill(block):
        degrees = slice(block * SUBLANES, (block + 1) * SUBLANES)
        empty = jnp.zeros((SUBLANES, 2, functions, SUBLANES, spread), jnp.float32)
        held_ref[:, :, :, degrees, :] = empty
        for f in range(functions):
            e_ref[f, degrees, :] = zero

    channels = [(part, f) for part in range(2) for f in range(functions)]
    some = SUBLANES // 2

    def work(block):
        factor_copy(block).wait()
        degrees = slice(block * SUBLANES, (block + 1) * SUBLANES)
        for half in range(2):
            totals = [[zero] * len(channels) for _ in range(some)]
            for chunk in range(block + 1):
                for i in range(SUBLANES // 2):
                    row = (chunk * SUBLANES // 2 + i) * SUBLANES
                    values = [t_ref[part, f, row : row + SUBLANES, :] for part, f in channels]
                    for j in range(some):
                        at = (half * some + j) * SUBLANES // 2 + i
                        factor = factor_ref[firsts[block] + chunk, at]
                        totals[j] = [t + factor * v for t, v in zip(totals[j], values)]
            for j in range(some):
                for (part, f), total in zip(channels, totals[j]):
                    c_ref[part, f, pl.ds(half * some + j, SUBLANES, stride=SUBLANES), :] = total
        for f in range(functions):
            energy = zero
            for part in range(2):
                for n in range(SUBLANES):
                    tile = c_ref[part, f, n * SUBLANES : (n + 1) * SUBLANES, :]
                    tile = tile + pltpu.roll(tile, spread, 1)
                    energy += tile * tile
                    held_ref[n, part, f, degrees, :] = tile[:, :spread]
            e_ref[f, degrees, :] = energy

    for block in range(blocks):
        pl.when(block < first_block)(lambda: fill(block))
        pl.when(block >= first_block)(lambda: work(block))
        out_copy(block).start()

    lane = lax.broadcasted_iota(jnp.int32, (SUBLANES, LANES), 1)
    fold = jnp.where(lane == 0, 1.0, jnp.where(lane < spread, 2.0, 0.0)).astype(jnp.bfloat16)
    across = lambda part: lax.dot_general(
        fold, part, (((1,), (1,)), ((), ())), preferred_element_type=jnp.float32
    )
    place = lax.broadcasted_iota(jnp.int32, (SUBLANES, spread), 0)
    power = jnp.zeros((SUBLANES, spread), jnp.float32)
    for f in range(functions):
        high, low = split_value(e_ref[f])
        rest = e_ref[f] - high.astype(jnp.float32) - low.astype(jnp.float32)
        total = across(high) + across(low) + across(rest.astype(jnp.bfloat16))
        power = jnp.where(place == f, total, power)
    power = jnp.concatenate([power, jnp.zeros_like(power)], axis=1)
    for d in range(pow_ref.shape[0]):
        pow_ref[d] = power

    for block in range(blocks):
        out_copy(block).wait()


def degree_call(received, factors, spread):
    functions = received.shape[1]
    high, low = split_pair(beta_table(spread))
    above = np.concatenate([high, high], axis=1)
    below = np.concatenate([low, np.zeros_like(low)], axis=1)
    tables = [np.concatenate([above, below], axis=0)]
    tables += [mask.astype(np.float32) for mask in sign_masks(spread)]
    shape = (SUBLANES, 2, functions, spread, spread)
    vmem = pl.BlockSpec(memory_space=pltpu.VMEM)
    return pl.pallas_call(
        degree_kernel,
        in_specs=[vmem] * 4 + [pl.BlockSpec(memory_space=pl.ANY)],
        out_specs=[pl.BlockSpec(memory_space=pl.ANY), vmem],
        out_shape=[
            jax.ShapeDtypeStruct(shape, jnp.float32),
            jax.ShapeDtypeStruct((received.shape[0], SUBLANES, LANES), jnp.float32),
        ],
        scratch_shapes=[
            pltpu.VMEM((2, functions, spread // 2 * SUBLANES, LANES), jnp.float32),
            pltpu.VMEM((2, functions, SUBLANES * SUBLANES, LANES), jnp.float32),
            pltpu.VMEM((functions, spread, LANES), jnp.float32),
            pltpu.VMEM(shape, jnp.float32),
            pltpu.VMEM(factors.shape, jnp.float32),
            pltpu.SemaphoreType.DMA((spread // SUBLANES,)),
            pltpu.SemaphoreType.DMA((spread // SUBLANES,)),
        ],
        compiler_params=pltpu.CompilerParams(vmem_limit_bytes=50 << 20),
        name="degrees",
    )(received, *tables, factors)


def fast_local(samples):
    devices = lax.axis_size("beta")
    device = lax.axis_index("beta")
    functions, grid_size = samples.shape[1:3]
    spread = grid_size // 2
    sent = spectrum_call(samples, devices)
    received = lax.all_to_all(sent, "beta", split_axis=0, concat_axis=0, tiled=True)
    gammas, alphas = quarter_tables(spread, devices)
    alphas = lax.dynamic_index_in_dim(jnp.asarray(alphas), device, 0, keepdims=False)
    factors = factor_call(jnp.asarray(gammas), alphas)
    coeffs, shares = degree_call(received, factors, spread)
    order = list(range(devices))[::-1]
    shares = lax.all_to_all(
        shares, "beta", split_axis=0, concat_axis=0, tiled=True, axis_index_groups=[order]
    )
    scale = (1.0 / (2.0 * np.arange(spread) + 1.0) ** 2).astype(np.float32)
    return coeffs, jnp.sum(shares[:, :functions, :spread], axis=0) * scale[None, :]


def local(samples):
    devices = lax.axis_size("beta")
    local_beta, functions, grid_size = samples.shape[:3]
    tiled = grid_size == LANES and local_beta == SUBLANES and grid_size == devices * SUBLANES
    if tiled and functions % 2 == 0:
        return fast_local(samples)
    return general_local(samples)


def solution(mesh):
    return jax.shard_map(
        local,
        mesh=mesh,
        in_specs=(P("beta", "grp", None, None),),
        out_specs=(P("beta", None, "grp", None, None), P("grp", None)),
        check_vma=False,
    )
```

```python
import math

import jax
import jax.numpy as jnp
import numpy as np
from jax import lax
from jax.experimental import pallas as pl
from jax.experimental.pallas import tpu as pltpu
from jax.sharding import PartitionSpec as P

HIGHEST = lax.Precision.HIGHEST
SUBLANES = 8
LANES = 128


def beta_angles(spread):
    grid_size = 2 * spread
    return (2.0 * jnp.arange(grid_size, dtype=jnp.float32) + 1.0) * (jnp.pi / (4.0 * spread))


def quadrature(spread):
    angles = beta_angles(spread)
    odd_terms = 2.0 * jnp.arange(spread, dtype=jnp.float32) + 1.0
    series = jnp.sum(jnp.sin(angles[:, None] * odd_terms[None, :]) / odd_terms[None, :], axis=1)
    return 2.0 / spread * jnp.sin(angles) * series


def gamma_table(spread):
    grid_size = 2 * spread
    positions = jnp.arange(grid_size, dtype=jnp.int32)
    orders = jnp.arange(spread, dtype=jnp.int32)
    phase_index = positions[:, None] * orders[None, :] % grid_size
    angles = phase_index.astype(jnp.float32) * (2.0 * jnp.pi / grid_size)
    return jnp.concatenate([jnp.cos(angles), -jnp.sin(angles)], axis=1)


def alpha_table(spread, row_index):
    grid_size = 2 * spread
    positions = jnp.arange(grid_size, dtype=jnp.int32)
    phase_index = row_index[:, None] * positions[None, :] % grid_size
    angles = phase_index.astype(jnp.float32) * (2.0 * jnp.pi / grid_size)
    cosine = jnp.cos(angles) / grid_size
    sine_part = jnp.sin(angles) / grid_size
    real_rows = jnp.stack([cosine, sine_part], axis=1)
    imag_rows = jnp.stack([-sine_part, cosine], axis=1)
    return jnp.stack([real_rows, imag_rows], axis=0)


def log_factorial(value, float_type):
    return lax.lgamma((value + 1).astype(float_type))


def wigner_start(alpha_order, gamma_order, log_cosine, log_sine):
    float_type = log_cosine.dtype
    lowest = jnp.maximum(jnp.abs(alpha_order), gamma_order)
    shift_low = jnp.maximum(0, gamma_order - alpha_order)
    magnitude = 0.5 * (
        log_factorial(lowest + alpha_order, float_type)
        + log_factorial(lowest - alpha_order, float_type)
        + log_factorial(lowest + gamma_order, float_type)
        + log_factorial(lowest - gamma_order, float_type)
    )
    magnitude = (
        magnitude
        - log_factorial(lowest + gamma_order - shift_low, float_type)
        - log_factorial(shift_low, float_type)
    )
    magnitude = magnitude - log_factorial(alpha_order - gamma_order + shift_low, float_type)
    magnitude = magnitude - log_factorial(lowest - alpha_order - shift_low, float_type)
    cos_power = (2 * lowest + gamma_order - alpha_order - 2 * shift_low).astype(float_type)
    sin_power = (alpha_order - gamma_order + 2 * shift_low).astype(float_type)
    parity = (alpha_order - gamma_order + shift_low) % 2
    sign_factor = (1 - 2 * parity).astype(float_type)
    return sign_factor * jnp.exp(magnitude + cos_power * log_cosine + sin_power * log_sine)


def advance(degree, carried, alpha_order, gamma_order, cos_angles, start_value, lowest):
    former, current = carried
    float_type = current.dtype
    previous = (degree - 1).astype(float_type)
    alpha_float = alpha_order.astype(float_type)
    gamma_float = gamma_order.astype(float_type)
    cross_ratio = alpha_float * gamma_float / jnp.maximum(previous * (previous + 1.0), 1.0)
    upper_term = ((previous + 1.0) * (previous + 1.0) - alpha_float * alpha_float) * (
        (previous + 1.0) * (previous + 1.0) - gamma_float * gamma_float
    )
    lower_term = (previous * previous - alpha_float * alpha_float) * (
        previous * previous - gamma_float * gamma_float
    )
    root_upper = jnp.sqrt(jnp.maximum(upper_term, 1.0))
    forward = (previous + 1.0) * (2.0 * previous + 1.0) / root_upper
    backward = (
        (previous + 1.0)
        * jnp.sqrt(jnp.maximum(lower_term, 0.0))
        / (jnp.maximum(previous, 1.0) * root_upper)
    )
    recurred = forward * (cos_angles - cross_ratio) * current - backward * former
    renewed = jnp.where(degree == lowest, start_value, recurred)
    return (current, renewed)


def degree_rows(row_index, weighted, spread):
    stride = 8
    grid_size = 2 * spread
    group_size = row_index.shape[0]
    channels = weighted.shape[2]
    block_count = spread // stride
    alpha_order = jnp.where(row_index < spread, row_index, row_index - grid_size)[:, None, None]
    gamma_order = jnp.arange(spread, dtype=jnp.int32)[None, None, :]
    angles = beta_angles(spread)
    cos_angles = jnp.cos(angles)[None, :, None]
    log_cosine = jnp.log(jnp.cos(0.5 * angles))[None, :, None]
    log_sine = jnp.log(jnp.sin(0.5 * angles))[None, :, None]
    lowest = jnp.maximum(jnp.abs(alpha_order), gamma_order)
    start_value = wigner_start(alpha_order, gamma_order, log_cosine, log_sine)
    first_block = jnp.min(jnp.abs(alpha_order)) // stride
    empty_state = jnp.zeros((group_size, grid_size, spread), jnp.float32)

    def compute_block(operands):
        block_index, former, current = operands
        levels = []
        for offset in range(stride):
            former, current = advance(
                block_index * stride + offset,
                (former, current),
                alpha_order,
                gamma_order,
                cos_angles,
                start_value,
                lowest,
            )
            levels.append(current)
        stacked = jnp.stack(levels, axis=0)
        block_part = jnp.einsum("jgkq,kgcq->gcjq", stacked, weighted, precision=HIGHEST)
        return (former, current, block_part)

    def skip_block(operands):
        block_index, former, current = operands
        return (former, current, jnp.zeros((group_size, channels, stride, spread), jnp.float32))

    def block_step(carried, block_index):
        former, current = carried
        former, current, block_part = lax.cond(
            block_index >= first_block, compute_block, skip_block, (block_index, former, current)
        )
        return ((former, current), block_part)

    _, parts = lax.scan(
        block_step, (empty_state, empty_state), jnp.arange(block_count, dtype=jnp.int32)
    )
    output = jnp.transpose(parts, (1, 2, 0, 3, 4)).reshape(group_size, channels, spread, spread)
    degree_scale = 8.0 * jnp.sqrt(2.0 * jnp.arange(spread, dtype=jnp.float32) + 1.0)
    return output * degree_scale[None, None, :, None]


def degree_energy(coeffs, functions, spread):
    split_view = coeffs.reshape(coeffs.shape[0], 2, functions, spread, spread)
    multiplicity = jnp.where(jnp.arange(spread) == 0, 1.0, 2.0).astype(jnp.float32)
    energy_sum = jnp.sum(split_view * split_view * multiplicity, axis=(0, 1, 4))
    degrees = 2.0 * jnp.arange(spread, dtype=jnp.float32) + 1.0
    return energy_sum / (degrees * degrees)[None, :]


def general_local(samples):
    devices = lax.axis_size("beta")
    device = lax.axis_index("beta")
    local_beta = samples.shape[0]
    functions = samples.shape[1]
    grid_size = samples.shape[2]
    spread = grid_size // 2
    channels = 2 * functions
    row_count = grid_size // devices
    natural_rows = jnp.arange(grid_size, dtype=jnp.int32)
    halfway = jnp.einsum("kfag,gx->kfax", samples, gamma_table(spread), precision=HIGHEST)
    halfway = halfway.reshape(local_beta, functions, grid_size, 2, spread)
    spectrum = jnp.einsum(
        "kfacq,spca->kpsfq", halfway, alpha_table(spread, natural_rows), precision=HIGHEST
    )
    spectrum = spectrum.reshape(local_beta, grid_size, channels, spread)
    received = lax.all_to_all(spectrum, "beta", split_axis=1, concat_axis=0, tiled=True)
    weighted = received * quadrature(spread)[:, None, None, None]
    owned_rows = lax.dynamic_slice_in_dim(natural_rows, device * row_count, row_count)
    computed = degree_rows(owned_rows, weighted, spread)
    power_part = degree_energy(computed, functions, spread)
    coeffs = computed
    power = lax.psum(power_part, "beta")
    coeffs = coeffs.reshape(row_count, 2, functions, spread, spread)
    return (coeffs, power)


def wigner_quarter(spread):
    alpha = np.arange(1 - spread, spread)[:, None]
    gamma = np.arange(spread)[None, :]
    lowest = np.maximum(np.abs(alpha), gamma)
    shift = np.maximum(0, gamma - alpha)
    logs = np.array([math.lgamma(value + 1.0) for value in range(2 * spread)])
    magnitude = 0.5 * (
        logs[lowest + alpha] + logs[lowest - alpha] + logs[lowest + gamma] + logs[lowest - gamma]
    )
    magnitude = magnitude - logs[lowest + gamma - shift] - logs[shift]
    magnitude = magnitude - logs[alpha - gamma + shift] - logs[lowest - alpha - shift]
    sign = 1.0 - 2.0 * ((alpha - gamma + shift) % 2)
    first = sign * np.exp(magnitude - lowest * math.log(2.0))
    squares_a, squares_g = alpha.astype(np.float64) ** 2, gamma.astype(np.float64) ** 2
    former, current, levels = np.zeros(first.shape), np.zeros(first.shape), []
    for degree in range(spread):
        before = degree - 1.0
        upper = np.sqrt(np.maximum((degree**2 - squares_a) * (degree**2 - squares_g), 1.0))
        lower = np.sqrt(np.maximum((before**2 - squares_a) * (before**2 - squares_g), 0.0))
        cross = alpha * gamma / max(before * degree, 1.0)
        follow = degree * (2.0 * before + 1.0) / upper * -cross * current
        follow = follow - degree * lower / (max(before, 1.0) * upper) * former
        former, current = current, np.where(lowest == degree, first, follow)
        levels.append(current)
    return np.stack(levels)


def split_pair(table):
    high = np.asarray(table).astype(jnp.bfloat16)
    return high, (table - high.astype(np.float64)).astype(jnp.bfloat16)


def fourier_tables(spread):
    grid = 2 * spread
    at = np.arange(grid)
    phase = 2.0 * np.pi / grid * (at[:, None] * np.arange(spread)[None, :] % grid)
    cosine, sine = np.cos(phase), -np.sin(phase)
    gamma_part = np.concatenate([cosine, sine], axis=1)
    phase = 2.0 * np.pi / grid * (at[:, None] * at[None, :] % grid)
    alpha_part = np.concatenate([np.cos(phase), np.sin(phase)], axis=1) / grid
    return gamma_part, alpha_part


def beta_table(spread):
    angles = (2.0 * np.arange(2 * spread) + 1.0) * (np.pi / (4.0 * spread))
    odd = 2.0 * np.arange(spread) + 1.0
    series = np.sum(np.sin(angles[:, None] * odd[None, :]) / odd[None, :], axis=1)
    weight = 2.0 / spread * np.sin(angles) * series
    order = np.concatenate([np.arange(0, spread, 2), np.arange(1, spread, 2)])
    fold = np.where(order == 0, 1.0, 2.0)[:, None] * weight[None, :]
    turn = order[:, None] * angles[None, :]
    return np.concatenate([fold * np.cos(turn), fold * np.sin(turn)], axis=0)


def sign_masks(spread):
    step = (np.arange(SUBLANES)[:, None] - np.arange(spread)[None, :]) % 4
    even = np.where(step == 0, 1.0, np.where(step == 2, -1.0, 0.0))
    odd = np.where(step == 3, 1.0, np.where(step == 1, -1.0, 0.0))
    return np.concatenate([even, even], axis=1), np.concatenate([odd, odd], axis=1)


def block_steps(spread):
    blocks = spread // SUBLANES
    return [(block, chunk) for block in range(blocks) for chunk in range(block + 1)]


def quarter_tables(spread, devices):
    quarter = wigner_quarter(spread)
    rows = np.arange(2 * spread)
    orders = np.where(rows < spread, rows, rows - 2 * spread)
    by_row = quarter[:, np.maximum(orders, 1 - spread) + spread - 1, :]
    by_row = np.where((orders > -spread)[None, :, None], by_row, 0.0)
    by_row = by_row * (8.0 * np.sqrt(2.0 * np.arange(spread) + 1.0))[:, None, None]
    gammas, alphas = [], []
    for block, chunk in block_steps(spread):
        degrees = slice(block * SUBLANES, (block + 1) * SUBLANES)
        part = slice(chunk * SUBLANES, (chunk + 1) * SUBLANES)
        gammas.append(np.swapaxes(quarter[degrees, spread - 1 :, part], 1, 2).reshape(-1, LANES))
        table = np.swapaxes(by_row[degrees, :, part], 0, 1)
        alphas.append(table.reshape(devices, SUBLANES, SUBLANES * SUBLANES))
    alphas = np.stack(alphas, axis=1)
    alphas = np.concatenate([alphas[:, 0::2], alphas[:, 1::2]], axis=-1)
    return np.stack(gammas).astype(np.float32), alphas.astype(np.float32)


def split_value(value):
    high = value.astype(jnp.bfloat16)
    return high, (value - high.astype(jnp.float32)).astype(jnp.bfloat16)


def dot(left, right):
    return jnp.dot(left, right, preferred_element_type=jnp.float32)


def spectrum_kernel(x_ref, gamma_two, alpha_two, out_ref):
    count, _, grid, _ = x_ref.shape
    blocks = out_ref.shape[0]
    for f in range(x_ref.shape[1]):
        high, low = split_value(x_ref[:, f].reshape(count * grid, grid))
        both = dot(jnp.concatenate([high, low], axis=1), gamma_two[...])
        half = both[:, :LANES] + both[:, LANES:]
        lane = lax.broadcasted_iota(jnp.int32, (1, LANES), 1)
        sign = jnp.where(lane < LANES // 2, 1.0, -1.0)
        for k in range(0, count, 2):
            pairs = [half[(k + i) * grid : (k + i + 1) * grid] for i in range(2)]
            pair = jnp.concatenate(
                [
                    jnp.concatenate(pairs, axis=1),
                    jnp.concatenate([pltpu.roll(p, LANES // 2, 1) * sign for p in pairs], axis=1),
                ],
                axis=0,
            )
            high, low = split_value(pair)
            both = dot(alpha_two[...], high)
            rows = both[:grid] + both[grid:] + dot(alpha_two[:grid], low)
            for i in range(2):
                for d in range(blocks):
                    out_ref[d, f, pl.ds(k + i, SUBLANES, stride=count), :] = rows[
                        d * SUBLANES : (d + 1) * SUBLANES, i * LANES : (i + 1) * LANES
                    ]


def spectrum_call(samples, devices):
    count, functions, grid, _ = samples.shape
    gamma_part, alpha_part = fourier_tables(grid // 2)
    gamma_hi, gamma_lo = split_pair(gamma_part)
    above = np.concatenate([gamma_hi, gamma_lo], axis=1)
    below = np.concatenate([gamma_hi, np.zeros_like(gamma_lo)], axis=1)
    tables = [np.concatenate([above, below], axis=0)]
    tables.append(np.concatenate(split_pair(alpha_part), axis=0))
    rows = grid // devices * count
    steps = 2
    some = functions // steps
    whole = lambda table: pl.BlockSpec(table.shape, lambda f: (0, 0))
    return pl.pallas_call(
        spectrum_kernel,
        grid=(steps,),
        in_specs=[pl.BlockSpec((count, some, grid, grid), lambda f: (0, f, 0, 0))]
        + [whole(table) for table in tables],
        out_specs=pl.BlockSpec((devices, some, rows, LANES), lambda f: (0, f, 0, 0)),
        out_shape=jax.ShapeDtypeStruct((devices, functions, rows, LANES), jnp.float32),
        name="spectrum",
    )(samples, *tables)


def factor_kernel(gamma_ref, alpha_ref, out_ref):
    pairs = out_ref.shape[1]
    left = lax.broadcasted_iota(jnp.int32, (SUBLANES, LANES), 1) < LANES // 2

    def step(at, carry):
        column = alpha_ref[at]
        for half in range(2):
            for i in range(pairs):
                lane = 2 * (half * pairs + i)
                wide = [
                    jnp.broadcast_to(column[:, lane + j : lane + j + 1], (SUBLANES, LANES))
                    for j in range(2)
                ]
                row = gamma_ref[2 * at + half, i : i + 1, :]
                out_ref[2 * at + half, i] = jnp.where(left, wide[0], wide[1]) * row
        return carry

    lax.fori_loop(0, alpha_ref.shape[0], step, 0)


def factor_call(gammas, alphas):
    steps, pairs, _ = gammas.shape
    return pl.pallas_call(
        factor_kernel,
        out_shape=jax.ShapeDtypeStruct((steps, pairs, SUBLANES, LANES), jnp.float32),
        name="factors",
    )(gammas, alphas)


def degree_kernel(
    r_ref, beta_two, even_ref, odd_ref, source_ref, out_ref, pow_ref,
    t_ref, c_ref, e_ref, held_ref, factor_ref, sems, factor_sems,
):
    sources, functions, held, _ = r_ref.shape
    count = held // SUBLANES
    spread = beta_two.shape[0] // 4
    blocks = spread // SUBLANES
    firsts = [block * (block + 1) // 2 for block in range(blocks)]

    def factor_copy(block):
        part = pl.ds(firsts[block], block + 1)
        return pltpu.make_async_copy(
            source_ref.at[part], factor_ref.at[part], factor_sems.at[block]
        )

    row = lax.axis_index("beta") * SUBLANES
    smallest = jnp.where(row < spread, row, 2 * spread - row - SUBLANES + 1)
    first_block = smallest // SUBLANES
    for block in range(blocks):

        @pl.when(block >= first_block)
        def _():
            factor_copy(block).start()

    left = lax.broadcasted_iota(jnp.int32, (spread // 2, LANES), 1) < spread
    for f in range(0, functions, 2):
        for n in range(SUBLANES):
            parts = [
                r_ref[:, f + i, n * count : (n + 1) * count, :].reshape(sources * count, LANES)
                for i in range(2)
            ]
            high, low = split_value(jnp.concatenate(parts, axis=1))
            both = dot(beta_two[...], jnp.concatenate([high, low], axis=0))
            both = both[: 2 * spread] + both[2 * spread :]
            turned = [
                jnp.where(
                    even_ref[n : n + 1] != 0.0,
                    both[:spread, i * LANES : (i + 1) * LANES] * even_ref[n : n + 1],
                    both[spread:, i * LANES : (i + 1) * LANES] * odd_ref[n : n + 1],
                )
                for i in range(2)
            ]
            for i in range(2):
                evens, odds = turned[i][: spread // 2], turned[i][spread // 2 :]
                parted = (
                    jnp.where(left, evens, pltpu.roll(odds, spread, 1)),
                    jnp.where(left, pltpu.roll(evens, spread, 1), odds),
                )
                for part in range(2):
                    for b in range(spread // (2 * SUBLANES)):
                        t_ref[
                            part, f + i, pl.ds(b * SUBLANES * SUBLANES + n, SUBLANES, stride=SUBLANES), :
                        ] = parted[part][b * SUBLANES : (b + 1) * SUBLANES]

    zero = jnp.zeros((SUBLANES, LANES), jnp.float32)

    def out_copy(block):
        part = (slice(None), slice(None), slice(None), pl.ds(block * SUBLANES, SUBLANES))
        return pltpu.make_async_copy(held_ref.at[part], out_ref.at[part], sems.at[block])

    def fill(block):
        degrees = slice(block * SUBLANES, (block + 1) * SUBLANES)
        empty = jnp.zeros((SUBLANES, 2, functions, SUBLANES, spread), jnp.float32)
        held_ref[:, :, :, degrees, :] = empty
        for f in range(functions):
            e_ref[f, degrees, :] = zero

    channels = [(part, f) for part in range(2) for f in range(functions)]
    some = SUBLANES // 2

    def work(block):
        factor_copy(block).wait()
        degrees = slice(block * SUBLANES, (block + 1) * SUBLANES)
        for half in range(2):
            totals = [[zero] * len(channels) for _ in range(some)]
            for chunk in range(block + 1):
                for i in range(SUBLANES // 2):
                    row = (chunk * SUBLANES // 2 + i) * SUBLANES
                    values = [t_ref[part, f, row : row + SUBLANES, :] for part, f in channels]
                    for j in range(some):
                        at = (half * some + j) * SUBLANES // 2 + i
                        factor = factor_ref[firsts[block] + chunk, at]
                        totals[j] = [t + factor * v for t, v in zip(totals[j], values)]
            for j in range(some):
                for (part, f), total in zip(channels, totals[j]):
                    c_ref[part, f, pl.ds(half * some + j, SUBLANES, stride=SUBLANES), :] = total
        for f in range(functions):
            energy = zero
            for part in range(2):
                for n in range(SUBLANES):
                    tile = c_ref[part, f, n * SUBLANES : (n + 1) * SUBLANES, :]
                    tile = tile + pltpu.roll(tile, spread, 1)
                    energy += tile * tile
                    held_ref[n, part, f, degrees, :] = tile[:, :spread]
            e_ref[f, degrees, :] = energy

    for block in range(blocks):
        pl.when(block < first_block)(lambda: fill(block))
        pl.when(block >= first_block)(lambda: work(block))
        out_copy(block).start()

    lane = lax.broadcasted_iota(jnp.int32, (SUBLANES, LANES), 1)
    fold = jnp.where(lane == 0, 1.0, jnp.where(lane < spread, 2.0, 0.0)).astype(jnp.bfloat16)
    across = lambda part: lax.dot_general(
        fold, part, (((1,), (1,)), ((), ())), preferred_element_type=jnp.float32
    )
    place = lax.broadcasted_iota(jnp.int32, (SUBLANES, spread), 0)
    power = jnp.zeros((SUBLANES, spread), jnp.float32)
    for f in range(functions):
        high, low = split_value(e_ref[f])
        rest = e_ref[f] - high.astype(jnp.float32) - low.astype(jnp.float32)
        total = across(high) + across(low) + across(rest.astype(jnp.bfloat16))
        power = jnp.where(place == f, total, power)
    power = jnp.concatenate([power, jnp.zeros_like(power)], axis=1)
    for d in range(pow_ref.shape[0]):
        pow_ref[d] = power[:functions]

    for block in range(blocks):
        out_copy(block).wait()


def degree_call(received, factors, spread):
    functions = received.shape[1]
    high, low = split_pair(beta_table(spread))
    above = np.concatenate([high, high], axis=1)
    below = np.concatenate([low, np.zeros_like(low)], axis=1)
    tables = [np.concatenate([above, below], axis=0)]
    tables += [mask.astype(np.float32) for mask in sign_masks(spread)]
    shape = (SUBLANES, 2, functions, spread, spread)
    vmem = pl.BlockSpec(memory_space=pltpu.VMEM)
    return pl.pallas_call(
        degree_kernel,
        in_specs=[vmem] * 4 + [pl.BlockSpec(memory_space=pl.ANY)],
        out_specs=[pl.BlockSpec(memory_space=pl.ANY), vmem],
        out_shape=[
            jax.ShapeDtypeStruct(shape, jnp.float32),
            jax.ShapeDtypeStruct((received.shape[0], functions, LANES), jnp.float32),
        ],
        scratch_shapes=[
            pltpu.VMEM((2, functions, spread // 2 * SUBLANES, LANES), jnp.float32),
            pltpu.VMEM((2, functions, SUBLANES * SUBLANES, LANES), jnp.float32),
            pltpu.VMEM((functions, spread, LANES), jnp.float32),
            pltpu.VMEM(shape, jnp.float32),
            pltpu.VMEM(factors.shape, jnp.float32),
            pltpu.SemaphoreType.DMA((spread // SUBLANES,)),
            pltpu.SemaphoreType.DMA((spread // SUBLANES,)),
        ],
        compiler_params=pltpu.CompilerParams(vmem_limit_bytes=50 << 20),
        name="degrees",
    )(received, *tables, factors)


def fast_local(samples):
    devices = lax.axis_size("beta")
    device = lax.axis_index("beta")
    functions, grid_size = samples.shape[1:3]
    spread = grid_size // 2
    sent = spectrum_call(samples, devices)
    received = lax.all_to_all(sent, "beta", split_axis=0, concat_axis=0, tiled=True)
    gammas, alphas = quarter_tables(spread, devices)
    alphas = lax.dynamic_index_in_dim(jnp.asarray(alphas), device, 0, keepdims=False)
    factors = factor_call(jnp.asarray(gammas), alphas)
    coeffs, shares = degree_call(received, factors, spread)
    order = list(range(devices))[::-1]
    shares = lax.all_to_all(
        shares, "beta", split_axis=0, concat_axis=0, tiled=True, axis_index_groups=[order]
    )
    scale = (1.0 / (2.0 * np.arange(spread) + 1.0) ** 2).astype(np.float32)
    return coeffs, jnp.sum(shares[:, :, :spread], axis=0) * scale[None, :]


def local(samples):
    devices = lax.axis_size("beta")
    local_beta, functions, grid_size = samples.shape[:3]
    tiled = grid_size == LANES and local_beta == SUBLANES and grid_size == devices * SUBLANES
    if tiled and functions % 2 == 0:
        return fast_local(samples)
    return general_local(samples)


def solution(mesh):
    return jax.shard_map(
        local,
        mesh=mesh,
        in_specs=(P("beta", "grp", None, None),),
        out_specs=(P("beta", None, "grp", None, None), P("grp", None)),
        check_vma=False,
    )
```

```python
import math

import jax
import jax.numpy as jnp
import numpy as np
from jax import lax
from jax.experimental import pallas as pl
from jax.experimental.pallas import tpu as pltpu
from jax.sharding import PartitionSpec as P

HIGHEST = lax.Precision.HIGHEST
SUBLANES = 8
LANES = 128


def beta_angles(spread):
    grid_size = 2 * spread
    return (2.0 * jnp.arange(grid_size, dtype=jnp.float32) + 1.0) * (jnp.pi / (4.0 * spread))


def quadrature(spread):
    angles = beta_angles(spread)
    odd_terms = 2.0 * jnp.arange(spread, dtype=jnp.float32) + 1.0
    series = jnp.sum(jnp.sin(angles[:, None] * odd_terms[None, :]) / odd_terms[None, :], axis=1)
    return 2.0 / spread * jnp.sin(angles) * series


def gamma_table(spread):
    grid_size = 2 * spread
    positions = jnp.arange(grid_size, dtype=jnp.int32)
    orders = jnp.arange(spread, dtype=jnp.int32)
    phase_index = positions[:, None] * orders[None, :] % grid_size
    angles = phase_index.astype(jnp.float32) * (2.0 * jnp.pi / grid_size)
    return jnp.concatenate([jnp.cos(angles), -jnp.sin(angles)], axis=1)


def alpha_table(spread, row_index):
    grid_size = 2 * spread
    positions = jnp.arange(grid_size, dtype=jnp.int32)
    phase_index = row_index[:, None] * positions[None, :] % grid_size
    angles = phase_index.astype(jnp.float32) * (2.0 * jnp.pi / grid_size)
    cosine = jnp.cos(angles) / grid_size
    sine_part = jnp.sin(angles) / grid_size
    real_rows = jnp.stack([cosine, sine_part], axis=1)
    imag_rows = jnp.stack([-sine_part, cosine], axis=1)
    return jnp.stack([real_rows, imag_rows], axis=0)


def log_factorial(value, float_type):
    return lax.lgamma((value + 1).astype(float_type))


def wigner_start(alpha_order, gamma_order, log_cosine, log_sine):
    float_type = log_cosine.dtype
    lowest = jnp.maximum(jnp.abs(alpha_order), gamma_order)
    shift_low = jnp.maximum(0, gamma_order - alpha_order)
    magnitude = 0.5 * (
        log_factorial(lowest + alpha_order, float_type)
        + log_factorial(lowest - alpha_order, float_type)
        + log_factorial(lowest + gamma_order, float_type)
        + log_factorial(lowest - gamma_order, float_type)
    )
    magnitude = (
        magnitude
        - log_factorial(lowest + gamma_order - shift_low, float_type)
        - log_factorial(shift_low, float_type)
    )
    magnitude = magnitude - log_factorial(alpha_order - gamma_order + shift_low, float_type)
    magnitude = magnitude - log_factorial(lowest - alpha_order - shift_low, float_type)
    cos_power = (2 * lowest + gamma_order - alpha_order - 2 * shift_low).astype(float_type)
    sin_power = (alpha_order - gamma_order + 2 * shift_low).astype(float_type)
    parity = (alpha_order - gamma_order + shift_low) % 2
    sign_factor = (1 - 2 * parity).astype(float_type)
    return sign_factor * jnp.exp(magnitude + cos_power * log_cosine + sin_power * log_sine)


def advance(degree, carried, alpha_order, gamma_order, cos_angles, start_value, lowest):
    former, current = carried
    float_type = current.dtype
    previous = (degree - 1).astype(float_type)
    alpha_float = alpha_order.astype(float_type)
    gamma_float = gamma_order.astype(float_type)
    cross_ratio = alpha_float * gamma_float / jnp.maximum(previous * (previous + 1.0), 1.0)
    upper_term = ((previous + 1.0) * (previous + 1.0) - alpha_float * alpha_float) * (
        (previous + 1.0) * (previous + 1.0) - gamma_float * gamma_float
    )
    lower_term = (previous * previous - alpha_float * alpha_float) * (
        previous * previous - gamma_float * gamma_float
    )
    root_upper = jnp.sqrt(jnp.maximum(upper_term, 1.0))
    forward = (previous + 1.0) * (2.0 * previous + 1.0) / root_upper
    backward = (
        (previous + 1.0)
        * jnp.sqrt(jnp.maximum(lower_term, 0.0))
        / (jnp.maximum(previous, 1.0) * root_upper)
    )
    recurred = forward * (cos_angles - cross_ratio) * current - backward * former
    renewed = jnp.where(degree == lowest, start_value, recurred)
    return (current, renewed)


def degree_rows(row_index, weighted, spread):
    stride = 8
    grid_size = 2 * spread
    group_size = row_index.shape[0]
    channels = weighted.shape[2]
    block_count = spread // stride
    alpha_order = jnp.where(row_index < spread, row_index, row_index - grid_size)[:, None, None]
    gamma_order = jnp.arange(spread, dtype=jnp.int32)[None, None, :]
    angles = beta_angles(spread)
    cos_angles = jnp.cos(angles)[None, :, None]
    log_cosine = jnp.log(jnp.cos(0.5 * angles))[None, :, None]
    log_sine = jnp.log(jnp.sin(0.5 * angles))[None, :, None]
    lowest = jnp.maximum(jnp.abs(alpha_order), gamma_order)
    start_value = wigner_start(alpha_order, gamma_order, log_cosine, log_sine)
    first_block = jnp.min(jnp.abs(alpha_order)) // stride
    empty_state = jnp.zeros((group_size, grid_size, spread), jnp.float32)

    def compute_block(operands):
        block_index, former, current = operands
        levels = []
        for offset in range(stride):
            former, current = advance(
                block_index * stride + offset,
                (former, current),
                alpha_order,
                gamma_order,
                cos_angles,
                start_value,
                lowest,
            )
            levels.append(current)
        stacked = jnp.stack(levels, axis=0)
        block_part = jnp.einsum("jgkq,kgcq->gcjq", stacked, weighted, precision=HIGHEST)
        return (former, current, block_part)

    def skip_block(operands):
        block_index, former, current = operands
        return (former, current, jnp.zeros((group_size, channels, stride, spread), jnp.float32))

    def block_step(carried, block_index):
        former, current = carried
        former, current, block_part = lax.cond(
            block_index >= first_block, compute_block, skip_block, (block_index, former, current)
        )
        return ((former, current), block_part)

    _, parts = lax.scan(
        block_step, (empty_state, empty_state), jnp.arange(block_count, dtype=jnp.int32)
    )
    output = jnp.transpose(parts, (1, 2, 0, 3, 4)).reshape(group_size, channels, spread, spread)
    degree_scale = 8.0 * jnp.sqrt(2.0 * jnp.arange(spread, dtype=jnp.float32) + 1.0)
    return output * degree_scale[None, None, :, None]


def degree_energy(coeffs, functions, spread):
    split_view = coeffs.reshape(coeffs.shape[0], 2, functions, spread, spread)
    multiplicity = jnp.where(jnp.arange(spread) == 0, 1.0, 2.0).astype(jnp.float32)
    energy_sum = jnp.sum(split_view * split_view * multiplicity, axis=(0, 1, 4))
    degrees = 2.0 * jnp.arange(spread, dtype=jnp.float32) + 1.0
    return energy_sum / (degrees * degrees)[None, :]


def general_local(samples):
    devices = lax.axis_size("beta")
    device = lax.axis_index("beta")
    local_beta = samples.shape[0]
    functions = samples.shape[1]
    grid_size = samples.shape[2]
    spread = grid_size // 2
    channels = 2 * functions
    row_count = grid_size // devices
    natural_rows = jnp.arange(grid_size, dtype=jnp.int32)
    halfway = jnp.einsum("kfag,gx->kfax", samples, gamma_table(spread), precision=HIGHEST)
    halfway = halfway.reshape(local_beta, functions, grid_size, 2, spread)
    spectrum = jnp.einsum(
        "kfacq,spca->kpsfq", halfway, alpha_table(spread, natural_rows), precision=HIGHEST
    )
    spectrum = spectrum.reshape(local_beta, grid_size, channels, spread)
    received = lax.all_to_all(spectrum, "beta", split_axis=1, concat_axis=0, tiled=True)
    weighted = received * quadrature(spread)[:, None, None, None]
    owned_rows = lax.dynamic_slice_in_dim(natural_rows, device * row_count, row_count)
    computed = degree_rows(owned_rows, weighted, spread)
    power_part = degree_energy(computed, functions, spread)
    coeffs = computed
    power = lax.psum(power_part, "beta")
    coeffs = coeffs.reshape(row_count, 2, functions, spread, spread)
    return (coeffs, power)


def wigner_quarter(spread):
    alpha = np.arange(1 - spread, spread)[:, None]
    gamma = np.arange(spread)[None, :]
    lowest = np.maximum(np.abs(alpha), gamma)
    shift = np.maximum(0, gamma - alpha)
    logs = np.array([math.lgamma(value + 1.0) for value in range(2 * spread)])
    magnitude = 0.5 * (
        logs[lowest + alpha] + logs[lowest - alpha] + logs[lowest + gamma] + logs[lowest - gamma]
    )
    magnitude = magnitude - logs[lowest + gamma - shift] - logs[shift]
    magnitude = magnitude - logs[alpha - gamma + shift] - logs[lowest - alpha - shift]
    sign = 1.0 - 2.0 * ((alpha - gamma + shift) % 2)
    first = sign * np.exp(magnitude - lowest * math.log(2.0))
    squares_a, squares_g = alpha.astype(np.float64) ** 2, gamma.astype(np.float64) ** 2
    former, current, levels = np.zeros(first.shape), np.zeros(first.shape), []
    for degree in range(spread):
        before = degree - 1.0
        upper = np.sqrt(np.maximum((degree**2 - squares_a) * (degree**2 - squares_g), 1.0))
        lower = np.sqrt(np.maximum((before**2 - squares_a) * (before**2 - squares_g), 0.0))
        cross = alpha * gamma / max(before * degree, 1.0)
        follow = degree * (2.0 * before + 1.0) / upper * -cross * current
        follow = follow - degree * lower / (max(before, 1.0) * upper) * former
        former, current = current, np.where(lowest == degree, first, follow)
        levels.append(current)
    return np.stack(levels)


def split_pair(table):
    high = np.asarray(table).astype(jnp.bfloat16)
    return high, (table - high.astype(np.float64)).astype(jnp.bfloat16)


def fourier_tables(spread):
    grid = 2 * spread
    at = np.arange(grid)
    phase = 2.0 * np.pi / grid * (at[:, None] * np.arange(spread)[None, :] % grid)
    cosine, sine = np.cos(phase), -np.sin(phase)
    gamma_part = np.concatenate([cosine, sine], axis=1)
    phase = 2.0 * np.pi / grid * (at[:, None] * at[None, :] % grid)
    alpha_part = np.concatenate([np.cos(phase), np.sin(phase)], axis=1) / grid
    return gamma_part, alpha_part


def beta_table(spread):
    angles = (2.0 * np.arange(2 * spread) + 1.0) * (np.pi / (4.0 * spread))
    odd = 2.0 * np.arange(spread) + 1.0
    series = np.sum(np.sin(angles[:, None] * odd[None, :]) / odd[None, :], axis=1)
    weight = 2.0 / spread * np.sin(angles) * series
    order = np.concatenate([np.arange(0, spread, 2), np.arange(1, spread, 2)])
    fold = np.where(order == 0, 1.0, 2.0)[:, None] * weight[None, :]
    turn = order[:, None] * angles[None, :]
    return np.concatenate([fold * np.cos(turn), fold * np.sin(turn)], axis=0)


def sign_masks(spread):
    step = (np.arange(SUBLANES)[:, None] - np.arange(spread)[None, :]) % 4
    even = np.where(step == 0, 1.0, np.where(step == 2, -1.0, 0.0))
    odd = np.where(step == 3, 1.0, np.where(step == 1, -1.0, 0.0))
    return np.concatenate([even, even], axis=1), np.concatenate([odd, odd], axis=1)


def block_steps(spread):
    blocks = spread // SUBLANES
    return [(block, chunk) for block in range(blocks) for chunk in range(block + 1)]


def quarter_tables(spread, devices):
    quarter = wigner_quarter(spread)
    rows = np.arange(2 * spread)
    orders = np.where(rows < spread, rows, rows - 2 * spread)
    by_row = quarter[:, np.maximum(orders, 1 - spread) + spread - 1, :]
    by_row = np.where((orders > -spread)[None, :, None], by_row, 0.0)
    by_row = by_row * (8.0 * np.sqrt(2.0 * np.arange(spread) + 1.0))[:, None, None]
    gammas, alphas = [], []
    for block, chunk in block_steps(spread):
        degrees = slice(block * SUBLANES, (block + 1) * SUBLANES)
        part = slice(chunk * SUBLANES, (chunk + 1) * SUBLANES)
        gammas.append(np.swapaxes(quarter[degrees, spread - 1 :, part], 1, 2).reshape(-1, LANES))
        table = np.swapaxes(by_row[degrees, :, part], 0, 1)
        alphas.append(table.reshape(devices, SUBLANES, SUBLANES * SUBLANES))
    alphas = np.stack(alphas, axis=1)
    alphas = np.concatenate([alphas[:, 0::2], alphas[:, 1::2]], axis=-1)
    return np.stack(gammas).astype(np.float32), alphas.astype(np.float32)


def split_value(value):
    high = value.astype(jnp.bfloat16)
    return high, (value - high.astype(jnp.float32)).astype(jnp.bfloat16)


def dot(left, right):
    return jnp.dot(left, right, preferred_element_type=jnp.float32)


def data_order(devices):
    return [(place + devices // 2) % devices for place in range(devices)]


def spectrum_kernel(x_ref, gamma_two, alpha_two, out_ref):
    count, _, grid, _ = x_ref.shape
    order = data_order(out_ref.shape[0])
    for f in range(x_ref.shape[1]):
        high, low = split_value(x_ref[:, f].reshape(count * grid, grid))
        both = dot(jnp.concatenate([high, low], axis=1), gamma_two[...])
        half = both[:, :LANES] + both[:, LANES:]
        lane = lax.broadcasted_iota(jnp.int32, (1, LANES), 1)
        sign = jnp.where(lane < LANES // 2, 1.0, -1.0)
        for k in range(0, count, 2):
            pairs = [half[(k + i) * grid : (k + i + 1) * grid] for i in range(2)]
            pair = jnp.concatenate(
                [
                    jnp.concatenate(pairs, axis=1),
                    jnp.concatenate([pltpu.roll(p, LANES // 2, 1) * sign for p in pairs], axis=1),
                ],
                axis=0,
            )
            high, low = split_value(pair)
            both = dot(alpha_two[...], high)
            rows = both[:grid] + both[grid:] + dot(alpha_two[:grid], low)
            for i in range(2):
                for place, d in enumerate(order):
                    out_ref[place, f, pl.ds(k + i, SUBLANES, stride=count), :] = rows[
                        d * SUBLANES : (d + 1) * SUBLANES, i * LANES : (i + 1) * LANES
                    ]


def spectrum_call(samples, devices):
    count, functions, grid, _ = samples.shape
    gamma_part, alpha_part = fourier_tables(grid // 2)
    gamma_hi, gamma_lo = split_pair(gamma_part)
    above = np.concatenate([gamma_hi, gamma_lo], axis=1)
    below = np.concatenate([gamma_hi, np.zeros_like(gamma_lo)], axis=1)
    tables = [np.concatenate([above, below], axis=0)]
    tables.append(np.concatenate(split_pair(alpha_part), axis=0))
    rows = grid // devices * count
    steps = 2
    some = functions // steps
    whole = lambda table: pl.BlockSpec(table.shape, lambda f: (0, 0))
    return pl.pallas_call(
        spectrum_kernel,
        grid=(steps,),
        in_specs=[pl.BlockSpec((count, some, grid, grid), lambda f: (0, f, 0, 0))]
        + [whole(table) for table in tables],
        out_specs=pl.BlockSpec((devices, some, rows, LANES), lambda f: (0, f, 0, 0)),
        out_shape=jax.ShapeDtypeStruct((devices, functions, rows, LANES), jnp.float32),
        name="spectrum",
    )(samples, *tables)


def factor_kernel(gamma_ref, alpha_ref, out_ref):
    pairs = out_ref.shape[1]
    left = lax.broadcasted_iota(jnp.int32, (SUBLANES, LANES), 1) < LANES // 2

    def step(at, carry):
        column = alpha_ref[at]
        for half in range(2):
            for i in range(pairs):
                lane = 2 * (half * pairs + i)
                wide = [
                    jnp.broadcast_to(column[:, lane + j : lane + j + 1], (SUBLANES, LANES))
                    for j in range(2)
                ]
                row = gamma_ref[2 * at + half, i : i + 1, :]
                out_ref[2 * at + half, i] = jnp.where(left, wide[0], wide[1]) * row
        return carry

    lax.fori_loop(0, alpha_ref.shape[0], step, 0)


def factor_call(gammas, alphas):
    steps, pairs, _ = gammas.shape
    return pl.pallas_call(
        factor_kernel,
        out_shape=jax.ShapeDtypeStruct((steps, pairs, SUBLANES, LANES), jnp.float32),
        name="factors",
    )(gammas, alphas)


def degree_kernel(
    r_ref, beta_two, even_ref, odd_ref, source_ref, out_ref, pow_ref,
    t_ref, c_ref, e_ref, held_ref, factor_ref, sems, factor_sems,
):
    sources, functions, held, _ = r_ref.shape
    count = held // SUBLANES
    spread = beta_two.shape[0] // 4
    blocks = spread // SUBLANES
    firsts = [block * (block + 1) // 2 for block in range(blocks)]

    def factor_copy(block):
        part = pl.ds(firsts[block], block + 1)
        return pltpu.make_async_copy(
            source_ref.at[part], factor_ref.at[part], factor_sems.at[block]
        )

    row = lax.axis_index("beta") * SUBLANES
    smallest = jnp.where(row < spread, row, 2 * spread - row - SUBLANES + 1)
    first_block = smallest // SUBLANES
    for block in range(blocks):

        @pl.when(block >= first_block)
        def _():
            factor_copy(block).start()

    left = lax.broadcasted_iota(jnp.int32, (spread // 2, LANES), 1) < spread
    for f in range(0, functions, 2):
        for n in range(SUBLANES):
            parts = [
                r_ref[:, f + i, n * count : (n + 1) * count, :].reshape(sources * count, LANES)
                for i in range(2)
            ]
            high, low = split_value(jnp.concatenate(parts, axis=1))
            both = dot(beta_two[...], jnp.concatenate([high, low], axis=0))
            both = both[: 2 * spread] + both[2 * spread :]
            turned = [
                jnp.where(
                    even_ref[n : n + 1] != 0.0,
                    both[:spread, i * LANES : (i + 1) * LANES] * even_ref[n : n + 1],
                    both[spread:, i * LANES : (i + 1) * LANES] * odd_ref[n : n + 1],
                )
                for i in range(2)
            ]
            for i in range(2):
                evens, odds = turned[i][: spread // 2], turned[i][spread // 2 :]
                parted = (
                    jnp.where(left, evens, pltpu.roll(odds, spread, 1)),
                    jnp.where(left, pltpu.roll(evens, spread, 1), odds),
                )
                for part in range(2):
                    for b in range(spread // (2 * SUBLANES)):
                        t_ref[
                            part, f + i, pl.ds(b * SUBLANES * SUBLANES + n, SUBLANES, stride=SUBLANES), :
                        ] = parted[part][b * SUBLANES : (b + 1) * SUBLANES]

    zero = jnp.zeros((SUBLANES, LANES), jnp.float32)

    def out_copy(block):
        part = (slice(None), slice(None), slice(None), pl.ds(block * SUBLANES, SUBLANES))
        return pltpu.make_async_copy(held_ref.at[part], out_ref.at[part], sems.at[block])

    def fill(block):
        degrees = slice(block * SUBLANES, (block + 1) * SUBLANES)
        empty = jnp.zeros((SUBLANES, 2, functions, SUBLANES, spread), jnp.float32)
        held_ref[:, :, :, degrees, :] = empty
        for f in range(functions):
            e_ref[f, degrees, :] = zero

    channels = [(part, f) for part in range(2) for f in range(functions)]
    some = SUBLANES // 2

    def work(block):
        factor_copy(block).wait()
        degrees = slice(block * SUBLANES, (block + 1) * SUBLANES)
        for half in range(2):
            totals = [[zero] * len(channels) for _ in range(some)]
            for chunk in range(block + 1):
                for i in range(SUBLANES // 2):
                    row = (chunk * SUBLANES // 2 + i) * SUBLANES
                    values = [t_ref[part, f, row : row + SUBLANES, :] for part, f in channels]
                    for j in range(some):
                        at = (half * some + j) * SUBLANES // 2 + i
                        factor = factor_ref[firsts[block] + chunk, at]
                        totals[j] = [t + factor * v for t, v in zip(totals[j], values)]
            for j in range(some):
                for (part, f), total in zip(channels, totals[j]):
                    c_ref[part, f, pl.ds(half * some + j, SUBLANES, stride=SUBLANES), :] = total
        for f in range(functions):
            energy = zero
            for part in range(2):
                for n in range(SUBLANES):
                    tile = c_ref[part, f, n * SUBLANES : (n + 1) * SUBLANES, :]
                    tile = tile + pltpu.roll(tile, spread, 1)
                    energy += tile * tile
                    held_ref[n, part, f, degrees, :] = tile[:, :spread]
            e_ref[f, degrees, :] = energy

    for block in range(blocks):
        pl.when(block < first_block)(lambda: fill(block))
        pl.when(block >= first_block)(lambda: work(block))
        out_copy(block).start()

    lane = lax.broadcasted_iota(jnp.int32, (SUBLANES, LANES), 1)
    fold = jnp.where(lane == 0, 1.0, jnp.where(lane < spread, 2.0, 0.0)).astype(jnp.bfloat16)
    across = lambda part: lax.dot_general(
        fold, part, (((1,), (1,)), ((), ())), preferred_element_type=jnp.float32
    )
    place = lax.broadcasted_iota(jnp.int32, (SUBLANES, spread), 0)
    power = jnp.zeros((SUBLANES, spread), jnp.float32)
    for f in range(functions):
        high, low = split_value(e_ref[f])
        rest = e_ref[f] - high.astype(jnp.float32) - low.astype(jnp.float32)
        total = across(high) + across(low) + across(rest.astype(jnp.bfloat16))
        power = jnp.where(place == f, total, power)
    power = jnp.concatenate([power, jnp.zeros_like(power)], axis=1)
    for d in range(pow_ref.shape[0]):
        pow_ref[d] = power[:functions]

    for block in range(blocks):
        out_copy(block).wait()


def degree_call(received, factors, spread):
    functions = received.shape[1]
    sources = received.shape[0]
    table = beta_table(spread).reshape(2 * spread, sources, -1)[:, data_order(sources)]
    high, low = split_pair(table.reshape(2 * spread, 2 * spread))
    above = np.concatenate([high, high], axis=1)
    below = np.concatenate([low, np.zeros_like(low)], axis=1)
    tables = [np.concatenate([above, below], axis=0)]
    tables += [mask.astype(np.float32) for mask in sign_masks(spread)]
    shape = (SUBLANES, 2, functions, spread, spread)
    vmem = pl.BlockSpec(memory_space=pltpu.VMEM)
    return pl.pallas_call(
        degree_kernel,
        in_specs=[vmem] * 4 + [pl.BlockSpec(memory_space=pl.ANY)],
        out_specs=[pl.BlockSpec(memory_space=pl.ANY), vmem],
        out_shape=[
            jax.ShapeDtypeStruct(shape, jnp.float32),
            jax.ShapeDtypeStruct((received.shape[0], functions, LANES), jnp.float32),
        ],
        scratch_shapes=[
            pltpu.VMEM((2, functions, spread // 2 * SUBLANES, LANES), jnp.float32),
            pltpu.VMEM((2, functions, SUBLANES * SUBLANES, LANES), jnp.float32),
            pltpu.VMEM((functions, spread, LANES), jnp.float32),
            pltpu.VMEM(shape, jnp.float32),
            pltpu.VMEM(factors.shape, jnp.float32),
            pltpu.SemaphoreType.DMA((spread // SUBLANES,)),
            pltpu.SemaphoreType.DMA((spread // SUBLANES,)),
        ],
        compiler_params=pltpu.CompilerParams(vmem_limit_bytes=50 << 20),
        name="degrees",
    )(received, *tables, factors)


def fast_local(samples):
    devices = lax.axis_size("beta")
    device = lax.axis_index("beta")
    functions, grid_size = samples.shape[1:3]
    spread = grid_size // 2
    sent = spectrum_call(samples, devices)
    received = lax.all_to_all(
        sent, "beta", split_axis=0, concat_axis=0, tiled=True, axis_index_groups=[data_order(devices)]
    )
    gammas, alphas = quarter_tables(spread, devices)
    alphas = lax.dynamic_index_in_dim(jnp.asarray(alphas), device, 0, keepdims=False)
    factors = factor_call(jnp.asarray(gammas), alphas)
    coeffs, shares = degree_call(received, factors, spread)
    order = list(range(devices))[::-1]
    shares = lax.all_to_all(
        shares, "beta", split_axis=0, concat_axis=0, tiled=True, axis_index_groups=[order]
    )
    scale = (1.0 / (2.0 * np.arange(spread) + 1.0) ** 2).astype(np.float32)
    return coeffs, jnp.sum(shares[:, :, :spread], axis=0) * scale[None, :]


def local(samples):
    devices = lax.axis_size("beta")
    local_beta, functions, grid_size = samples.shape[:3]
    tiled = grid_size == LANES and local_beta == SUBLANES and grid_size == devices * SUBLANES
    if tiled and functions % 2 == 0:
        return fast_local(samples)
    return general_local(samples)


def solution(mesh):
    return jax.shard_map(
        local,
        mesh=mesh,
        in_specs=(P("beta", "grp", None, None),),
        out_specs=(P("beta", None, "grp", None, None), P("grp", None)),
        check_vma=False,
    )
```
